16 devices in a mesh: node: 2 (over z), local: 8 (over y, x, core).
Axes of the slice: x: 2, y: 2, z: 2, core: 2. Of those that a mesh axis runs over, the one named last changes fastest.
Arguments:
- x: bfloat16 [16, 256, 512], P(('node', 'local'))
- y_cot: bfloat16 [16, 256, 512], P(('node', 'local'))
- ln1_gain: bfloat16 [2, 512], P(None, ('node', 'local'))
- ln1_bias: bfloat16 [2, 512], P(None, ('node', 'local'))
- qkv_weight: bfloat16 [2, 512, 8, 192], P(None, ('node', 'local'))
- qkv_bias: bfloat16 [2, 1536], P(None, ('node', 'local'))
- out_weight: bfloat16 [2, 512, 512], P(None, ('node', 'local'))
- out_bias: bfloat16 [2, 512], P(None, ('node', 'local'))
- ln2_gain: bfloat16 [2, 512], P(None, ('node', 'local'))
- ln2_bias: bfloat16 [2, 512], P(None, ('node', 'local'))
- up_weight: bfloat16 [2, 512, 2048], P(None, ('node', 'local'))
- up_bias: bfloat16 [2, 2048], P(None, ('node', 'local'))
- down_weight: bfloat16 [2, 2048, 512], P(None, ('node', 'local'))
- down_bias: bfloat16 [2, 512], P(None, ('node', 'local'))
Outputs:
- output 1: bfloat16 [16, 256, 512], P(('node', 'local'))
- output 2: bfloat16 [16, 256, 512], P(('node', 'local'))
- output 3: bfloat16 [2, 512], P(None, ('node', 'local'))
- output 4: bfloat16 [2, 512], P(None, ('node', 'local'))
- output 5: bfloat16 [2, 512, 8, 192], P(None, ('node', 'local'))
- output 6: bfloat16 [2, 1536], P(None, ('node', 'local'))
- output 7: bfloat16 [2, 512, 512], P(None, ('node', 'local'))
- output 8: bfloat16 [2, 512], P(None, ('node', 'local'))
- output 9: bfloat16 [2, 512], P(None, ('node', 'local'))
- output 10: bfloat16 [2, 512], P(None, ('node', 'local'))
- output 11: bfloat16 [2, 512, 2048], P(None, ('node', 'local'))
- output 12: bfloat16 [2, 2048], P(None, ('node', 'local'))
- output 13: bfloat16 [2, 2048, 512], P(None, ('node', 'local'))
- output 14: bfloat16 [2, 512], P(None, ('node', 'local'))
All inputs are finite; a program needn't handle non-finite values.
Results may differ from the reference program's by a relative error of at most 0.0164011.
Values are sent between devices in bfloat16 or wider.
A program may use at most 1 GiB of HBM per device.

```python
import jax
import jax.numpy as jnp
from jax import lax

D_MODEL = 512
HEADS = 8
SEQ_LEN = 256
BATCH = 16
LAYERS = 2
HEAD_DIM = D_MODEL // HEADS
ROT_DIM = HEAD_DIM // 4
FF_DIM = 4 * D_MODEL
EPSILON = 1e-5


def slow_waves(rng_key, frequencies):
    amp_key, phase_key = jax.random.split(rng_key)
    positions = jnp.arange(SEQ_LEN, dtype=jnp.float32)[None, :, None] / SEQ_LEN
    wave_sum = jnp.zeros((BATCH, SEQ_LEN, D_MODEL), jnp.float32)
    for wave_idx, frequency in enumerate(frequencies):
        amplitude = jax.random.normal(jax.random.fold_in(amp_key, wave_idx), (BATCH, 1, D_MODEL), jnp.float32)
        phase_off = jax.random.uniform(jax.random.fold_in(phase_key, wave_idx), (BATCH, 1, D_MODEL), jnp.float32, 0.0, 6.283185307179586)
        wave_sum = wave_sum + amplitude * jnp.cos(6.283185307179586 * frequency * positions + phase_off)
    return wave_sum * (2.0 / len(frequencies)) ** 0.5


def normal_draw(rng_key, out_shape, spread, offset=0.0):
    return (offset + spread * jax.random.normal(rng_key, out_shape, jnp.float32)).astype(jnp.bfloat16)


def setup_inputs(seed: int = 0) -> dict:
    sub_keys = jax.random.split(jax.random.key(seed), 16)
    white_noise = jax.random.normal(sub_keys[0], (BATCH, SEQ_LEN, D_MODEL), jnp.float32)
    x = (0.8 * slow_waves(sub_keys[1], (0.5, 1.0, 2.0, 3.0)) + 0.6 * white_noise).astype(jnp.bfloat16)
    y_cot = normal_draw(sub_keys[2], (BATCH, SEQ_LEN, D_MODEL), (BATCH * SEQ_LEN) ** -0.25)
    width_scale = D_MODEL ** -0.5
    return {
        'x': x,
        'y_cot': y_cot,
        'ln1_gain': normal_draw(sub_keys[3], (LAYERS, D_MODEL), 0.25, 1.0),
        'ln1_bias': normal_draw(sub_keys[4], (LAYERS, D_MODEL), 0.25),
        'qkv_weight': normal_draw(sub_keys[5], (LAYERS, D_MODEL, HEADS, 3 * HEAD_DIM), width_scale),
        'qkv_bias': normal_draw(sub_keys[6], (LAYERS, 3 * D_MODEL), 0.3),
        'out_weight': normal_draw(sub_keys[7], (LAYERS, D_MODEL, D_MODEL), 1.5 * width_scale),
        'out_bias': normal_draw(sub_keys[8], (LAYERS, D_MODEL), 0.3),
        'ln2_gain': normal_draw(sub_keys[9], (LAYERS, D_MODEL), 0.25, 1.0),
        'ln2_bias': normal_draw(sub_keys[10], (LAYERS, D_MODEL), 0.25),
        'up_weight': normal_draw(sub_keys[11], (LAYERS, D_MODEL, FF_DIM), width_scale),
        'up_bias': normal_draw(sub_keys[12], (LAYERS, FF_DIM), 0.3),
        'down_weight': normal_draw(sub_keys[13], (LAYERS, FF_DIM, D_MODEL), FF_DIM ** -0.5),
        'down_bias': normal_draw(sub_keys[14], (LAYERS, D_MODEL), 0.3),
    }


def to_bf16(values):
    return values.astype(jnp.bfloat16).astype(jnp.float32)


def rope_tables():
    inv_freq = 1.0 / (10000.0 ** (jnp.arange(0, ROT_DIM, 2, dtype=jnp.float32) / ROT_DIM))
    angles = jnp.arange(SEQ_LEN, dtype=jnp.float32)[:, None] * inv_freq[None, :]
    angles = jnp.concatenate([angles, angles], axis=-1)
    return jnp.cos(angles), jnp.sin(angles)


def apply_rotary(vectors, cos_tab, sin_tab):
    half_dim = ROT_DIM // 2
    rot_part = vectors[..., :ROT_DIM]
    pass_part = vectors[..., ROT_DIM:]
    turned = jnp.concatenate([-rot_part[..., half_dim:], rot_part[..., :half_dim]], axis=-1)
    rot_part = rot_part * cos_tab[:, None, :] + turned * sin_tab[:, None, :]
    return jnp.concatenate([rot_part, pass_part], axis=-1)


def layer_norm(hidden, ln_gain, ln_bias):
    center = hidden - jnp.mean(hidden, axis=-1, keepdims=True)
    variance = jnp.mean(center * center, axis=-1, keepdims=True)
    return center * lax.rsqrt(variance + EPSILON) * ln_gain + ln_bias


def layer_forward(hidden, weights, cos_tab, sin_tab):
    (ln1_gain, ln1_bias, qkv_weight, qkv_bias, out_weight, out_bias,
     ln2_gain, ln2_bias, up_weight, up_bias, down_weight, down_bias) = weights
    normed_attn = to_bf16(layer_norm(hidden, ln1_gain, ln1_bias))
    normed_mlp = to_bf16(layer_norm(hidden, ln2_gain, ln2_bias))
    qkv_all = jnp.einsum('sd,dhe->she', normed_attn, qkv_weight) + qkv_bias.reshape(HEADS, 3 * HEAD_DIM)
    query_rot = to_bf16(apply_rotary(qkv_all[..., :HEAD_DIM], cos_tab, sin_tab))
    key_rot = to_bf16(apply_rotary(qkv_all[..., HEAD_DIM:2 * HEAD_DIM], cos_tab, sin_tab))
    values = to_bf16(qkv_all[..., 2 * HEAD_DIM:])
    scores = jnp.einsum('qhd,khd->hqk', query_rot, key_rot) * HEAD_DIM ** -0.5
    causal = jnp.arange(SEQ_LEN)[:, None] >= jnp.arange(SEQ_LEN)[None, :]
    scores = jnp.where(causal[None], scores, -1e30)
    attn_probs = to_bf16(jax.nn.softmax(scores, axis=-1))
    context = to_bf16(jnp.einsum('hqk,khd->qhd', attn_probs, values))
    attn_out = jnp.einsum('qhd,hde->qe', context, out_weight.reshape(HEADS, HEAD_DIM, D_MODEL)) + out_bias
    mlp_act = to_bf16(jax.nn.gelu(jnp.dot(normed_mlp, up_weight) + up_bias, approximate=False))
    mlp_out = jnp.dot(mlp_act, down_weight) + down_bias
    return hidden + attn_out + mlp_out


def reference(x, y_cot, ln1_gain, ln1_bias, qkv_weight, qkv_bias, out_weight, out_bias,
              ln2_gain, ln2_bias, up_weight, up_bias, down_weight, down_bias):
    stacked = tuple(tensor.astype(jnp.float32) for tensor in (
        ln1_gain, ln1_bias, qkv_weight, qkv_bias, out_weight, out_bias,
        ln2_gain, ln2_bias, up_weight, up_bias, down_weight, down_bias))
    cos_tab, sin_tab = rope_tables()

    def both_layers(x_seq, params):
        hidden = x_seq
        for layer_idx in range(LAYERS):
            hidden = to_bf16(layer_forward(hidden, [tensor[layer_idx] for tensor in params], cos_tab, sin_tab))
        return hidden

    def seq_step(grad_sums, seq_pair):
        x_seq, cot_seq = seq_pair
        seq_out, pullback = jax.vjp(both_layers, x_seq.astype(jnp.float32), stacked)
        x_bar, param_bars = pullback(cot_seq.astype(jnp.float32))
        grad_sums = tuple(grad_sum + part_grad for grad_sum, part_grad in zip(grad_sums, param_bars))
        return grad_sums, (seq_out.astype(jnp.bfloat16), x_bar.astype(jnp.bfloat16))

    zero_sums = tuple(jnp.zeros_like(tensor) for tensor in stacked)
    grad_sums, (y_out, x_grad) = lax.scan(seq_step, zero_sums, (x, y_cot))
    grad_list = [grad_sum.astype(jnp.bfloat16) for grad_sum in grad_sums]
    return (y_out, x_grad, grad_list[0], grad_list[1], grad_list[2], grad_list[3], grad_list[4], grad_list[5],
            grad_list[6], grad_list[7], grad_list[8], grad_list[9], grad_list[10], grad_list[11])
```

```python
import numpy as np
import jax
import jax.numpy as jnp
from jax import lax
from jax.experimental import pallas as pl
from jax.experimental.pallas import tpu as pltpu
from jax.sharding import PartitionSpec as P

BF, F32 = jnp.bfloat16, jnp.float32
MESH = pl.DeviceIdType.MESH
EPSILON = 1e-5
LAYERS, SEQ, DM, FF, ND = 2, 256, 512, 2048, 16
SH, HD, LN, Q3 = 32, 64, 128, 1536
ROWS = (SH, SH, LN)
COLS = (FF, FF, DM)
AO, UP, DN = 0, 1, 2
ORDERS = ((1, 2, 4), (2, 4, 1), (4, 1, 2))


def bit(v, a):
    return lax.rem(lax.div(v, a), 2)


def flip(v, mask):
    for a in (1, 2, 4):
        if mask & a:
            v = v + a - 2 * a * bit(v, a)
    return v


def mm(a, b):
    return jnp.dot(a, b, preferred_element_type=F32)


def mm_nt(a, b):
    return lax.dot_general(a, b, (((1,), (1,)), ((), ())), preferred_element_type=F32)


def mm_tn(a, b):
    return lax.dot_general(a, b, (((0,), (0,)), ((), ())), preferred_element_type=F32)


def axis_of(a, axes):
    return axes.index(a)


def kernel(x_ref, cot_ref, wa_in, wu_in, wd_in, small_in, rc_ref, r1_ref, r2_ref,
           y_ref, xg_ref, oa_ref, ou_ref, od_ref, os_ref,
           wa, wu, wd, ga, gu, gd, ra0, ru0, rd0, ra1, ru1, rd1, ra2, ru2, rd2, ra3, ru3, rd3,
           smalls, vec, upb, qkvb, gs, gr, gvec, gub, gqb,
           h1, dh, na, nm, nat, nmt, qkv, dqkv, ctx, dctx, acc, dnm,
           loc_sem, ag_send, ag_ici, ag_d2d, rs_send, rs_recv, sm_send, sm_recv, gr_send, gr_recv):
    me = lax.axis_index('node') * 8 + lax.axis_index('local')
    chip = lax.div(me, 2)
    core = lax.rem(me, 2)
    other = 1 - core
    W, G = (wa, wu, wd), (ga, gu, gd)
    R0, R1, R2, R3 = (ra0, ru0, rd0), (ra1, ru1, rd1), (ra2, ru2, rd2), (ra3, ru3, rd3)
    pend = []

    def dev(c, k):
        i = c * 2 + k
        return (lax.div(i, 8), lax.rem(i, 8))

    def block(l, w, c, k):
        return W[w].at[l, pl.ds(pl.multiple_of((c * 2 + k) * ROWS[w], ROWS[w]), ROWS[w])]

    counts = {}

    def ag_copy(l, w, src_mask, to, recv_sem):
        n = counts.get((l, w), 0)
        counts[(l, w)] = n + 1
        blk = block(l, w, flip(chip, src_mask), core)
        cp = pltpu.make_async_remote_copy(src_ref=blk, dst_ref=blk, send_sem=ag_send.at[l, w, n],
                                          recv_sem=recv_sem, device_id=to, device_id_type=MESH)
        cp.start()
        pend.append(cp)

    def to_link(l, w, mask, a):
        ag_copy(l, w, mask, dev(flip(chip, a), core), ag_ici.at[l, w, mask ^ a])

    def to_partner(l, w, mask):
        ag_copy(l, w, mask, dev(chip, other), ag_d2d.at[l, w, mask])

    def got(l, w, mask):
        blk = block(l, w, flip(chip, mask), core)
        pltpu.make_async_remote_copy(src_ref=blk, dst_ref=blk, send_sem=ag_send.at[l, w, 0],
                                     recv_sem=ag_ici.at[l, w, mask], device_id=dev(flip(chip, 1), core),
                                     device_id_type=MESH).wait_recv()

    def got_partner(l, w):
        for mask in range(8):
            blk = block(l, w, flip(chip, mask), other)
            pltpu.make_async_remote_copy(src_ref=blk, dst_ref=blk, send_sem=ag_send.at[l, w, 0],
                                         recv_sem=ag_d2d.at[l, w, mask], device_id=dev(chip, other),
                                         device_id_type=MESH).wait_recv()

    def ag0(l, w):
        a, b, c = ORDERS[w]
        to_link(l, w, 0, a)
        to_link(l, w, 0, b)
        to_link(l, w, 0, c)
        to_partner(l, w, 0)

    def ag1(l, w):
        a, b, c = ORDERS[w]
        got(l, w, a)
        to_link(l, w, a, b)
        to_link(l, w, a, c)
        to_partner(l, w, a)

    def ag2(l, w):
        a, b, c = ORDERS[w]
        for m in (b, a | b):
            got(l, w, m)
            to_link(l, w, m, c)
            to_partner(l, w, m)

    def ag3(l, w):
        a, b, c = ORDERS[w]
        for m in (c, a | c, b | c, 7):
            got(l, w, m)
            to_partner(l, w, m)

    def rs_copy(l, w, stage, src, dst, to):
        cp = pltpu.make_async_remote_copy(src_ref=src, dst_ref=dst, send_sem=rs_send.at[l, w, stage],
                                          recv_sem=rs_recv.at[l, w, stage], device_id=to, device_id_type=MESH)
        cp.start()
        return cp

    rs = {}

    def s0(l, w):
        rs[l, w, 0] = rs_copy(l, w, 0, G[w].at[:, :, :, other], R0[w].at[l], dev(chip, other))

    def pick(ax, n, v):
        return tuple(v if i == ax else slice(None) for i in range(n))

    def s1(l, w):
        a, b, c = ORDERS[w]
        rs[l, w, 0].wait_recv()
        for z in range(2):
            for y in range(2):
                for x in range(2):
                    R0[w][l, z, y, x] = R0[w][l, z, y, x] + G[w][z, y, x, core]
        ax = axis_of(a, [4, 2, 1])
        rs[l, w, 1] = rs_copy(l, w, 1, R0[w].at[(l,) + pick(ax, 3, 1 - bit(chip, a))], R1[w].at[l],
                              dev(flip(chip, a), core))

    def s2(l, w):
        a, b, c = ORDERS[w]
        rs[l, w, 1].wait_recv()
        ax = axis_of(a, [4, 2, 1])
        mine = bit(chip, a)
        for i in range(2):
            for j in range(2):
                idx = [i, j]
                idx.insert(ax, mine)
                R1[w][l, i, j] = R1[w][l, i, j] + R0[w][(l,) + tuple(idx)]
        ax = axis_of(b, [m for m in (4, 2, 1) if m != a])
        rs[l, w, 2] = rs_copy(l, w, 2, R1[w].at[(l,) + pick(ax, 2, 1 - bit(chip, b))], R2[w].at[l],
                              dev(flip(chip, b), core))

    def s3(l, w):
        a, b, c = ORDERS[w]
        rs[l, w, 2].wait_recv()
        ax = axis_of(b, [m for m in (4, 2, 1) if m != a])
        mine = bit(chip, b)
        for i in range(2):
            idx = [i]
            idx.insert(ax, mine)
            R2[w][l, i] = R2[w][l, i] + R1[w][(l,) + tuple(idx)]
        rs[l, w, 3] = rs_copy(l, w, 3, R2[w].at[l, 1 - bit(chip, c)], R3[w].at[l], dev(flip(chip, c), core))

    def s4(l, w):
        c = ORDERS[w][2]
        rs[l, w, 3].wait_recv()
        (oa_ref, ou_ref, od_ref)[w][l] = (R3[w][l] + R2[w][l, bit(chip, c)]).astype(BF)

    def normed(h_bf, l):
        h32 = h_bf.astype(F32)
        cen = h32 - jnp.mean(h32, axis=-1, keepdims=True)
        rstd = lax.rsqrt(jnp.mean(cen * cen, axis=-1, keepdims=True) + EPSILON)
        return cen * rstd, rstd

    def norms(h_ref, l, bwd):
        xhat, _ = normed(h_ref[...], l)
        n1 = (xhat * vec[l, 0:1, :] + vec[l, 1:2, :]).astype(BF)
        n2 = (xhat * vec[l, 3:4, :] + vec[l, 4:5, :]).astype(BF)
        na[...] = n1
        nm[...] = n2
        if bwd:
            nat[...] = n1.T
            nmt[...] = n2.T

    def rope(xs, back):
        c, p, q = rc_ref[...], r1_ref[...], r2_ref[...]
        if back:
            return xs * c + pltpu.roll(xs * p, 8, 1) + pltpu.roll(xs * q, 120, 1)
        return xs * c + pltpu.roll(xs, 120, 1) * p + pltpu.roll(xs, 8, 1) * q

    def make_qkv(l):
        for t in range(3):
            cols = slice(DM * t, DM * t + DM)
            raw = mm(na[...], wa[l, :, cols]) + qkvb[l, :, cols]
            for s in range(4):
                part = raw[:, LN * s:LN * s + LN]
                if t < 2:
                    part = rope(part, False)
                qkv[:, DM * t + LN * s:DM * t + LN * s + LN] = part.astype(BF)

    def heads(l, bwd):
        lane = lax.broadcasted_iota(jnp.int32, (1, LN), 1)
        masks = [(lane < HD).astype(F32).astype(BF), (lane >= HD).astype(F32).astype(BF)]
        causal = (lax.broadcasted_iota(jnp.int32, (SEQ, SEQ), 0) >= lax.broadcasted_iota(jnp.int32, (SEQ, SEQ), 1))

        def body(j, carry):
            col = pl.multiple_of(j * LN, LN)
            q, k, v = (qkv[:, pl.ds(col + DM * t, LN)] for t in range(3))
            ctx_sum = jnp.zeros((SEQ, LN), F32)
            if bwd:
                dc = dctx[:, pl.ds(col, LN)]
                dq = jnp.zeros((SEQ, LN), F32)
                dk = jnp.zeros((SEQ, LN), F32)
                dv = jnp.zeros((SEQ, LN), F32)
            for mask in masks:
                qm = q * mask
                sc = jnp.where(causal, mm_nt(qm, k) * 0.125, -1e30)
                e = jnp.exp(sc - jnp.max(sc, axis=-1, keepdims=True))
                p = e / jnp.sum(e, axis=-1, keepdims=True)
                pb = p.astype(BF)
                ctx_sum = ctx_sum + mm(pb, v * mask)
                if bwd:
                    dcm = dc * mask
                    dp = mm_nt(dcm, v).astype(BF).astype(F32)
                    dv = dv + mm_tn(pb, dcm)
                    ds = (p * (dp - jnp.sum(dp * p, axis=-1, keepdims=True)) * 0.125).astype(BF)
                    dq = dq + mm(ds, k * mask)
                    dk = dk + mm_tn(ds, qm)
            ctx[:, pl.ds(col, LN)] = ctx_sum.astype(BF)
            if bwd:
                for t, d in enumerate((dq, dk, dv)):
                    d = d.astype(BF).astype(F32)
                    if t < 2:
                        d = rope(d, True)
                    gqb[0:1, pl.ds(col + DM * t, LN)] = jnp.sum(d, axis=0, keepdims=True)
                    dqkv[:, pl.ds(col + DM * t, LN)] = d.astype(BF)
            return carry

        lax.fori_loop(0, 4, body, 0)

    def mlp(l, dout, fwd):
        if fwd:
            acc[...] = jnp.zeros_like(acc)
        if dout is not None:
            dnm[...] = jnp.zeros_like(dnm)

        def body(t, carry):
            col = pl.multiple_of(t * DM, DM)
            wu_t = wu[l, :, pl.ds(col, DM)]
            wd_t = wd[l, pl.ds(col, DM), :]
            pre = mm(nm[...], wu_t) + upb[l, :, pl.ds(col, DM)]
            cdf = 0.5 * (1.0 + lax.erf(pre * 0.7071067811865476))
            act = (pre * cdf).astype(BF)
            if fwd:
                acc[...] += mm(act, wd_t)
            if dout is not None:
                slope = cdf + pre * (0.3989422804014327 * jnp.exp(-0.5 * pre * pre))
                gt = mm_tn(act, dout[...])
                t4 = lax.div(t, 2)
                for i in range(2):
                    gd[t4, lax.rem(t, 2), i] = gt[256 * i:256 * i + 256].reshape(2, LN, DM)
                dpre = mm_nt(dout[...], wd_t).astype(BF).astype(F32) * slope
                gub[0:1, pl.ds(col, DM)] = jnp.sum(dpre, axis=0, keepdims=True)
                dpb = dpre.astype(BF)
                gu[:, :, :, :, :, pl.ds(col, DM)] = mm(nmt[...], dpb).reshape(2, 2, 2, 2, SH, DM)
                dnm[...] += mm_nt(dpb, wu_t)
            return carry

        lax.fori_loop(0, 4, body, 0)

    def attn_grads(l, dout):
        ga[:, :, :, :, :, Q3:FF] = mm_tn(ctx[...], dout[...]).reshape(2, 2, 2, 2, SH, DM)
        for t in range(3):
            cols = slice(DM * t, DM * t + DM)
            ga[:, :, :, :, :, cols] = mm(nat[...], dqkv[:, cols]).reshape(2, 2, 2, 2, SH, DM)

    def layer_end(h_ref, l, dout):
        dna = mm_nt(dqkv[...], wa[l, :, 0:Q3]).astype(BF).astype(F32)
        dnm32 = dnm[...].astype(BF).astype(F32)
        xhat, rstd = normed(h_ref[...], l)
        d32 = dout[...].astype(F32)
        gvec[0:1, :] = jnp.sum(dna * xhat, axis=0, keepdims=True)
        gvec[1:2, :] = jnp.sum(dna, axis=0, keepdims=True)
        gvec[2:3, :] = jnp.sum(d32, axis=0, keepdims=True)
        gvec[3:4, :] = jnp.sum(dnm32 * xhat, axis=0, keepdims=True)
        gvec[4:5, :] = jnp.sum(dnm32, axis=0, keepdims=True)
        gvec[5:6, :] = gvec[2:3, :]
        dx = dna * vec[l, 0:1, :] + dnm32 * vec[l, 3:4, :]
        dhid = rstd * (dx - jnp.mean(dx, axis=-1, keepdims=True) - xhat * jnp.mean(dx * xhat, axis=-1, keepdims=True))
        return (d32 + dhid).astype(BF)

    def small_grads(l):
        for d in range(ND):
            gs[l, d] = jnp.zeros((8, LN), F32)
            gs[l, d, 0:6, 0:SH] = gvec[0:6, SH * d:SH * d + SH]
            gs[l, d, 6:7, :] = gub[0:1, LN * d:LN * d + LN]
            for lo, col, n in bias_parts(d):
                gs[l, d, 7:8, lo:lo + n] = gqb[0:1, col:col + n]

    def bias_parts(d):
        base = HD * (d // 2)
        if d % 2 == 0:
            return ((0, base, HD), (HD, DM + base, SH))
        return ((0, DM + base + SH, SH), (SH, 1024 + base, HD))

    def peer(i):
        t = lax.rem(me + i, ND)
        return t, (lax.div(t, 8), lax.rem(t, 8))

    def small_send(l):
        def body(i, carry):
            t, to = peer(i)
            pltpu.make_async_remote_copy(src_ref=gs.at[l, t], dst_ref=gr.at[l, me], send_sem=gr_send.at[l],
                                         recv_sem=gr_recv.at[l], device_id=to, device_id_type=MESH).start()
            return carry
        lax.fori_loop(1, ND, body, 0)
        gr[l, me] = gs[l, me]

    def small_finish(l):
        whole = pltpu.make_async_remote_copy(src_ref=gs.at[l, pl.ds(0, ND - 1)], dst_ref=gr.at[l, pl.ds(0, ND - 1)],
                                             send_sem=gr_send.at[l], recv_sem=gr_recv.at[l],
                                             device_id=dev(chip, other), device_id_type=MESH)
        whole.wait_send()
        whole.wait_recv()
        total = gr[l, 0]
        for d in range(1, ND):
            total = total + gr[l, d]
        os_ref[l] = total

    local = []
    for w, src in enumerate((wa_in, wu_in, wd_in)):
        for l in range(LAYERS):
            cp = pltpu.make_async_copy(src.at[l], block(l, w, chip, core), loc_sem.at[l, w])
            cp.start()
            local.append(cp)
    cp = pltpu.make_async_copy(small_in, smalls.at[me], loc_sem.at[0, 3])
    cp.start()
    local.append(cp)
    for cp in local:
        cp.wait()

    def send_small(i, carry):
        t, to = peer(i)
        pltpu.make_async_remote_copy(src_ref=smalls.at[me], dst_ref=smalls.at[me], send_sem=sm_send,
                                     recv_sem=sm_recv, device_id=to, device_id_type=MESH).start()
        return carry

    groups = (AO, UP, DN)
    for w in groups:
        ag0(0, w)
    lax.fori_loop(1, ND, send_small, 0)
    for w in groups:
        ag1(0, w)
    whole = pltpu.make_async_remote_copy(src_ref=smalls.at[pl.ds(0, ND - 1)], dst_ref=smalls.at[pl.ds(0, ND - 1)],
                                         send_sem=sm_send, recv_sem=sm_recv, device_id=dev(chip, other),
                                         device_id_type=MESH)
    whole.wait_send()
    whole.wait_recv()
    for l in range(LAYERS):
        for d in range(ND):
            vec[l, 0:6, SH * d:SH * d + SH] = smalls[d, l, 0:6, 0:SH]
            upb[l, 0:1, LN * d:LN * d + LN] = smalls[d, l, 6:7, :]
            for lo, col, n in bias_parts(d):
                qkvb[l, 0:1, col:col + n] = smalls[d, l, 7:8, lo:lo + n]
    norms(x_ref, 0, False)
    for w in groups:
        ag2(0, w)
    for w in groups:
        ag0(1, w)
    for w in groups:
        ag3(0, w)
    for w in groups:
        ag1(1, w)
    got_partner(0, AO)
    make_qkv(0)
    heads(0, False)
    for w in groups:
        ag2(1, w)
    got_partner(0, UP)
    got_partner(0, DN)
    mlp(0, None, True)
    acc[...] += mm(ctx[...], wa[0, :, Q3:FF])
    h1[...] = (x_ref[...].astype(F32) + acc[...] + vec[0, 2:3, :] + vec[0, 5:6, :]).astype(BF)

    norms(h1, 1, True)
    ag3(1, UP)
    ag3(1, DN)
    got_partner(1, UP)
    got_partner(1, DN)
    mlp(1, cot_ref, True)
    s0(1, DN)
    s0(1, UP)
    ag3(1, AO)
    got_partner(1, AO)
    make_qkv(1)
    dctx[...] = mm_nt(cot_ref[...], wa[1, :, Q3:FF]).astype(BF)
    s1(1, DN)
    s1(1, UP)
    heads(1, True)
    attn_grads(1, cot_ref)
    s0(1, AO)
    acc[...] += mm(ctx[...], wa[1, :, Q3:FF])
    y_ref[...] = (h1[...].astype(F32) + acc[...] + vec[1, 2:3, :] + vec[1, 5:6, :]).astype(BF)
    dh[...] = layer_end(h1, 1, cot_ref)
    small_grads(1)
    small_send(1)
    s1(1, AO)

    norms(x_ref, 0, True)
    rs[1, DN, 0].wait_send()
    rs[1, UP, 0].wait_send()
    mlp(0, dh, False)
    s0(0, DN)
    s0(0, UP)
    make_qkv(0)
    dctx[...] = mm_nt(dh[...], wa[0, :, Q3:FF]).astype(BF)
    s1(0, DN)
    s1(0, UP)
    heads(0, True)
    rs[1, AO, 0].wait_send()
    attn_grads(0, dh)
    s0(0, AO)
    xg_ref[...] = layer_end(x_ref, 0, dh)
    small_grads(0)
    small_send(0)
    s1(0, AO)
    order = ((1, DN), (1, UP), (1, AO), (0, DN), (0, UP), (0, AO))
    for l, w in order:
        s2(l, w)
    for l, w in order:
        s3(l, w)
    for l, w in order:
        s4(l, w)
    small_finish(1)
    small_finish(0)
    for w in groups:
        rs[0, w, 0].wait_send()
        for l in range(LAYERS):
            for stage in range(1, 4):
                rs[l, w, stage].wait_send()
    for cp in pend:
        cp.wait_send()


def rope_constants():
    rot, half, hd = 16, 8, HD
    inv = (1.0 / (10000.0 ** (np.arange(0, rot, 2, dtype=np.float32) / np.float32(rot)))).astype(np.float32)
    ang = np.arange(SEQ, dtype=np.float32)[:, None] * inv[None, :]
    cos, sin = np.cos(ang).astype(np.float32), np.sin(ang).astype(np.float32)
    c = np.ones((SEQ, LN), np.float32)
    p = np.zeros((SEQ, LN), np.float32)
    q = np.zeros((SEQ, LN), np.float32)
    for base in (0, hd):
        c[:, base:base + half] = cos
        c[:, base + half:base + rot] = cos
        p[:, base:base + half] = -sin
        q[:, base + half:base + rot] = sin
    return c, p, q


def solution(mesh):
    shard_axes = ('node', 'local')
    act_spec = P(shard_axes)
    param_spec = P(None, shard_axes)
    consts = rope_constants()
    vm = pl.BlockSpec(memory_space=pltpu.VMEM)
    hbm = pl.BlockSpec(memory_space=pl.ANY)

    def device_step(x, y_cot, g1, b1, wqkv, bqkv, wout, bout, g2, b2, wup, bup, wdn, bdn):
        qkv_cols = wqkv.reshape(LAYERS, SH, 8, 3, HD).transpose(0, 1, 3, 2, 4).reshape(LAYERS, SH, Q3)
        wa = jnp.concatenate([qkv_cols, wout], axis=-1)
        small = jnp.stack([jnp.pad(v, ((0, 0), (0, LN - v.shape[1])))
                           for v in (g1, b1, bout, g2, b2, bdn, bup, bqkv)], axis=1).astype(F32)

        def v(shape, dt):
            return pltpu.VMEM(shape, dt)

        wshape = [(LAYERS, ND * ROWS[w], COLS[w]) for w in range(3)]
        scratch = [v(wshape[w], BF) for w in range(3)]
        scratch += [v((2, 2, 2, 2, ROWS[w], COLS[w]), F32) for w in range(3)]
        for lead in ((2, 2, 2), (2, 2), (2,), ()):
            scratch += [v((LAYERS,) + lead + (ROWS[w], COLS[w]), F32) for w in range(3)]
        scratch += [v((ND, LAYERS, 8, LN), F32), v((LAYERS, 8, DM), F32), v((LAYERS, 1, FF), F32),
                    v((LAYERS, 1, 3 * DM), F32), v((LAYERS, ND, 8, LN), F32), v((LAYERS, ND, 8, LN), F32),
                    v((8, DM), F32), v((1, FF), F32), v((1, 3 * DM), F32)]
        scratch += [v((SEQ, DM), BF), v((SEQ, DM), BF), v((SEQ, DM), BF), v((SEQ, DM), BF),
                    v((DM, SEQ), BF), v((DM, SEQ), BF), v((SEQ, 3 * DM), BF), v((SEQ, 3 * DM), BF),
                    v((SEQ, DM), BF), v((SEQ, DM), BF), v((SEQ, DM), F32), v((SEQ, DM), F32)]
        dma = pltpu.SemaphoreType.DMA
        scratch += [dma((LAYERS, 4)), dma((LAYERS, 3, 15)), dma((LAYERS, 3, 8)), dma((LAYERS, 3, 8)),
                    dma((LAYERS, 3, 4)), dma((LAYERS, 3, 4)), dma, dma, dma((LAYERS,)), dma((LAYERS,))]
        sds = jax.ShapeDtypeStruct
        y, xg, oa, ou, od, osm = pl.pallas_call(
            kernel,
            out_shape=[sds((SEQ, DM), BF), sds((SEQ, DM), BF), sds((LAYERS, SH, FF), BF),
                       sds((LAYERS, SH, FF), BF), sds((LAYERS, LN, DM), BF), sds((LAYERS, 8, LN), F32)],
            in_specs=[vm, vm, hbm, hbm, hbm, hbm, vm, vm, vm],
            out_specs=[vm] * 6,
            scratch_shapes=scratch,
            compiler_params=pltpu.CompilerParams(has_side_effects=True, vmem_limit_bytes=67043328),
            name='step',
        )(x[0], y_cot[0], wa, wup, wdn, small, *consts)
        gqkv = oa[:, :, :Q3].reshape(LAYERS, SH, 3, 8, HD).transpose(0, 1, 3, 2, 4).reshape(LAYERS, SH, 8, 192)
        sm = osm.astype(BF)
        return (y[None], xg[None], sm[:, 0, :SH], sm[:, 1, :SH], gqkv, sm[:, 7, :96], oa[:, :, Q3:], sm[:, 2, :SH],
                sm[:, 3, :SH], sm[:, 4, :SH], ou, sm[:, 6, :], od, sm[:, 5, :SH])

    return jax.shard_map(device_step, mesh=mesh,
                         in_specs=(act_spec, act_spec) + (param_spec,) * 12,
                         out_specs=(act_spec, act_spec) + (param_spec,) * 12,
                         check_vma=False)
```

```python
import numpy as np
import jax
import jax.numpy as jnp
from jax import lax
from jax.experimental import pallas as pl
from jax.experimental.pallas import tpu as pltpu
from jax.sharding import PartitionSpec as P

BF, F32 = jnp.bfloat16, jnp.float32
MESH = pl.DeviceIdType.MESH
EPSILON = 1e-5
LAYERS, SEQ, DM, FF, ND = 2, 256, 512, 2048, 16
SH, HD, LN, Q3 = 32, 64, 128, 1536
ROWS = (SH, SH, LN)
COLS = (FF, FF, DM)
AO, UP, DN = 0, 1, 2
ORDERS = ((1, 2, 4), (2, 4, 1), (4, 1, 2))
CHIP_AXES = [4, 2, 1]
HALVES = ((UP, 0), (UP, 1), (DN, 0), (DN, 1), (AO, 0), (AO, 1))
UP0, UP1, DN0, DN1, AO0, AO1 = range(6)


def bit(v, a):
    return lax.rem(lax.div(v, a), 2)


def flip(v, mask):
    for a in (1, 2, 4):
        if mask & a:
            v = v + a - 2 * a * bit(v, a)
    return v


def mm(a, b):
    return jnp.dot(a, b, preferred_element_type=F32)


def mm_nt(a, b):
    return lax.dot_general(a, b, (((1,), (1,)), ((), ())), preferred_element_type=F32)


def mm_tn(a, b):
    return lax.dot_general(a, b, (((0,), (0,)), ((), ())), preferred_element_type=F32)


def kernel(x_ref, cot_ref, wq_in, wo_in, wu_in, wd_in, p0, p1, p2, p3, p4, p5, p6, p7, rc_ref, r1_ref, r2_ref,
           y_ref, xg_ref, oq_ref, oo_ref, ou_ref, od_ref, os_ref,
           wa, wu, wd, ga, gu, gd, ra0, ru0, rd0, ra1, ru1, rd1, ra2, ru2, rd2, ra3, ru3, rd3,
           smalls, v0, v1, v2, v3, v4, v5, v6, v7, vec, upb, qkvb, gs, gr, gvec, gub, gqb,
           h1, dh, na, nm, nat, nmt, qkv, dqkv, ctx, dctx, acc, dnm,
           loc_sem, ag_send, ag_ici, ag_d2d, rs_send, rs_recv, sm_send, sm_recv, gr_send, gr_recv):
    me = lax.axis_index('node') * 8 + lax.axis_index('local')
    chip = lax.div(me, 2)
    core = lax.rem(me, 2)
    other = 1 - core
    W, G = (wa, wu, wd), (ga, gu, gd)
    R0, R1, R2, R3 = (ra0, ru0, rd0), (ra1, ru1, rd1), (ra2, ru2, rd2), (ra3, ru3, rd3)
    pend = []

    def dev(c, k):
        i = c * 2 + k
        return (lax.div(i, 8), lax.rem(i, 8))

    def block(l, w, c, k):
        return W[w].at[l, pl.ds(pl.multiple_of((c * 2 + k) * ROWS[w], ROWS[w]), ROWS[w])]

    counts = {}

    def ag_copy(l, w, src_mask, to, recv_sem):
        n = counts.get((l, w), 0)
        counts[(l, w)] = n + 1
        blk = block(l, w, flip(chip, src_mask), core)
        cp = pltpu.make_async_remote_copy(src_ref=blk, dst_ref=blk, send_sem=ag_send.at[l, w, n],
                                          recv_sem=recv_sem, device_id=to, device_id_type=MESH)
        cp.start()
        pend.append(cp)

    def to_link(l, w, mask, a):
        ag_copy(l, w, mask, dev(flip(chip, a), core), ag_ici.at[l, w, mask ^ a])

    def to_partner(l, w, mask):
        ag_copy(l, w, mask, dev(chip, other), ag_d2d.at[l, w, mask])

    def got(l, w, mask):
        blk = block(l, w, flip(chip, mask), core)
        pltpu.make_async_remote_copy(src_ref=blk, dst_ref=blk, send_sem=ag_send.at[l, w, 0],
                                     recv_sem=ag_ici.at[l, w, mask], device_id=dev(flip(chip, 1), core),
                                     device_id_type=MESH).wait_recv()

    def got_partner(l, w):
        for mask in range(8):
            blk = block(l, w, flip(chip, mask), other)
            pltpu.make_async_remote_copy(src_ref=blk, dst_ref=blk, send_sem=ag_send.at[l, w, 0],
                                         recv_sem=ag_d2d.at[l, w, mask], device_id=dev(chip, other),
                                         device_id_type=MESH).wait_recv()

    def ag0(l, ws):
        for i in range(3):
            for w in ws:
                to_link(l, w, 0, ORDERS[w][i])
        for w in ws:
            to_partner(l, w, 0)

    def ag1(l, ws):
        for w in ws:
            a, b, c = ORDERS[w]
            got(l, w, a)
            to_link(l, w, a, b)
        for w in ws:
            a, b, c = ORDERS[w]
            to_link(l, w, a, c)
            to_partner(l, w, a)

    def ag2(l, ws, first):
        for w in ws:
            a, b, c = ORDERS[w]
            m = b if first else a | b
            got(l, w, m)
            to_link(l, w, m, c)
            to_partner(l, w, m)

    def ag3(l, ws):
        for k in range(4):
            for w in ws:
                a, b, c = ORDERS[w]
                m = (c, a | c, b | c, 7)[k]
                got(l, w, m)
                to_partner(l, w, m)

    rs = {}

    def rs_copy(l, g, stage, src, dst, to):
        cp = pltpu.make_async_remote_copy(src_ref=src, dst_ref=dst, send_sem=rs_send.at[l, g, stage],
                                          recv_sem=rs_recv.at[l, g, stage], device_id=to, device_id_type=MESH)
        cp.start()
        rs[l, g, stage] = cp

    def half(g):
        w, h = HALVES[g]
        n = COLS[w] // 2
        return w, ORDERS[g % 3], slice(n * h, n * h + n)

    def pick(axes, a, v):
        return tuple(v if m == a else slice(None) for m in axes)

    def s0(l, g):
        w, _, cs = half(g)
        rs_copy(l, g, 0, G[w].at[:, :, :, other, :, cs], R0[w].at[l, :, :, :, :, cs], dev(chip, other))

    def s1(l, g):
        w, (a, b, c), cs = half(g)
        rs[l, g, 0].wait_recv()
        for z in range(2):
            for y in range(2):
                for x in range(2):
                    R0[w][l, z, y, x, :, cs] = R0[w][l, z, y, x, :, cs] + G[w][z, y, x, core, :, cs]
        src = R0[w].at[(l,) + pick(CHIP_AXES, a, 1 - bit(chip, a)) + (slice(None), cs)]
        rs_copy(l, g, 1, src, R1[w].at[l, :, :, :, cs], dev(flip(chip, a), core))

    def s2(l, g):
        w, (a, b, c), cs = half(g)
        rs[l, g, 1].wait_recv()
        left = [m for m in CHIP_AXES if m != a]
        for i in range(2):
            for j in range(2):
                idx = [i, j]
                idx.insert(CHIP_AXES.index(a), bit(chip, a))
                R1[w][l, i, j, :, cs] = R1[w][l, i, j, :, cs] + R0[w][(l,) + tuple(idx) + (slice(None), cs)]
        src = R1[w].at[(l,) + pick(left, b, 1 - bit(chip, b)) + (slice(None), cs)]
        rs_copy(l, g, 2, src, R2[w].at[l, :, :, cs], dev(flip(chip, b), core))

    def s3(l, g):
        w, (a, b, c), cs = half(g)
        rs[l, g, 2].wait_recv()
        left = [m for m in CHIP_AXES if m != a]
        for i in range(2):
            idx = [i]
            idx.insert(left.index(b), bit(chip, b))
            R2[w][l, i, :, cs] = R2[w][l, i, :, cs] + R1[w][(l,) + tuple(idx) + (slice(None), cs)]
        rs_copy(l, g, 3, R2[w].at[l, 1 - bit(chip, c), :, cs], R3[w].at[l, :, cs], dev(flip(chip, c), core))

    def s4(l, g):
        w, (a, b, c), cs = half(g)
        rs[l, g, 3].wait_recv()
        total = (R3[w][l, :, cs] + R2[w][l, bit(chip, c), :, cs]).astype(BF)
        if g == AO1:
            oq_ref[l, :, 2 * DM:] = total[:, :DM]
            oo_ref[l] = total[:, DM:]
        elif g == AO0:
            oq_ref[l, :, cs] = total
        else:
            (None, ou_ref, od_ref)[w][l, :, cs] = total

    def normed(h_bf, l):
        h32 = h_bf.astype(F32)
        cen = h32 - jnp.mean(h32, axis=-1, keepdims=True)
        rstd = lax.rsqrt(jnp.mean(cen * cen, axis=-1, keepdims=True) + EPSILON)
        return cen * rstd, rstd

    def norms(h_ref, l, bwd):
        xhat, _ = normed(h_ref[...], l)
        n1 = (xhat * vec[l, 0:1, :] + vec[l, 1:2, :]).astype(BF)
        n2 = (xhat * vec[l, 3:4, :] + vec[l, 4:5, :]).astype(BF)
        na[...] = n1
        nm[...] = n2
        if bwd:
            nat[...] = n1.T
            nmt[...] = n2.T

    def rope(xs, back):
        c, p, q = rc_ref[...], r1_ref[...], r2_ref[...]
        if back:
            return xs * c + pltpu.roll(xs * p, 8, 1) + pltpu.roll(xs * q, 120, 1)
        return xs * c + pltpu.roll(xs, 120, 1) * p + pltpu.roll(xs, 8, 1) * q

    def make_qkv(l):
        for t in range(3):
            cols = slice(DM * t, DM * t + DM)
            raw = mm(na[...], wa[l, :, cols]) + qkvb[l, :, cols]
            for s in range(4):
                part = raw[:, LN * s:LN * s + LN]
                if t < 2:
                    part = rope(part, False)
                qkv[:, DM * t + LN * s:DM * t + LN * s + LN] = part.astype(BF)

    def heads(l, bwd):
        lane = lax.broadcasted_iota(jnp.int32, (1, LN), 1)
        masks = [(lane < HD).astype(F32).astype(BF), (lane >= HD).astype(F32).astype(BF)]
        causal = (lax.broadcasted_iota(jnp.int32, (SEQ, SEQ), 0) >= lax.broadcasted_iota(jnp.int32, (SEQ, SEQ), 1))

        def body(j, carry):
            col = pl.multiple_of(j * LN, LN)
            q, k, v = (qkv[:, pl.ds(col + DM * t, LN)] for t in range(3))
            ctx_sum = jnp.zeros((SEQ, LN), F32)
            if bwd:
                dc = dctx[:, pl.ds(col, LN)]
                dq = jnp.zeros((SEQ, LN), F32)
                dk = jnp.zeros((SEQ, LN), F32)
                dv = jnp.zeros((SEQ, LN), F32)
            for mask in masks:
                qm = q * mask
                sc = jnp.where(causal, mm_nt(qm, k) * 0.125, -1e30)
                e = jnp.exp(sc - jnp.max(sc, axis=-1, keepdims=True))
                p = e / jnp.sum(e, axis=-1, keepdims=True)
                pb = p.astype(BF)
                ctx_sum = ctx_sum + mm(pb, v * mask)
                if bwd:
                    dcm = dc * mask
                    dp = mm_nt(dcm, v).astype(BF).astype(F32)
                    dv = dv + mm_tn(pb, dcm)
                    ds = (p * (dp - jnp.sum(dp * p, axis=-1, keepdims=True)) * 0.125).astype(BF)
                    dq = dq + mm(ds, k * mask)
                    dk = dk + mm_tn(ds, qm)
            ctx[:, pl.ds(col, LN)] = ctx_sum.astype(BF)
            if bwd:
                for t, d in enumerate((dq, dk, dv)):
                    d = d.astype(BF).astype(F32)
                    if t < 2:
                        d = rope(d, True)
                    gqb[0:1, pl.ds(col + DM * t, LN)] = jnp.sum(d, axis=0, keepdims=True)
                    dqkv[:, pl.ds(col + DM * t, LN)] = d.astype(BF)
            return carry

        lax.fori_loop(0, 4, body, 0)

    def mlp(l, dout, fwd, middle):
        if fwd:
            acc[...] = jnp.zeros_like(acc)
        if dout is not None:
            dnm[...] = jnp.zeros_like(dnm)

        def body(t, carry):
            col = pl.multiple_of(t * DM, DM)
            wu_t = wu[l, :, pl.ds(col, DM)]
            wd_t = wd[l, pl.ds(col, DM), :]
            pre = mm(nm[...], wu_t) + upb[l, :, pl.ds(col, DM)]
            cdf = 0.5 * (1.0 + lax.erf(pre * 0.7071067811865476))
            act = (pre * cdf).astype(BF)
            if fwd:
                acc[...] += mm(act, wd_t)
            if dout is not None:
                slope = cdf + pre * (0.3989422804014327 * jnp.exp(-0.5 * pre * pre))
                gt = mm_tn(act, dout[...])
                t4 = lax.div(t, 2)
                for i in range(2):
                    gd[t4, lax.rem(t, 2), i] = gt[256 * i:256 * i + 256].reshape(2, LN, DM)
                dpre = mm_nt(dout[...], wd_t).astype(BF).astype(F32) * slope
                gub[0:1, pl.ds(col, DM)] = jnp.sum(dpre, axis=0, keepdims=True)
                dpb = dpre.astype(BF)
                gu[:, :, :, :, :, pl.ds(col, DM)] = mm(nmt[...], dpb).reshape(2, 2, 2, 2, SH, DM)
                dnm[...] += mm_nt(dpb, wu_t)
            return carry

        lax.fori_loop(0, 2, body, 0)
        middle()
        lax.fori_loop(2, 4, body, 0)

    def attn_grads(l, dout):
        ga[:, :, :, :, :, Q3:] = mm_tn(ctx[...], dout[...]).reshape(2, 2, 2, 2, SH, DM)
        for t in (2, 0, 1):
            cols = slice(DM * t, DM * t + DM)
            ga[:, :, :, :, :, cols] = mm(nat[...], dqkv[:, cols]).reshape(2, 2, 2, 2, SH, DM)
            if t == 2:
                s0(l, AO1)
        s0(l, AO0)

    def layer_end(h_ref, l, dout):
        dna = mm_nt(dqkv[...], wa[l, :, 0:Q3]).astype(BF).astype(F32)
        dnm32 = dnm[...].astype(BF).astype(F32)
        xhat, rstd = normed(h_ref[...], l)
        d32 = dout[...].astype(F32)
        gvec[0:1, :] = jnp.sum(dna * xhat, axis=0, keepdims=True)
        gvec[1:2, :] = jnp.sum(dna, axis=0, keepdims=True)
        gvec[2:3, :] = jnp.sum(d32, axis=0, keepdims=True)
        gvec[3:4, :] = jnp.sum(dnm32 * xhat, axis=0, keepdims=True)
        gvec[4:5, :] = jnp.sum(dnm32, axis=0, keepdims=True)
        gvec[5:6, :] = gvec[2:3, :]
        dx = dna * vec[l, 0:1, :] + dnm32 * vec[l, 3:4, :]
        dhid = rstd * (dx - jnp.mean(dx, axis=-1, keepdims=True) - xhat * jnp.mean(dx * xhat, axis=-1, keepdims=True))
        return (d32 + dhid).astype(BF)

    def small_grads(l):
        for d in range(ND):
            gs[l, d] = jnp.zeros((8, LN), F32)
            gs[l, d, 0:6, 0:SH] = gvec[0:6, SH * d:SH * d + SH]
            gs[l, d, 6:7, :] = gub[0:1, LN * d:LN * d + LN]
            for lo, col, n in bias_parts(d):
                gs[l, d, 7:8, lo:lo + n] = gqb[0:1, col:col + n]

    def bias_parts(d):
        base = HD * (d // 2)
        if d % 2 == 0:
            return ((0, base, HD), (HD, DM + base, SH))
        return ((0, DM + base + SH, SH), (SH, 1024 + base, HD))

    def peer(i):
        t = lax.rem(me + i, ND)
        return t, (lax.div(t, 8), lax.rem(t, 8))

    def small_send(l):
        def body(i, carry):
            t, to = peer(i)
            pltpu.make_async_remote_copy(src_ref=gs.at[l, t], dst_ref=gr.at[l, me], send_sem=gr_send.at[l],
                                         recv_sem=gr_recv.at[l], device_id=to, device_id_type=MESH).start()
            return carry
        lax.fori_loop(1, ND, body, 0)
        gr[l, me] = gs[l, me]

    def small_finish(l):
        whole = pltpu.make_async_remote_copy(src_ref=gs.at[l, pl.ds(0, ND - 1)], dst_ref=gr.at[l, pl.ds(0, ND - 1)],
                                             send_sem=gr_send.at[l], recv_sem=gr_recv.at[l],
                                             device_id=dev(chip, other), device_id_type=MESH)
        whole.wait_send()
        whole.wait_recv()
        total = gr[l, 0]
        for d in range(1, ND):
            total = total + gr[l, d]
        os_ref[l] = total

    def place(l):
        cps = []
        qo = pl.multiple_of(me * SH, SH)
        pairs = [(wq_in, W[AO].at[l, pl.ds(qo, SH), pl.ds(0, Q3)]), (wo_in, W[AO].at[l, pl.ds(qo, SH), pl.ds(Q3, DM)]),
                 (wu_in, block(l, UP, chip, core)), (wd_in, block(l, DN, chip, core))]
        for i, (src, dst) in enumerate(pairs):
            cps.append(pltpu.make_async_copy(src.at[l], dst, loc_sem.at[l, i]))
        for cp in cps:
            cp.start()
        return cps

    first, second = place(0), place(1)
    params, tmp = (p0, p1, p2, p3, p4, p5, p6, p7), (v0, v1, v2, v3, v4, v5, v6, v7)
    little = [pltpu.make_async_copy(params[i], tmp[i], loc_sem.at[2 + i // 4, i % 4]) for i in range(8)]
    for cp in little:
        cp.start()

    def send_small(i, carry):
        t, to = peer(i)
        pltpu.make_async_remote_copy(src_ref=smalls.at[me], dst_ref=smalls.at[me], send_sem=sm_send,
                                     recv_sem=sm_recv, device_id=to, device_id_type=MESH).start()
        return carry

    groups = (UP, DN, AO)
    for cp in first:
        cp.wait()
    ag0(0, groups)
    for i in range(8):
        little[i].wait()
        for l in range(LAYERS):
            smalls[me, l, i:i + 1, 0:tmp[i].shape[1]] = tmp[i][l:l + 1, :].astype(F32)
    lax.fori_loop(1, ND, send_small, 0)
    for cp in second:
        cp.wait()
    ag1(0, groups)
    whole = pltpu.make_async_remote_copy(src_ref=smalls.at[pl.ds(0, ND - 1)], dst_ref=smalls.at[pl.ds(0, ND - 1)],
                                         send_sem=sm_send, recv_sem=sm_recv, device_id=dev(chip, other),
                                         device_id_type=MESH)
    whole.wait_send()
    whole.wait_recv()
    ag2(0, groups, True)
    for l in range(LAYERS):
        for d in range(ND):
            vec[l, 0:6, SH * d:SH * d + SH] = smalls[d, l, 0:6, 0:SH]
            upb[l, 0:1, LN * d:LN * d + LN] = smalls[d, l, 6:7, :]
            for lo, col, n in bias_parts(d):
                qkvb[l, 0:1, col:col + n] = smalls[d, l, 7:8, lo:lo + n]
    norms(x_ref, 0, False)
    ag2(0, groups, False)
    ag0(1, groups)
    ag3(0, (AO, UP, DN))
    got_partner(0, AO)
    make_qkv(0)
    ag1(1, groups)
    heads(0, False)
    ag2(1, groups, True)
    got_partner(0, UP)
    got_partner(0, DN)
    mlp(0, None, True, lambda: None)
    ag2(1, groups, False)
    acc[...] += mm(ctx[...], wa[0, :, Q3:])
    h1[...] = (x_ref[...].astype(F32) + acc[...] + vec[0, 2:3, :] + vec[0, 5:6, :]).astype(BF)

    norms(h1, 1, True)
    ag3(1, groups)
    got_partner(1, UP)
    got_partner(1, DN)
    mlp(1, cot_ref, True, lambda: s0(1, UP0))
    for g in (UP1, DN0, DN1):
        s0(1, g)
    s1(1, UP0)
    got_partner(1, AO)
    make_qkv(1)
    dctx[...] = mm_nt(cot_ref[...], wa[1, :, Q3:]).astype(BF)
    for g in (UP1, DN0, DN1):
        s1(1, g)
    heads(1, True)
    attn_grads(1, cot_ref)
    acc[...] += mm(ctx[...], wa[1, :, Q3:])
    y_ref[...] = (h1[...].astype(F32) + acc[...] + vec[1, 2:3, :] + vec[1, 5:6, :]).astype(BF)
    s1(1, AO1)
    s1(1, AO0)
    dh[...] = layer_end(h1, 1, cot_ref)
    small_grads(1)
    small_send(1)

    norms(x_ref, 0, True)
    for g in (UP0, UP1, DN0, DN1):
        rs[1, g, 0].wait_send()
    mlp(0, dh, False, lambda: s0(0, UP0))
    for g in (UP1, DN0, DN1):
        s0(0, g)
    s1(0, UP0)
    for g in (UP0, UP1, DN0):
        s2(1, g)
    make_qkv(0)
    dctx[...] = mm_nt(dh[...], wa[0, :, Q3:]).astype(BF)
    for g in (UP1, DN0, DN1):
        s1(0, g)
    heads(0, True)
    s2(1, DN1)
    for g in (AO0, AO1):
        rs[1, g, 0].wait_send()
    attn_grads(0, dh)
    xg_ref[...] = layer_end(x_ref, 0, dh)
    s1(0, AO1)
    s1(0, AO0)
    small_grads(0)
    small_send(0)
    mlp_halves, attn_halves = (UP0, UP1, DN0, DN1), (AO1, AO0)
    for stage, l, gs_ in ((s2, 1, attn_halves), (s3, 1, mlp_halves), (s2, 0, mlp_halves), (s3, 1, attn_halves),
                          (s2, 0, attn_halves), (s3, 0, mlp_halves), (s4, 1, mlp_halves), (s4, 1, attn_halves),
                          (s3, 0, attn_halves), (s4, 0, mlp_halves), (s4, 0, attn_halves)):
        for g in gs_:
            stage(l, g)
    small_finish(1)
    small_finish(0)
    for g in range(6):
        rs[0, g, 0].wait_send()
        for l in range(LAYERS):
            for stage in range(1, 4):
                rs[l, g, stage].wait_send()
    for cp in pend:
        cp.wait_send()


def finish(y, xg, oo, ou, od, osm, *outs):
    yo, xo, g1, b1, bq, go, bo, g2, b2, gup, bu, gdn, bd = outs
    yo[0] = y[...]
    xo[0] = xg[...]
    go[...] = oo[...]
    gup[...] = ou[...]
    gdn[...] = od[...]
    for row, ref in enumerate((g1, b1, bo, g2, b2, bd, bu, bq)):
        for l in range(LAYERS):
            ref[l:l + 1, :] = osm[l, row:row + 1, 0:ref.shape[1]].astype(BF)


def rope_constants():
    rot, half, hd = 16, 8, HD
    inv = (1.0 / (10000.0 ** (np.arange(0, rot, 2, dtype=np.float32) / np.float32(rot)))).astype(np.float32)
    ang = np.arange(SEQ, dtype=np.float32)[:, None] * inv[None, :]
    cos, sin = np.cos(ang).astype(np.float32), np.sin(ang).astype(np.float32)
    c = np.ones((SEQ, LN), np.float32)
    p = np.zeros((SEQ, LN), np.float32)
    q = np.zeros((SEQ, LN), np.float32)
    for base in (0, hd):
        c[:, base:base + half] = cos
        c[:, base + half:base + rot] = cos
        p[:, base:base + half] = -sin
        q[:, base + half:base + rot] = sin
    return c, p, q


def solution(mesh):
    shard_axes = ('node', 'local')
    act_spec = P(shard_axes)
    param_spec = P(None, shard_axes)
    consts = rope_constants()
    vm = pl.BlockSpec(memory_space=pltpu.VMEM)
    hbm = pl.BlockSpec(memory_space=pl.ANY)

    def device_step(x, y_cot, g1, b1, wqkv, bqkv, wout, bout, g2, b2, wup, bup, wdn, bdn):
        wq = wqkv.reshape(LAYERS, SH, 8, 3, HD).transpose(0, 1, 3, 2, 4).reshape(LAYERS, SH, Q3)
        little = (g1, b1, bout, g2, b2, bdn, bup, bqkv)

        def v(shape, dt):
            return pltpu.VMEM(shape, dt)

        wshape = [(LAYERS, ND * ROWS[w], COLS[w]) for w in range(3)]
        scratch = [v(wshape[w], BF) for w in range(3)]
        scratch += [v((2, 2, 2, 2, ROWS[w], COLS[w]), F32) for w in range(3)]
        for lead in ((2, 2, 2), (2, 2), (2,), ()):
            scratch += [v((LAYERS,) + lead + (ROWS[w], COLS[w]), F32) for w in range(3)]
        scratch += [v((ND, LAYERS, 8, LN), F32)] + [v(p.shape, BF) for p in little]
        scratch += [v((LAYERS, 8, DM), F32), v((LAYERS, 1, FF), F32),
                    v((LAYERS, 1, 3 * DM), F32), v((LAYERS, ND, 8, LN), F32), v((LAYERS, ND, 8, LN), F32),
                    v((8, DM), F32), v((1, FF), F32), v((1, 3 * DM), F32)]
        scratch += [v((SEQ, DM), BF), v((SEQ, DM), BF), v((SEQ, DM), BF), v((SEQ, DM), BF),
                    v((DM, SEQ), BF), v((DM, SEQ), BF), v((SEQ, 3 * DM), BF), v((SEQ, 3 * DM), BF),
                    v((SEQ, DM), BF), v((SEQ, DM), BF), v((SEQ, DM), F32), v((SEQ, DM), F32)]
        dma = pltpu.SemaphoreType.DMA
        scratch += [dma((4, 4)), dma((LAYERS, 3, 15)), dma((LAYERS, 3, 8)), dma((LAYERS, 3, 8)),
                    dma((LAYERS, 6, 4)), dma((LAYERS, 6, 4)), dma, dma, dma((LAYERS,)), dma((LAYERS,))]
        sds = jax.ShapeDtypeStruct
        mids = pl.pallas_call(
            kernel,
            out_shape=[sds((SEQ, DM), BF), sds((SEQ, DM), BF), sds((LAYERS, SH, Q3), BF), sds((LAYERS, SH, DM), BF),
                       sds((LAYERS, SH, FF), BF), sds((LAYERS, LN, DM), BF), sds((LAYERS, 8, LN), F32)],
            in_specs=[vm, vm] + [hbm] * 12 + [vm] * 3,
            out_specs=[vm] * 7,
            scratch_shapes=scratch,
            compiler_params=pltpu.CompilerParams(has_side_effects=True, vmem_limit_bytes=67043328),
            name='step',
        )(x[0], y_cot[0], wq, wout, wup, wdn, *little, *consts)
        y, xg, oq, oo, ou, od, osm = mids
        gqkv = oq.reshape(LAYERS, SH, 3, 8, HD).transpose(0, 1, 3, 2, 4).reshape(LAYERS, SH, 8, 3 * HD)
        like = (x, y_cot, g1, b1, bqkv, wout, bout, g2, b2, wup, bup, wdn, bdn)
        outs = pl.pallas_call(finish, out_shape=[sds(p.shape, BF) for p in like], in_specs=[vm] * 6,
                              out_specs=[vm] * 13, name='finish')(y, xg, oo, ou, od, osm)
        return tuple(outs[:4]) + (gqkv,) + tuple(outs[4:])

    return jax.shard_map(device_step, mesh=mesh,
                         in_specs=(act_spec, act_spec) + (param_spec,) * 12,
                         out_specs=(act_spec, act_spec) + (param_spec,) * 12,
                         check_vma=False)
```

```python
import numpy as np
import jax
import jax.numpy as jnp
from jax import lax
from jax.experimental import pallas as pl
from jax.experimental.pallas import tpu as pltpu
from jax.sharding import PartitionSpec as P

BF, F32 = jnp.bfloat16, jnp.float32
MESH = pl.DeviceIdType.MESH
EPSILON = 1e-5
LAYERS, SEQ, DM, FF, ND = 2, 256, 512, 2048, 16
SH, HD, LN, Q3 = 32, 64, 128, 1536
ROWS = (SH, SH, LN)
COLS = (FF, FF, DM)
AO, UP, DN = 0, 1, 2
ORDERS = ((1, 2, 4), (2, 4, 1), (4, 1, 2))
CHIP_AXES = [4, 2, 1]
CUTS = ((0, 640, 1280, FF), (0, 640, 1280, FF), (0, 48, 96, LN))
ALL, EV = slice(None), ...


def piece(w, k):
    lo, hi = CUTS[w][k], CUTS[w][k + 1]
    return (slice(lo, hi), ALL) if w == DN else (ALL, slice(lo, hi))


def bit(v, a):
    return lax.rem(lax.div(v, a), 2)


def flip(v, mask):
    for a in (1, 2, 4):
        if mask & a:
            v = v + a - 2 * a * bit(v, a)
    return v


def col_sum(v):
    return jnp.sum(v, axis=0, keepdims=True)


def row_of(f, v):
    return f(v, axis=-1, keepdims=True)


def mm(a, b):
    return jnp.dot(a, b, preferred_element_type=F32)


def mm_nt(a, b):
    return lax.dot_general(a, b, (((1,), (1,)), ((), ())), preferred_element_type=F32)


def mm_tn(a, b):
    return lax.dot_general(a, b, (((0,), (0,)), ((), ())), preferred_element_type=F32)


def kernel(x_in, cot_in, wq_in, wo_in, wu_in, wd_in, p0, p1, p2, p3, p4, p5, p6, p7, rope_in,
           y_ref, xg_ref, oq_ref, oo_ref, ou_ref, od_ref, os_ref,
           wa, wu, wd, ga, gu, gd, ra0, ru0, rd0, ra1, ru1, rd1, ra2, ru2, rd2, ra3, ru3, rd3,
           smalls, v0, v1, v2, v3, v4, v5, v6, v7, vec, upb, qkvb, gs, gr, gvec, gub, gqb,
           x_ref, cot_ref, rope_ref, native, spread, act_s, slope_s,
           h1, dh, na, nm, nat, nmt, qkv, dqkv, ctx, dctx, acc, dnm,
           loc_sem, ag_send, ag_ici, ag_d2d, rs_send, rs_recv, sm_send, sm_recv, gr_send, gr_recv):
    me = lax.axis_index('node') * 8 + lax.axis_index('local')
    chip = lax.div(me, 2)
    core = lax.rem(me, 2)
    other = 1 - core
    W, G = (wa, wu, wd), (ga, gu, gd)
    R0, R1, R2, R3 = (ra0, ru0, rd0), (ra1, ru1, rd1), (ra2, ru2, rd2), (ra3, ru3, rd3)

    def dev(c, k):
        i = c * 2 + k
        return (lax.div(i, 8), lax.rem(i, 8))

    def block(l, w, c, k):
        return W[w].at[l, pl.ds(pl.multiple_of((c * 2 + k) * ROWS[w], ROWS[w]), ROWS[w])]

    def part(l, w, k, mask):
        base = (flip(chip, mask) * 2 + core) * ROWS[w]
        rs_, cs = piece(w, k)
        if w == DN:
            n = rs_.stop - rs_.start
            return W[w].at[l, pl.ds(pl.multiple_of(base + rs_.start, 16), n)]
        return W[w].at[l, pl.ds(pl.multiple_of(base, SH), SH), cs]

    def push(l, w, src, to, recv_sem):
        pltpu.make_async_remote_copy(src_ref=src, dst_ref=src, send_sem=ag_send.at[l, w], recv_sem=recv_sem,
                                     device_id=to, device_id_type=MESH).start()

    def to_link(l, w, k, mask, a):
        push(l, w, part(l, w, k, mask), dev(flip(chip, a), core), ag_ici.at[l, w, k, mask ^ a])

    def to_partner(l, w, k, mask):
        push(l, w, part(l, w, k, mask), dev(chip, other), ag_d2d.at[l, w])

    def await_in(l, w, src, recv_sem):
        pltpu.make_async_remote_copy(src_ref=src, dst_ref=src, send_sem=ag_send.at[l, w], recv_sem=recv_sem,
                                     device_id=dev(chip, other), device_id_type=MESH).wait_recv()

    def got(l, w, k, mask):
        await_in(l, w, part(l, w, k, mask), ag_ici.at[l, w, k, mask])

    def got_partner(l, w):
        await_in(l, w, W[w].at[l, pl.ds(0, 8 * ROWS[w])], ag_d2d.at[l, w])

    def sent(l, w):
        src = W[w].at[l, pl.ds(0, 15 * ROWS[w])]
        pltpu.make_async_remote_copy(src_ref=src, dst_ref=src, send_sem=ag_send.at[l, w], recv_sem=ag_d2d.at[l, w],
                                     device_id=dev(chip, other), device_id_type=MESH).wait_send()

    def own(l, w):
        for i in range(3):
            for k in range(3):
                to_link(l, w, k, 0, ORDERS[k][i])
        push(l, w, block(l, w, chip, core), dev(chip, other), ag_d2d.at[l, w])

    def f1(l, w):
        for k, (a, b, c) in enumerate(ORDERS):
            got(l, w, k, a)
            to_link(l, w, k, a, b)
        for k, (a, b, c) in enumerate(ORDERS):
            to_link(l, w, k, a, c)
            to_partner(l, w, k, a)

    def f2(l, w):
        for k, (a, b, c) in enumerate(ORDERS):
            got(l, w, k, b)
            to_link(l, w, k, b, c)
            to_partner(l, w, k, b)

    def f3(l, w):
        for k, (a, b, c) in enumerate(ORDERS):
            got(l, w, k, a | b)
            to_link(l, w, k, a | b, c)
            to_partner(l, w, k, a | b)

    def f4(l, w):
        for i in range(4):
            for k, (a, b, c) in enumerate(ORDERS):
                m = (c, a | c, b | c, 7)[i]
                got(l, w, k, m)
                to_partner(l, w, k, m)

    rs = {}

    def rs_copy(l, w, k, stage, src, dst, to):
        cp = pltpu.make_async_remote_copy(src_ref=src, dst_ref=dst, send_sem=rs_send.at[l, w, k, stage],
                                          recv_sem=rs_recv.at[l, w, k, stage], device_id=to, device_id_type=MESH)
        cp.start()
        rs[l, w, k, stage] = cp

    def pick(axes, a, v):
        return tuple(v if m == a else ALL for m in axes)

    def drained(l, w, stage):
        for k in range(3):
            rs[l, w, k, stage].wait_send()

    def s0(l, w):
        for k in range(3):
            cut = piece(w, k)
            rs_copy(l, w, k, 0, G[w].at[(ALL, ALL, ALL, other) + cut], R0[w].at[(l, ALL, ALL, ALL) + cut],
                    dev(chip, other))

    def s1(l, w):
        for k, (a, b, c) in enumerate(ORDERS):
            cut = piece(w, k)
            rs[l, w, k, 0].wait_recv()
            for z in range(2):
                for y in range(2):
                    for x in range(2):
                        at = (l, z, y, x) + cut
                        R0[w][at] = R0[w][at] + G[w][(z, y, x, core) + cut]
            src = R0[w].at[(l,) + pick(CHIP_AXES, a, 1 - bit(chip, a)) + cut]
            rs_copy(l, w, k, 1, src, R1[w].at[(l, ALL, ALL) + cut], dev(flip(chip, a), core))

    def s2(l, w):
        for k, (a, b, c) in enumerate(ORDERS):
            cut = piece(w, k)
            rs[l, w, k, 1].wait_recv()
            left = [m for m in CHIP_AXES if m != a]
            for i in range(2):
                for j in range(2):
                    idx = [i, j]
                    idx.insert(CHIP_AXES.index(a), bit(chip, a))
                    at = (l, i, j) + cut
                    R1[w][at] = R1[w][at] + R0[w][(l,) + tuple(idx) + cut]
            src = R1[w].at[(l,) + pick(left, b, 1 - bit(chip, b)) + cut]
            rs_copy(l, w, k, 2, src, R2[w].at[(l, ALL) + cut], dev(flip(chip, b), core))

    def s3(l, w):
        for k, (a, b, c) in enumerate(ORDERS):
            cut = piece(w, k)
            rs[l, w, k, 2].wait_recv()
            left = [m for m in CHIP_AXES if m != a]
            for i in range(2):
                idx = [i]
                idx.insert(left.index(b), bit(chip, b))
                at = (l, i) + cut
                R2[w][at] = R2[w][at] + R1[w][(l,) + tuple(idx) + cut]
            rs_copy(l, w, k, 3, R2[w].at[(l, 1 - bit(chip, c)) + cut], R3[w].at[(l,) + cut], dev(flip(chip, c), core))

    def s4(l, w):
        for k, (a, b, c) in enumerate(ORDERS):
            cut = piece(w, k)
            rs[l, w, k, 3].wait_recv()
            total = (R3[w][(l,) + cut] + R2[w][(l, bit(chip, c)) + cut]).astype(BF)
            if w != AO:
                (None, ou_ref, od_ref)[w][(l,) + cut] = total
            elif k < 2:
                oq_ref[(l,) + cut] = total
            else:
                n = Q3 - cut[1].start
                oq_ref[l, :, cut[1].start:] = total[:, :n]
                oo_ref[l] = total[:, n:]

    def normed(h_bf, l):
        h32 = h_bf.astype(F32)
        cen = h32 - row_of(jnp.mean, h32)
        rstd = lax.rsqrt(row_of(jnp.mean, cen * cen) + EPSILON)
        return cen * rstd, rstd

    def norms(h_ref, l, bwd):
        xhat, _ = normed(h_ref[EV], l)
        n1 = (xhat * vec[l, 0:1, :] + vec[l, 1:2, :]).astype(BF)
        n2 = (xhat * vec[l, 3:4, :] + vec[l, 4:5, :]).astype(BF)
        na[EV] = n1
        nm[EV] = n2
        if bwd:
            nat[EV] = n1.T
            nmt[EV] = n2.T

    def rope(xs, back):
        c, p, q = rope_ref[0], rope_ref[1], rope_ref[2]
        if back:
            return xs * c + pltpu.roll(xs * p, 8, 1) + pltpu.roll(xs * q, 120, 1)
        return xs * c + pltpu.roll(xs, 120, 1) * p + pltpu.roll(xs, 8, 1) * q

    def make_qkv(l):
        for t in range(3):
            cols = slice(DM * t, DM * t + DM)
            raw = mm(na[EV], wa[l, :, cols]) + qkvb[l, :, cols]
            for s in range(4):
                part = raw[:, LN * s:LN * s + LN]
                if t < 2:
                    part = rope(part, False)
                qkv[:, DM * t + LN * s:DM * t + LN * s + LN] = part.astype(BF)

    def heads(bwd, lo, hi):
        lane = lax.broadcasted_iota(jnp.int32, (1, LN), 1)
        masks = [(lane < HD).astype(F32).astype(BF), (lane >= HD).astype(F32).astype(BF)]
        causal = (lax.broadcasted_iota(jnp.int32, (SEQ, SEQ), 0) >= lax.broadcasted_iota(jnp.int32, (SEQ, SEQ), 1))

        def body(j, carry):
            col = pl.multiple_of(j * LN, LN)
            q, k, v = (qkv[:, pl.ds(col + DM * t, LN)] for t in range(3))
            ctx_sum = jnp.zeros((SEQ, LN), F32)
            if bwd:
                dc = dctx[:, pl.ds(col, LN)]
                dq = jnp.zeros((SEQ, LN), F32)
                dk = jnp.zeros((SEQ, LN), F32)
                dv = jnp.zeros((SEQ, LN), F32)
            for mask in masks:
                qm = q * mask
                sc = jnp.where(causal, mm_nt(qm, k) * 0.125, -1e30)
                e = jnp.exp(sc - row_of(jnp.max, sc))
                p = e / row_of(jnp.sum, e)
                pb = p.astype(BF)
                ctx_sum = ctx_sum + mm(pb, v * mask)
                if bwd:
                    dcm = dc * mask
                    dp = mm_nt(dcm, v).astype(BF).astype(F32)
                    dv = dv + mm_tn(pb, dcm)
                    ds = (p * (dp - row_of(jnp.sum, dp * p)) * 0.125).astype(BF)
                    dq = dq + mm(ds, k * mask)
                    dk = dk + mm_tn(ds, qm)
            ctx[:, pl.ds(col, LN)] = ctx_sum.astype(BF)
            if bwd:
                for t, d in enumerate((dq, dk, dv)):
                    d = d.astype(BF).astype(F32)
                    if t < 2:
                        d = rope(d, True)
                    gqb[0:1, pl.ds(col + DM * t, LN)] = col_sum(d)
                    dqkv[:, pl.ds(col + DM * t, LN)] = d.astype(BF)
            return carry

        lax.fori_loop(lo, hi, body, 0)

    def up_part(l, t):
        col = pl.multiple_of(t * DM, DM)
        pre = mm(nm[EV], wu[l, :, pl.ds(col, DM)]) + upb[l, :, pl.ds(col, DM)]
        cdf = 0.5 * (1.0 + lax.erf(pre * 0.7071067811865476))
        return col, pre, cdf, (pre * cdf).astype(BF)

    def mlp_fwd(l):
        def body(t, carry):
            col, pre, cdf, act = up_part(l, t)
            acc[EV] += mm(act, wd[l, pl.ds(col, DM), :])
            return carry

        acc[EV] = jnp.zeros_like(acc)
        lax.fori_loop(0, 4, body, 0)

    def mlp_a(l, dout):
        def body(t, carry):
            col, pre, cdf, act = up_part(l, t)
            act_s[:, pl.ds(col, DM)] = act
            slope_s[:, pl.ds(col, DM)] = cdf + pre * (0.3989422804014327 * jnp.exp(-0.5 * pre * pre))
            gt = mm_tn(act, dout[EV])
            for i in range(2):
                gd[lax.div(t, 2), lax.rem(t, 2), i] = gt[SEQ * i:SEQ * i + SEQ].reshape(2, LN, DM)
            return carry

        lax.fori_loop(0, 4, body, 0)

    def mlp_b(l, dout, fwd):
        def body(t, carry):
            col = pl.multiple_of(t * DM, DM)
            wd_t = wd[l, pl.ds(col, DM), :]
            if fwd:
                acc[EV] += mm(act_s[:, pl.ds(col, DM)], wd_t)
            dpre = mm_nt(dout[EV], wd_t).astype(BF).astype(F32) * slope_s[:, pl.ds(col, DM)]
            gub[0:1, pl.ds(col, DM)] = col_sum(dpre)
            dpb = dpre.astype(BF)
            gu[:, :, :, :, :, pl.ds(col, DM)] = mm(nmt[EV], dpb).reshape(2, 2, 2, 2, SH, DM)
            dnm[EV] += mm_nt(dpb, wu[l, :, pl.ds(col, DM)])
            return carry

        if fwd:
            acc[EV] = jnp.zeros_like(acc)
        dnm[EV] = jnp.zeros_like(dnm)
        lax.fori_loop(0, 4, body, 0)

    def attn_grads(l, dout):
        ga[:, :, :, :, :, Q3:] = mm_tn(ctx[EV], dout[EV]).reshape(2, 2, 2, 2, SH, DM)
        for t in (2, 0, 1):
            cols = slice(DM * t, DM * t + DM)
            ga[:, :, :, :, :, cols] = mm(nat[EV], dqkv[:, cols]).reshape(2, 2, 2, 2, SH, DM)

    def layer_end(h_ref, l, dout):
        dna = mm_nt(dqkv[EV], wa[l, :, 0:Q3]).astype(BF).astype(F32)
        dnm32 = dnm[EV].astype(BF).astype(F32)
        xhat, rstd = normed(h_ref[EV], l)
        d32 = dout[EV].astype(F32)
        gvec[0:1, :] = col_sum(dna * xhat)
        gvec[1:2, :] = col_sum(dna)
        gvec[2:3, :] = col_sum(d32)
        gvec[3:4, :] = col_sum(dnm32 * xhat)
        gvec[4:5, :] = col_sum(dnm32)
        gvec[5:6, :] = gvec[2:3, :]
        dx = dna * vec[l, 0:1, :] + dnm32 * vec[l, 3:4, :]
        dhid = rstd * (dx - row_of(jnp.mean, dx) - xhat * row_of(jnp.mean, dx * xhat))
        return (d32 + dhid).astype(BF)

    def small_grads(l):
        for d in range(ND):
            gs[l, d] = jnp.zeros((8, LN), F32)
            gs[l, d, 0:6, 0:SH] = gvec[0:6, SH * d:SH * d + SH]
            gs[l, d, 6:7, :] = gub[0:1, LN * d:LN * d + LN]
            for lo, col, n in bias_parts(d):
                gs[l, d, 7:8, lo:lo + n] = gqb[0:1, col:col + n]

    def bias_parts(d):
        base = HD * (d // 2)
        if d % 2 == 0:
            return ((0, base, HD), (HD, DM + base, SH))
        return ((0, DM + base + SH, SH), (SH, 1024 + base, HD))

    def peer(i):
        t = lax.rem(me + i, ND)
        return t, (lax.div(t, 8), lax.rem(t, 8))

    def small_send(l):
        def body(i, carry):
            t, to = peer(i)
            pltpu.make_async_remote_copy(src_ref=gs.at[l, t], dst_ref=gr.at[l, me], send_sem=gr_send.at[l],
                                         recv_sem=gr_recv.at[l], device_id=to, device_id_type=MESH).start()
            return carry
        lax.fori_loop(1, ND, body, 0)
        gr[l, me] = gs[l, me]

    def small_finish(l):
        whole = pltpu.make_async_remote_copy(src_ref=gs.at[l, pl.ds(0, ND - 1)], dst_ref=gr.at[l, pl.ds(0, ND - 1)],
                                             send_sem=gr_send.at[l], recv_sem=gr_recv.at[l],
                                             device_id=dev(chip, other), device_id_type=MESH)
        whole.wait_send()
        whole.wait_recv()
        total = gr[l, 0]
        for d in range(1, ND):
            total = total + gr[l, d]
        os_ref[l] = total

    native_in = pltpu.make_async_copy(wq_in, native, loc_sem.at[0, 0])
    first = [pltpu.make_async_copy(wu_in.at[0], block(0, UP, chip, core), loc_sem.at[0, 1])]
    qo = pl.ds(pl.multiple_of(me * SH, SH), SH)
    rest = [pltpu.make_async_copy(wo_in.at[l], W[AO].at[l, qo, pl.ds(Q3, DM)], loc_sem.at[l + 2, 2])
            for l in range(LAYERS)]
    rest += [pltpu.make_async_copy(wd_in.at[l], block(l, DN, chip, core), loc_sem.at[l + 2, 3]) for l in range(LAYERS)]
    rest += [pltpu.make_async_copy(wu_in.at[1], block(1, UP, chip, core), loc_sem.at[0, 2]),
             pltpu.make_async_copy(x_in, x_ref, loc_sem.at[0, 3]),
             pltpu.make_async_copy(cot_in, cot_ref, loc_sem.at[1, 0]),
             pltpu.make_async_copy(rope_in, rope_ref, loc_sem.at[1, 1])]
    params, tmp = (p0, p1, p2, p3, p4, p5, p6, p7), (v0, v1, v2, v3, v4, v5, v6, v7)
    little = [pltpu.make_async_copy(params[i], tmp[i], loc_sem.at[4 + i // 4, i % 4]) for i in range(8)]
    first[0].start()
    native_in.start()
    for cp in little + rest:
        cp.start()

    barrier = pltpu.get_barrier_semaphore()

    def greet(i, carry):
        pl.semaphore_signal(barrier, inc=1, device_id=peer(i)[1], device_id_type=MESH)
        return carry

    lax.fori_loop(1, ND, greet, 0)
    first[0].wait()
    pl.semaphore_wait(barrier, ND - 1)
    own(0, UP)

    native_in.wait()
    for l in range(LAYERS):
        flat = native[l].astype(F32).reshape(SEQ, 3 * HD)
        spread[0] = flat[:, :LN]
        spread[1, :, :HD] = flat[:, LN:]
        for h in range(8):
            rows = [spread[i, pl.ds(h, SH, stride=8), :].astype(BF) for i in range(2)]
            for t in range(3):
                lo = HD * (t % 2)
                wa[l, qo, DM * t + HD * h:DM * t + HD * h + HD] = rows[t // 2][:, lo:lo + HD]
        if l == 0:
            for cp in rest:
                cp.wait()
            own(0, AO)
    for i in range(8):
        little[i].wait()
        for l in range(LAYERS):
            smalls[me, l, i:i + 1, 0:tmp[i].shape[1]] = tmp[i][l:l + 1, :].astype(F32)

    def send_small(i, carry):
        pltpu.make_async_remote_copy(src_ref=smalls.at[me], dst_ref=smalls.at[me], send_sem=sm_send,
                                     recv_sem=sm_recv, device_id=peer(i)[1], device_id_type=MESH).start()
        return carry

    lax.fori_loop(1, ND, send_small, 0)
    f1(0, UP)
    f2(0, UP)
    own(0, DN)
    f1(0, AO)
    f3(0, UP)
    f2(0, AO)
    whole = pltpu.make_async_remote_copy(src_ref=smalls.at[pl.ds(0, ND - 1)], dst_ref=smalls.at[pl.ds(0, ND - 1)],
                                         send_sem=sm_send, recv_sem=sm_recv, device_id=dev(chip, other),
                                         device_id_type=MESH)
    whole.wait_send()
    whole.wait_recv()
    for l in range(LAYERS):
        for d in range(ND):
            vec[l, 0:6, SH * d:SH * d + SH] = smalls[d, l, 0:6, 0:SH]
            upb[l, 0:1, LN * d:LN * d + LN] = smalls[d, l, 6:7, :]
            for lo, col, n in bias_parts(d):
                qkvb[l, 0:1, col:col + n] = smalls[d, l, 7:8, lo:lo + n]
    norms(x_ref, 0, False)
    f1(0, DN)
    f3(0, AO)
    f4(0, UP)
    own(1, UP)
    f2(0, DN)
    f4(0, AO)
    got_partner(0, AO)
    make_qkv(0)
    f3(0, DN)
    f1(1, UP)
    heads(False, 0, 2)
    own(1, DN)
    heads(False, 2, 4)
    f2(1, UP)
    f3(1, UP)
    f1(1, DN)
    f4(0, DN)
    got_partner(0, UP)
    got_partner(0, DN)
    mlp_fwd(0)
    f2(1, DN)
    own(1, AO)
    acc[EV] += mm(ctx[EV], wa[0, :, Q3:])
    h1[EV] = (x_ref[EV].astype(F32) + acc[EV] + vec[0, 2:3, :] + vec[0, 5:6, :]).astype(BF)
    norms(h1, 1, True)
    f3(1, DN)
    f4(1, UP)
    got_partner(1, UP)
    f1(1, AO)
    f2(1, AO)
    mlp_a(1, cot_ref)
    s0(1, DN)
    f4(1, DN)
    s1(1, DN)
    f3(1, AO)
    got_partner(1, DN)
    mlp_b(1, cot_ref, True)
    s0(1, UP)
    s1(1, UP)
    f4(1, AO)
    got_partner(1, AO)
    make_qkv(1)
    dctx[EV] = mm_nt(cot_ref[EV], wa[1, :, Q3:]).astype(BF)
    heads(True, 0, 2)
    s2(1, DN)
    heads(True, 2, 4)
    attn_grads(1, cot_ref)
    s0(1, AO)
    s2(1, UP)
    acc[EV] += mm(ctx[EV], wa[1, :, Q3:])
    y_ref[EV] = (h1[EV].astype(F32) + acc[EV] + vec[1, 2:3, :] + vec[1, 5:6, :]).astype(BF)
    dh[EV] = layer_end(h1, 1, cot_ref)
    s1(1, AO)
    small_grads(1)
    small_send(1)

    norms(x_ref, 0, True)
    drained(1, DN, 0)
    drained(1, UP, 0)
    mlp_a(0, dh)
    s0(0, DN)
    s3(1, DN)
    s1(0, DN)
    mlp_b(0, dh, False)
    s0(0, UP)
    make_qkv(0)
    dctx[EV] = mm_nt(dh[EV], wa[0, :, Q3:]).astype(BF)
    s1(0, UP)
    heads(True, 0, 4)
    s2(1, AO)
    s3(1, UP)
    drained(1, AO, 0)
    attn_grads(0, dh)
    s0(0, AO)
    xg_ref[EV] = layer_end(x_ref, 0, dh)
    small_grads(0)
    small_send(0)
    s1(0, AO)
    for stage, l, w in ((s2, 0, DN), (s2, 0, UP), (s3, 1, AO), (s2, 0, AO), (s3, 0, DN), (s3, 0, UP), (s4, 1, DN),
                        (s4, 1, UP), (s4, 1, AO), (s3, 0, AO)):
        stage(l, w)
    small_finish(1)
    small_finish(0)
    for w in (DN, UP, AO):
        s4(0, w)
    for w in (DN, UP, AO):
        drained(0, w, 0)
        for l in range(LAYERS):
            sent(l, w)
            for stage in range(1, 4):
                drained(l, w, stage)


def finish(y, xg, oq, oo, ou, od, osm, *outs):
    *outs, spread = outs
    yo, xo, g1, b1, gq, bq, go, bo, g2, b2, gup, bu, gdn, bd = outs
    yo[0] = y[EV]
    xo[0] = xg[EV]
    go[EV] = oo[EV]
    gup[EV] = ou[EV]
    gdn[EV] = od[EV]
    for row, ref in enumerate((g1, b1, bo, g2, b2, bd, bu, bq)):
        for l in range(LAYERS):
            ref[l:l + 1, :] = osm[l, row:row + 1, 0:ref.shape[1]].astype(BF)
    for l in range(LAYERS):
        for h in range(8):
            q, k, v = (oq[l, :, DM * t + HD * h:DM * t + HD * h + HD].astype(F32) for t in range(3))
            spread[0, pl.ds(h, SH, stride=8), :] = jnp.concatenate([q, k], axis=1)
            spread[1, pl.ds(h, SH, stride=8), :] = jnp.concatenate([v, v], axis=1)
        gq[l, :, :, :LN] = spread[0].reshape(SH, 8, LN).astype(BF)
        gq[l, :, :, LN:] = spread[1, :, :HD].reshape(SH, 8, HD).astype(BF)


def rope_constants():
    rot, half, hd = 16, 8, HD
    inv = (1.0 / (10000.0 ** (np.arange(0, rot, 2, dtype=np.float32) / np.float32(rot)))).astype(np.float32)
    ang = np.arange(SEQ, dtype=np.float32)[:, None] * inv[None, :]
    cos, sin = np.cos(ang).astype(np.float32), np.sin(ang).astype(np.float32)
    c = np.ones((SEQ, LN), np.float32)
    p = np.zeros((SEQ, LN), np.float32)
    q = np.zeros((SEQ, LN), np.float32)
    for base in (0, hd):
        c[:, base:base + half] = cos
        c[:, base + half:base + rot] = cos
        p[:, base:base + half] = -sin
        q[:, base + half:base + rot] = sin
    return np.stack([c, p, q])


def solution(mesh):
    shard_axes = ('node', 'local')
    act_spec = P(shard_axes)
    param_spec = P(None, shard_axes)
    consts = rope_constants()
    vm = pl.BlockSpec(memory_space=pltpu.VMEM)
    hbm = pl.BlockSpec(memory_space=pl.ANY)

    def device_step(x, y_cot, g1, b1, wqkv, bqkv, wout, bout, g2, b2, wup, bup, wdn, bdn):
        little = (g1, b1, bout, g2, b2, bdn, bup, bqkv)

        def v(shape, dt):
            return pltpu.VMEM(shape, dt)

        wshape = [(LAYERS, ND * ROWS[w], COLS[w]) for w in range(3)]
        scratch = [v(wshape[w], BF) for w in range(3)]
        scratch += [v((2, 2, 2, 2, ROWS[w], COLS[w]), F32) for w in range(3)]
        for lead in ((2, 2, 2), (2, 2), (2,), ()):
            scratch += [v((LAYERS,) + lead + (ROWS[w], COLS[w]), F32) for w in range(3)]
        scratch += [v((ND, LAYERS, 8, LN), F32)] + [v(p.shape, BF) for p in little]
        scratch += [v((LAYERS, 8, DM), F32), v((LAYERS, 1, FF), F32),
                    v((LAYERS, 1, 3 * DM), F32), v((LAYERS, ND, 8, LN), F32), v((LAYERS, ND, 8, LN), F32),
                    v((8, DM), F32), v((1, FF), F32), v((1, 3 * DM), F32)]
        scratch += [v((SEQ, DM), BF), v((SEQ, DM), BF), v((3, SEQ, LN), F32), v((LAYERS, SH, 8, 3 * HD), BF),
                    v((2, SEQ, LN), F32), v((SEQ, FF), BF), v((SEQ, FF), F32)]
        scratch += [v((SEQ, DM), BF), v((SEQ, DM), BF), v((SEQ, DM), BF), v((SEQ, DM), BF),
                    v((DM, SEQ), BF), v((DM, SEQ), BF), v((SEQ, 3 * DM), BF), v((SEQ, 3 * DM), BF),
                    v((SEQ, DM), BF), v((SEQ, DM), BF), v((SEQ, DM), F32), v((SEQ, DM), F32)]
        dma = pltpu.SemaphoreType.DMA
        scratch += [dma((6, 4)), dma((LAYERS, 3)), dma((LAYERS, 3, 3, 8)), dma((LAYERS, 3)), dma((LAYERS, 3, 3, 4)),
                    dma((LAYERS, 3, 3, 4)), dma, dma, dma((LAYERS,)), dma((LAYERS,))]
        sds = jax.ShapeDtypeStruct
        mids = pl.pallas_call(
            kernel,
            out_shape=[sds((SEQ, DM), BF), sds((SEQ, DM), BF), sds((LAYERS, SH, Q3), BF), sds((LAYERS, SH, DM), BF),
                       sds((LAYERS, SH, FF), BF), sds((LAYERS, LN, DM), BF), sds((LAYERS, 8, LN), F32)],
            in_specs=[hbm] * 15,
            out_specs=[vm] * 7,
            scratch_shapes=scratch,
            compiler_params=pltpu.CompilerParams(has_side_effects=True, collective_id=0, vmem_limit_bytes=67043328),
            name='step',
        )(x[0], y_cot[0], wqkv, wout, wup, wdn, *little, consts)
        y, xg, oq, oo, ou, od, osm = mids
        like = (x, y_cot, g1, b1, wqkv, bqkv, wout, bout, g2, b2, wup, bup, wdn, bdn)
        return pl.pallas_call(finish, out_shape=[sds(p.shape, BF) for p in like], in_specs=[vm] * 7,
                              out_specs=[vm] * 14, scratch_shapes=[v((2, SEQ, LN), F32)],
                              name='finish')(y, xg, oq, oo, ou, od, osm)

    return jax.shard_map(device_step, mesh=mesh,
                         in_specs=(act_spec, act_spec) + (param_spec,) * 12,
                         out_specs=(act_spec, act_spec) + (param_spec,) * 12,
                         check_vma=False)
```

```python
import numpy as np
import jax
import jax.numpy as jnp
from jax import lax
from jax.experimental import pallas as pl
from jax.experimental.pallas import tpu as pltpu
from jax.sharding import PartitionSpec as P

BF, F32 = jnp.bfloat16, jnp.float32
MESH = pl.DeviceIdType.MESH
EPSILON = 1e-5
LAYERS, SEQ, DM, FF, ND = 2, 256, 512, 2048, 16
SH, HD, LN, Q3 = 32, 64, 128, 1536
ROWS = (SH, SH, LN, 8)
COLS = (FF, FF, DM, LN)
WIDTH = FF + LN
AO, UP, DN, SM = range(4)
ORDERS = ((1, 2, 4), (2, 4, 1), (4, 1, 2))
CHIP_AXES = [4, 2, 1]
CUTS = ((0, 384, 1152, FF), (0, 384, 1152, FF), (0, SH, 80, LN))
WIDE = (0, 384, 1152, WIDTH)
ROUTES = ((1, 2), (2, 1))
ALL, EV = slice(None), ...
TOK = 2 * SEQ


def routes(w):
    return ORDERS[:1] if w == SM else ROUTES


def axes_of(w):
    return CHIP_AXES if w == SM else CHIP_AXES[1:]


def piece(w, k):
    if w == SM:
        return ALL, ALL
    n = (ROWS if w == DN else COLS)[w] // 2
    part = slice(n * k, n * k + n)
    return (part, ALL) if w == DN else (ALL, part)


def bit(v, a):
    return lax.rem(lax.div(v, a), 2)


def flip(v, mask):
    for a in (1, 2, 4):
        if mask & a:
            v = v + a - 2 * a * bit(v, a)
    return v


def col_sum(v):
    return jnp.sum(v, axis=0, keepdims=True)


def row_of(f, v):
    return f(v, axis=-1, keepdims=True)


def mm(a, b):
    return jnp.dot(a, b, preferred_element_type=F32)


def mm_nt(a, b):
    return lax.dot_general(a, b, (((1,), (1,)), ((), ())), preferred_element_type=F32)


def mm_tn(a, b):
    return lax.dot_general(a, b, (((0,), (0,)), ((), ())), preferred_element_type=F32)


def kernel(x_in, cot_in, wq_in, wo_in, wu_in, wd_in, p0, p1, p2, p3, p4, p5, p6, p7, rope_in,
           y_ref, xg_ref, oq_ref, oo_ref, ou_ref, od_ref, os_ref,
           wa, wu, wd, ga, gu, gd, gs, ra0, ra1, ra2, ru0, ru1, ru2, rd0, rd1, rd2, rs0, rs1, rs2, rs3,
           v0, v1, v2, v3, v4, v5, v6, v7, vec, upb, qkvb, gvec, gub, gqb,
           x_ref, cot_ref, rope_ref, native, spread, act_s, slope_s,
           h1, dh, na, nm, nat, nmt, qkv, dqkv, ctx, dctx, acc, dnm,
           loc_sem, ag_send, ag_ici, ag_d2d, rs_send, rs_recv, ex_send, ex_recv):
    me = lax.axis_index('node') * 8 + lax.axis_index('local')
    chip = lax.div(me, 2)
    core = lax.rem(me, 2)
    other = 1 - core
    W, G = (wa, wu, wd), (ga, gu, gd, gs)
    R = ((ra0, ra1, ra2), (ru0, ru1, ru2), (rd0, rd1, rd2), (rs0, rs1, rs2, rs3))
    node = lax.div(chip, 4)
    zrows = pl.ds(pl.multiple_of(node * SEQ, SEQ), SEQ)

    def dev(c, k):
        i = c * 2 + k
        return (lax.div(i, 8), lax.rem(i, 8))

    def rows_of(l, w, start, n):
        rows = pl.ds(start, n * ROWS[w])
        if w == AO and l == 1:
            return W[w].at[l, rows, pl.ds(0, FF)]
        return W[w].at[l, rows]

    def block(l, w, c, k):
        return rows_of(l, w, pl.multiple_of((c * 2 + k) * ROWS[w], ROWS[w]), 1)

    def part(l, w, k, mask):
        base = (flip(chip, mask) * 2 + core) * ROWS[w]
        cuts = WIDE if w == AO and l == 0 else CUTS[w]
        lo, hi = cuts[k], cuts[k + 1]
        if w == DN:
            return W[w].at[l, pl.ds(pl.multiple_of(base + lo, 16), hi - lo)]
        return W[w].at[l, pl.ds(pl.multiple_of(base, SH), SH), lo:hi]

    def push(l, w, src, to, recv_sem):
        pltpu.make_async_remote_copy(src_ref=src, dst_ref=src, send_sem=ag_send.at[l, w], recv_sem=recv_sem,
                                     device_id=to, device_id_type=MESH).start()

    def to_link(l, w, k, mask, a):
        push(l, w, part(l, w, k, mask), dev(flip(chip, a), core), ag_ici.at[l, w, k, mask ^ a])

    def to_partner(l, w, k, mask):
        push(l, w, part(l, w, k, mask), dev(chip, other), ag_d2d.at[l, w])

    def await_in(l, w, src, recv_sem):
        pltpu.make_async_remote_copy(src_ref=src, dst_ref=src, send_sem=ag_send.at[l, w], recv_sem=recv_sem,
                                     device_id=dev(chip, other), device_id_type=MESH).wait_recv()

    def got(l, w, k, mask):
        await_in(l, w, part(l, w, k, mask), ag_ici.at[l, w, k, mask])

    def got_partner(l, w):
        await_in(l, w, rows_of(l, w, 0, 8), ag_d2d.at[l, w])

    def sent(l, w):
        src = rows_of(l, w, 0, 15)
        pltpu.make_async_remote_copy(src_ref=src, dst_ref=src, send_sem=ag_send.at[l, w], recv_sem=ag_d2d.at[l, w],
                                     device_id=dev(chip, other), device_id_type=MESH).wait_send()

    def own(l, w):
        for i in range(3):
            for k in range(3):
                to_link(l, w, k, 0, ORDERS[k][i])
        push(l, w, block(l, w, chip, core), dev(chip, other), ag_d2d.at[l, w])

    def f1(l, w):
        for k, (a, b, c) in enumerate(ORDERS):
            got(l, w, k, a)
            to_link(l, w, k, a, b)
        for k, (a, b, c) in enumerate(ORDERS):
            to_link(l, w, k, a, c)
            to_partner(l, w, k, a)

    def f2(l, w):
        for k, (a, b, c) in enumerate(ORDERS):
            got(l, w, k, b)
            to_link(l, w, k, b, c)
            to_partner(l, w, k, b)

    def f3(l, w):
        for k, (a, b, c) in enumerate(ORDERS):
            got(l, w, k, a | b)
            to_link(l, w, k, a | b, c)
            to_partner(l, w, k, a | b)

    def f4(l, w):
        for i in range(4):
            for k, (a, b, c) in enumerate(ORDERS):
                m = (c, a | c, b | c, 7)[i]
                got(l, w, k, m)
                to_partner(l, w, k, m)

    rs = {}

    def rs_copy(l, w, k, stage, src, dst, to):
        cp = pltpu.make_async_remote_copy(src_ref=src, dst_ref=dst, send_sem=rs_send.at[l, w, k, stage],
                                          recv_sem=rs_recv.at[l, w, k, stage], device_id=to, device_id_type=MESH)
        cp.start()
        rs[l, w, k, stage] = cp

    def pick(axes, a, v):
        return tuple(v if m == a else ALL for m in axes)

    def drained(l, w, stage):
        for k in range(len(routes(w))):
            rs[l, w, k, stage].wait_send()

    def step(l, w, stage):
        axes = axes_of(w)
        n = len(axes)
        for k, route in enumerate(routes(w)):
            cut = piece(w, k)
            if stage == 0:
                rs_copy(l, w, k, 0, G[w].at[(ALL,) * n + (other,) + cut], R[w][0].at[(l,) + (ALL,) * n + cut],
                        dev(chip, other))
                continue
            rs[l, w, k, stage - 1].wait_recv()
            buf = R[w][stage - 1]
            left = [m for m in axes if m not in route[:stage - 1]]
            before = [m for m in axes if m not in route[:stage - 2]] if stage > 1 else axes

            def mine(where):
                if stage == 1:
                    return G[w][where + (core,) + cut]
                at = list(where)
                at.insert(before.index(route[stage - 2]), bit(chip, route[stage - 2]))
                return R[w][stage - 2][(l,) + tuple(at) + cut]

            if stage == n + 1:
                emit(l, w, k, cut, buf[(l,) + cut] + mine(()))
                continue
            for i in range(2 ** len(left)):
                where = tuple((i >> j) & 1 for j in range(len(left)))
                at = (l,) + where + cut
                buf[at] = buf[at] + mine(where)
            a = route[stage - 1]
            src = buf.at[(l,) + pick(left, a, 1 - bit(chip, a)) + cut]
            rs_copy(l, w, k, stage, src, R[w][stage].at[(l,) + (ALL,) * (len(left) - 1) + cut],
                    dev(flip(chip, a), core))

    def emit(l, w, k, cut, total):
        if w == SM:
            os_ref[l] = total
            return
        total = total.astype(BF)
        if w != AO:
            (None, ou_ref, od_ref)[w][(l,) + cut] = total
        elif k == 0:
            oq_ref[(l,) + cut] = total
        else:
            n = Q3 - cut[1].start
            oq_ref[l, :, cut[1].start:] = total[:, :n]
            oo_ref[l] = total[:, n:]

    def s0(l, w):
        step(l, w, 0)

    def s1(l, w):
        step(l, w, 1)

    def s2(l, w):
        step(l, w, 2)

    def s3(l, w):
        step(l, w, 3)

    def s4(l, w):
        step(l, w, 4)

    def normed(h_bf):
        h32 = h_bf.astype(F32)
        cen = h32 - row_of(jnp.mean, h32)
        rstd = lax.rsqrt(row_of(jnp.mean, cen * cen) + EPSILON)
        return cen * rstd, rstd

    def norms(h_ref, l, bwd):
        xhat, _ = normed(h_ref[EV])
        n1 = (xhat * vec[l, 0:1, :] + vec[l, 1:2, :]).astype(BF)
        n2 = (xhat * vec[l, 3:4, :] + vec[l, 4:5, :]).astype(BF)
        na[EV] = n1
        nm[EV] = n2
        if bwd:
            nat[EV] = n1.T
            nmt[EV] = n2.T

    def rope(xs, back, n):
        c, p, q = (rope_ref[t, :n] for t in range(3))
        if back:
            return xs * c + pltpu.roll(xs * p, 8, 1) + pltpu.roll(xs * q, 120, 1)
        return xs * c + pltpu.roll(xs, 120, 1) * p + pltpu.roll(xs, 8, 1) * q

    def make_qkv(l):
        for t in range(3):
            cols = slice(DM * t, DM * t + DM)
            raw = mm(na[EV], wa[l, :, cols]) + qkvb[l, :, cols]
            for s in range(4):
                part = raw[:, LN * s:LN * s + LN]
                if t < 2:
                    part = rope(part, False, TOK)
                qkv[:, DM * t + LN * s:DM * t + LN * s + LN] = part.astype(BF)

    def heads(bwd, lo, hi):
        lane = lax.broadcasted_iota(jnp.int32, (1, LN), 1)
        masks = [(lane < HD).astype(F32).astype(BF), (lane >= HD).astype(F32).astype(BF)]
        causal = (lax.broadcasted_iota(jnp.int32, (SEQ, SEQ), 0) >= lax.broadcasted_iota(jnp.int32, (SEQ, SEQ), 1))

        def body(j, carry):
            seq = lax.div(j, 4)
            rows = pl.ds(pl.multiple_of(seq * SEQ, SEQ), SEQ)
            col = pl.multiple_of((j - 4 * seq) * LN, LN)
            q, k, v = (qkv[rows, pl.ds(col + DM * t, LN)] for t in range(3))
            ctx_sum = jnp.zeros((SEQ, LN), F32)
            if bwd:
                dc = dctx[rows, pl.ds(col, LN)]
                dq = jnp.zeros((SEQ, LN), F32)
                dk = jnp.zeros((SEQ, LN), F32)
                dv = jnp.zeros((SEQ, LN), F32)
            for mask in masks:
                qm = q * mask
                sc = jnp.where(causal, mm_nt(qm, k) * 0.125, -1e30)
                e = jnp.exp(sc - row_of(jnp.max, sc))
                p = e / row_of(jnp.sum, e)
                pb = p.astype(BF)
                ctx_sum = ctx_sum + mm(pb, v * mask)
                if bwd:
                    dcm = dc * mask
                    dp = mm_nt(dcm, v).astype(BF).astype(F32)
                    dv = dv + mm_tn(pb, dcm)
                    ds = (p * (dp - row_of(jnp.sum, dp * p)) * 0.125).astype(BF)
                    dq = dq + mm(ds, k * mask)
                    dk = dk + mm_tn(ds, qm)
            ctx[rows, pl.ds(col, LN)] = ctx_sum.astype(BF)
            if bwd:
                for t, d in enumerate((dq, dk, dv)):
                    d = d.astype(BF).astype(F32)
                    if t < 2:
                        d = rope(d, True, SEQ)
                    gqb[seq, :, pl.ds(col + DM * t, LN)] = col_sum(d)
                    dqkv[rows, pl.ds(col + DM * t, LN)] = d.astype(BF)
            return carry

        lax.fori_loop(lo, hi, body, 0)

    def up_part(l, t):
        col = pl.multiple_of(t * DM, DM)
        pre = mm(nm[EV], wu[l, :, pl.ds(col, DM)]) + upb[l, :, pl.ds(col, DM)]
        cdf = 0.5 * (1.0 + lax.erf(pre * 0.7071067811865476))
        return col, pre, cdf, (pre * cdf).astype(BF)

    def mlp_fwd(l):
        def body(t, carry):
            col, pre, cdf, act = up_part(l, t)
            acc[EV] += mm(act, wd[l, pl.ds(col, DM), :])
            return carry

        acc[EV] = jnp.zeros_like(acc)
        lax.fori_loop(0, 4, body, 0)

    def mlp_a(l, dout):
        def body(t, carry):
            col, pre, cdf, act = up_part(l, t)
            act_s[:, pl.ds(col, DM)] = act
            slope_s[:, pl.ds(col, DM)] = cdf + pre * (0.3989422804014327 * jnp.exp(-0.5 * pre * pre))
            return carry

        def grad(t, carry):
            col = pl.multiple_of(node * 2 * DM + t * DM, DM)
            gd[t] = mm_tn(act_s[:, pl.ds(col, DM)], dout[EV]).reshape(2, 2, LN, DM)
            return carry

        lax.fori_loop(0, 4, body, 0)
        lax.fori_loop(0, 2, grad, 0)

    def mlp_b(l, dout, fwd):
        def body(t, carry):
            col = pl.multiple_of(t * DM, DM)
            wd_t = wd[l, pl.ds(col, DM), :]
            if fwd:
                acc[:SEQ] += mm(act_s[:SEQ, pl.ds(col, DM)], wd_t)
            dpre = mm_nt(dout[EV], wd_t).astype(BF).astype(F32) * slope_s[:, pl.ds(col, DM)]
            gub[0:1, pl.ds(col, DM)] = col_sum(dpre[:SEQ])
            dpb = dpre.astype(BF)
            gu[:, :, :, :, pl.ds(col, DM)] = mm(nmt[zrows, :], dpb).reshape(2, 2, 2, SH, DM)
            dnm[EV] += mm_nt(dpb, wu[l, :, pl.ds(col, DM)])
            return carry

        if fwd:
            acc[EV] = jnp.zeros_like(acc)
        dnm[EV] = jnp.zeros_like(dnm)
        lax.fori_loop(0, 4, body, 0)

    def attn_grads(l, dout):
        ga[:, :, :, :, Q3:] = mm_tn(ctx[:, zrows], dout[EV]).reshape(2, 2, 2, SH, DM)
        for t in range(3):
            cols = slice(DM * t, DM * t + DM)
            ga[:, :, :, :, cols] = mm(nat[zrows, :], dqkv[:, cols]).reshape(2, 2, 2, SH, DM)

    def layer_end(h_ref, l, dout, n):
        dna = mm_nt(dqkv[:n], wa[l, :, 0:Q3]).astype(BF).astype(F32)
        dnm32 = dnm[:n].astype(BF).astype(F32)
        xhat, rstd = normed(h_ref[:n])
        d32 = dout[:n].astype(F32)
        own_tok = slice(0, SEQ)
        sums = [dna * xhat, dna, d32, dnm32 * xhat, dnm32, d32]
        for i, v in enumerate(sums):
            gvec[i:i + 1, :] = col_sum(v[own_tok])
        dx = dna * vec[l, 0:1, :] + dnm32 * vec[l, 3:4, :]
        dhid = rstd * (dx - row_of(jnp.mean, dx) - xhat * row_of(jnp.mean, dx * xhat))
        return (d32 + dhid).astype(BF)

    def small_grads():
        for d in range(ND):
            at = (d // 8, d // 4 % 2, d // 2 % 2, d % 2)
            gs[at] = jnp.zeros((8, LN), F32)
            gs[at + (slice(0, 6), slice(0, SH))] = gvec[0:6, SH * d:SH * d + SH]
            gs[at + (slice(6, 7), ALL)] = gub[0:1, LN * d:LN * d + LN]
            for lo, col, n in bias_parts(d):
                gs[at + (slice(7, 8), slice(lo, lo + n))] = gqb[0, :, col:col + n]

    def vectors():
        for d in range(ND):
            both = wa[0, SH * d:SH * d + 16, FF:].astype(F32)
            for l in range(LAYERS):
                rows = both[8 * l:8 * l + 8]
                vec[l, 0:6, SH * d:SH * d + SH] = rows[0:6, 0:SH]
                upb[l, 0:1, LN * d:LN * d + LN] = rows[6:7]
                for lo, col, n in bias_parts(d):
                    qkvb[l, 0:1, col:col + n] = rows[7:8, lo:lo + n]

    def bias_parts(d):
        base = HD * (d // 2)
        if d % 2 == 0:
            return ((0, base, HD), (HD, DM + base, SH))
        return ((0, DM + base + SH, SH), (SH, 1024 + base, HD))

    def swap(i, ref):
        return pltpu.make_async_remote_copy(src_ref=ref.at[pl.ds(0, SEQ)], dst_ref=ref.at[pl.ds(SEQ, SEQ)],
                                            send_sem=ex_send.at[i], recv_sem=ex_recv.at[i],
                                            device_id=dev(flip(chip, 4), core), device_id_type=MESH)

    swap_x, swap_cot = swap(0, x_ref), swap(1, cot_ref)
    native_in = pltpu.make_async_copy(wq_in, native, loc_sem.at[0, 0])
    first = [pltpu.make_async_copy(wu_in.at[0], block(0, UP, chip, core), loc_sem.at[0, 1])]
    qo = pl.ds(pl.multiple_of(me * SH, SH), SH)
    rest = [pltpu.make_async_copy(wo_in.at[l], W[AO].at[l, qo, pl.ds(Q3, DM)], loc_sem.at[l + 2, 2])
            for l in range(LAYERS)]
    rest += [pltpu.make_async_copy(wd_in.at[l], block(l, DN, chip, core), loc_sem.at[l + 2, 3]) for l in range(LAYERS)]
    rest += [pltpu.make_async_copy(wu_in.at[1], block(1, UP, chip, core), loc_sem.at[0, 2]),
             pltpu.make_async_copy(x_in, x_ref.at[pl.ds(0, SEQ)], loc_sem.at[0, 3]),
             pltpu.make_async_copy(cot_in, cot_ref.at[pl.ds(0, SEQ)], loc_sem.at[1, 0]),
             pltpu.make_async_copy(rope_in, rope_ref, loc_sem.at[1, 1])]
    params, tmp = (p0, p1, p2, p3, p4, p5, p6, p7), (v0, v1, v2, v3, v4, v5, v6, v7)
    little = [pltpu.make_async_copy(params[i], tmp[i], loc_sem.at[4 + i // 4, i % 4]) for i in range(8)]
    first[0].start()
    native_in.start()
    for cp in little + rest:
        cp.start()

    barrier = pltpu.get_barrier_semaphore()
    near = [dev(chip, other)] + [dev(flip(chip, a), core) for a in CHIP_AXES]
    for to in near:
        pl.semaphore_signal(barrier, inc=1, device_id=to, device_id_type=MESH)
    first[0].wait()
    pl.semaphore_wait(barrier, len(near))
    own(0, UP)

    native_in.wait()
    for l in range(LAYERS):
        flat = native[l].astype(F32).reshape(SEQ, 3 * HD)
        spread[0] = flat[:, :LN]
        spread[1, :, :HD] = flat[:, LN:]
        for h in range(8):
            rows = [spread[i, pl.ds(h, SH, stride=8), :].astype(BF) for i in range(2)]
            for t in range(3):
                lo = HD * (t % 2)
                wa[l, qo, DM * t + HD * h:DM * t + HD * h + HD] = rows[t // 2][:, lo:lo + HD]
        if l == 0:
            for cp in little + rest:
                cp.wait()
            spread[0, 0:SH] = jnp.zeros((SH, LN), F32)
            for i in range(8):
                for m in range(LAYERS):
                    spread[0, 8 * m + i:8 * m + i + 1, 0:tmp[i].shape[1]] = tmp[i][m:m + 1, :].astype(F32)
            wa[0, qo, FF:] = spread[0, 0:SH].astype(BF)
            own(0, AO)
    swap_x.start()
    f1(0, UP)
    f2(0, UP)
    own(0, DN)
    f1(0, AO)
    f3(0, UP)
    f2(0, AO)
    f1(0, DN)
    f3(0, AO)
    f4(0, UP)
    own(1, UP)
    f2(0, DN)
    swap_cot.start()
    f4(0, AO)
    got_partner(0, AO)
    vectors()
    swap_x.wait_recv()
    norms(x_ref, 0, False)
    make_qkv(0)
    f3(0, DN)
    f1(1, UP)
    heads(False, 0, 2)
    own(1, DN)
    heads(False, 2, 4)
    f2(1, UP)
    heads(False, 4, 6)
    f3(1, UP)
    f4(0, DN)
    heads(False, 6, 8)
    f1(1, DN)
    got_partner(0, UP)
    got_partner(0, DN)
    mlp_fwd(0)
    f2(1, DN)
    own(1, AO)
    acc[EV] += mm(ctx[EV], wa[0, :, Q3:FF])
    h1[EV] = (x_ref[EV].astype(F32) + acc[EV] + vec[0, 2:3, :] + vec[0, 5:6, :]).astype(BF)
    f3(1, DN)
    f4(1, UP)
    norms(h1, 1, True)
    f1(1, AO)
    f2(1, AO)
    got_partner(1, UP)
    swap_cot.wait_recv()
    mlp_a(1, cot_ref)
    s0(1, DN)
    f4(1, DN)
    s1(1, DN)
    f3(1, AO)
    got_partner(1, DN)
    mlp_b(1, cot_ref, True)
    s0(1, UP)
    f4(1, AO)
    s1(1, UP)
    got_partner(1, AO)
    make_qkv(1)
    dctx[EV] = mm_nt(cot_ref[EV], wa[1, :, Q3:FF]).astype(BF)
    heads(True, 0, 4)
    s2(1, DN)
    heads(True, 4, 8)
    attn_grads(1, cot_ref)
    s0(1, AO)
    s2(1, UP)
    acc[:SEQ] += mm(ctx[:SEQ], wa[1, :, Q3:FF])
    y_ref[EV] = (h1[:SEQ].astype(F32) + acc[:SEQ] + vec[1, 2:3, :] + vec[1, 5:6, :]).astype(BF)
    dh[EV] = layer_end(h1, 1, cot_ref, TOK)
    s1(1, AO)
    small_grads()
    s0(1, SM)

    norms(x_ref, 0, True)
    drained(1, DN, 0)
    drained(1, UP, 0)
    mlp_a(0, dh)
    s0(0, DN)
    s1(1, SM)
    s1(0, DN)
    mlp_b(0, dh, False)
    s0(0, UP)
    s2(1, AO)
    make_qkv(0)
    dctx[EV] = mm_nt(dh[EV], wa[0, :, Q3:FF]).astype(BF)
    s1(0, UP)
    heads(True, 0, 4)
    s2(0, DN)
    s2(1, SM)
    heads(True, 4, 8)
    drained(1, SM, 0)
    drained(1, AO, 0)
    attn_grads(0, dh)
    s0(0, AO)
    s3(1, SM)
    xg_ref[EV] = layer_end(x_ref, 0, dh, SEQ)
    s1(0, AO)
    small_grads()
    s0(0, SM)
    s2(0, UP)
    s1(0, SM)
    for stage, l, w in ((s3, 1, DN), (s3, 1, UP), (s3, 1, AO), (s4, 1, SM), (s2, 0, SM), (s3, 0, DN), (s2, 0, AO),
                        (s3, 0, UP), (s3, 0, SM), (s4, 0, SM), (s3, 0, AO)):
        stage(l, w)
    swap_x.wait_send()
    swap_cot.wait_send()
    for w in (DN, UP, AO, SM):
        drained(0, w, 0)
        for l in range(LAYERS):
            if w != SM:
                sent(l, w)
            for stage in range(1, len(axes_of(w)) + 1):
                drained(l, w, stage)


def finish(y, xg, oq, oo, ou, od, osm, *outs):
    *outs, spread = outs
    yo, xo, g1, b1, gq, bq, go, bo, g2, b2, gup, bu, gdn, bd = outs
    yo[0] = y[EV]
    xo[0] = xg[EV]
    go[EV] = oo[EV]
    gup[EV] = ou[EV]
    gdn[EV] = od[EV]
    for row, ref in enumerate((g1, b1, bo, g2, b2, bd, bu, bq)):
        for l in range(LAYERS):
            ref[l:l + 1, :] = osm[l, row:row + 1, 0:ref.shape[1]].astype(BF)
    for l in range(LAYERS):
        for h in range(8):
            q, k, v = (oq[l, :, DM * t + HD * h:DM * t + HD * h + HD].astype(F32) for t in range(3))
            spread[0, pl.ds(h, SH, stride=8), :] = jnp.concatenate([q, k], axis=1)
            spread[1, pl.ds(h, SH, stride=8), :] = jnp.concatenate([v, v], axis=1)
        gq[l, :, :, :LN] = spread[0].reshape(SH, 8, LN).astype(BF)
        gq[l, :, :, LN:] = spread[1, :, :HD].reshape(SH, 8, HD).astype(BF)


def rope_constants():
    rot, half, hd = 16, 8, HD
    inv = (1.0 / (10000.0 ** (np.arange(0, rot, 2, dtype=np.float32) / np.float32(rot)))).astype(np.float32)
    ang = np.arange(SEQ, dtype=np.float32)[:, None] * inv[None, :]
    cos, sin = np.cos(ang).astype(np.float32), np.sin(ang).astype(np.float32)
    c = np.ones((SEQ, LN), np.float32)
    p = np.zeros((SEQ, LN), np.float32)
    q = np.zeros((SEQ, LN), np.float32)
    for base in (0, hd):
        c[:, base:base + half] = cos
        c[:, base + half:base + rot] = cos
        p[:, base:base + half] = -sin
        q[:, base + half:base + rot] = sin
    return np.tile(np.stack([c, p, q]), (1, 2, 1))


def solution(mesh):
    shard_axes = ('node', 'local')
    act_spec = P(shard_axes)
    param_spec = P(None, shard_axes)
    consts = rope_constants()
    vm = pl.BlockSpec(memory_space=pltpu.VMEM)
    hbm = pl.BlockSpec(memory_space=pl.ANY)

    def device_step(x, y_cot, g1, b1, wqkv, bqkv, wout, bout, g2, b2, wup, bup, wdn, bdn):
        little = (g1, b1, bout, g2, b2, bdn, bup, bqkv)

        def v(shape, dt):
            return pltpu.VMEM(shape, dt)

        wshape = [(LAYERS, ND * ROWS[w], WIDTH if w == AO else COLS[w]) for w in range(3)]
        scratch = [v(wshape[w], BF) for w in range(3)]
        scratch += [v((2,) * (len(axes_of(w)) + 1) + (ROWS[w], COLS[w]), F32) for w in range(4)]
        for w in range(4):
            n = len(axes_of(w))
            scratch += [v((LAYERS,) + (2,) * (n - i) + (ROWS[w], COLS[w]), F32) for i in range(n + 1)]
        scratch += [v(p.shape, BF) for p in little]
        scratch += [v((LAYERS, 8, DM), F32), v((LAYERS, 1, FF), F32), v((LAYERS, 1, Q3), F32),
                    v((8, DM), F32), v((1, FF), F32), v((2, 1, Q3), F32)]
        scratch += [v((TOK, DM), BF)] * 2
        scratch += [v((3, TOK, LN), F32), v((LAYERS, SH, 8, 3 * HD), BF), v((2, SEQ, LN), F32), v((TOK, FF), BF),
                    v((TOK, FF), F32)]
        scratch += [v((TOK, DM), BF)] * 4 + [v((DM, TOK), BF)] * 2 + [v((TOK, Q3), BF)] * 2
        scratch += [v((TOK, DM), BF)] * 2 + [v((TOK, DM), F32)] * 2
        dma = pltpu.SemaphoreType.DMA
        scratch += [dma((6, 4)), dma((LAYERS, 3)), dma((LAYERS, 3, 3, 8)), dma((LAYERS, 3)), dma((LAYERS, 4, 3, 4)),
                    dma((LAYERS, 4, 3, 4)), dma((2,)), dma((2,))]
        sds = jax.ShapeDtypeStruct
        mids = pl.pallas_call(
            kernel,
            out_shape=[sds((SEQ, DM), BF), sds((SEQ, DM), BF), sds((LAYERS, SH, Q3), BF), sds((LAYERS, SH, DM), BF),
                       sds((LAYERS, SH, FF), BF), sds((LAYERS, LN, DM), BF), sds((LAYERS, 8, LN), F32)],
            in_specs=[hbm] * 15,
            out_specs=[vm] * 7,
            scratch_shapes=scratch,
            compiler_params=pltpu.CompilerParams(has_side_effects=True, collective_id=0, vmem_limit_bytes=67043328),
            name='step',
        )(x[0], y_cot[0], wqkv, wout, wup, wdn, *little, consts)
        y, xg, oq, oo, ou, od, osm = mids
        like = (x, y_cot, g1, b1, wqkv, bqkv, wout, bout, g2, b2, wup, bup, wdn, bdn)
        return pl.pallas_call(finish, out_shape=[sds(p.shape, BF) for p in like], in_specs=[vm] * 7,
                              out_specs=[vm] * 14, scratch_shapes=[v((2, SEQ, LN), F32)],
                              name='finish')(y, xg, oq, oo, ou, od, osm)

    return jax.shard_map(device_step, mesh=mesh,
                         in_specs=(act_spec, act_spec) + (param_spec,) * 12,
                         out_specs=(act_spec, act_spec) + (param_spec,) * 12,
                         check_vma=False)
```

```python
import numpy as np
import jax
import jax.numpy as jnp
from jax import lax
from jax.experimental import pallas as pl
from jax.experimental.pallas import tpu as pltpu
from jax.sharding import PartitionSpec as P

BF, F32 = jnp.bfloat16, jnp.float32
MESH = pl.DeviceIdType.MESH
EPSILON = 1e-5
LAYERS, SEQ, DM, FF, ND = 2, 256, 512, 2048, 16
SH, HD, LN, Q3 = 32, 64, 128, 1536
ROWS = (SH, SH, LN, 8)
COLS = (FF, FF, DM, LN)
WIDTH = FF + LN
AO, UP, DN, SM = range(4)
ORDERS = ((1, 2, 4), (2, 4, 1), (4, 1, 2))
CHIP_AXES = [4, 2, 1]
CUTS = ((0, 384, 1152, FF), (0, 384, 1152, FF), (0, SH, 80, LN))
WIDE = (0, 384, 1152, WIDTH)
ROUTES = ((1, 2), (2, 1))
ALL, EV = slice(None), ...
TOK = 2 * SEQ


def routes(w):
    return ORDERS[:1] if w == SM else ROUTES


def axes_of(w):
    return CHIP_AXES if w == SM else CHIP_AXES[1:]


def piece(w, k):
    if w == SM:
        return ALL, ALL
    n = (ROWS if w == DN else COLS)[w] // 2
    part = slice(n * k, n * k + n)
    return (part, ALL) if w == DN else (ALL, part)


def bit(v, a):
    return lax.rem(lax.div(v, a), 2)


def flip(v, mask):
    for a in (1, 2, 4):
        if mask & a:
            v = v + a - 2 * a * bit(v, a)
    return v


def col_sum(v):
    return jnp.sum(v, axis=0, keepdims=True)


def row_of(f, v):
    return f(v, axis=-1, keepdims=True)


def mm(a, b):
    return jnp.dot(a, b, preferred_element_type=F32)


def mm_nt(a, b):
    return lax.dot_general(a, b, (((1,), (1,)), ((), ())), preferred_element_type=F32)


def mm_tn(a, b):
    return lax.dot_general(a, b, (((0,), (0,)), ((), ())), preferred_element_type=F32)


def kernel(x_in, cot_in, wq_in, wo_in, wu_in, wd_in, p0, p1, p2, p3, p4, p5, p6, p7, rope_in,
           y_ref, xg_ref, oq_ref, oo_ref, ou_ref, od_ref, os_ref,
           wa, wu, wd, ga, gu, gd, gs, ra0, ra1, ra2, ru0, ru1, ru2, rd0, rd1, rd2, rs0, rs1, rs2, rs3,
           v0, v1, v2, v3, v4, v5, v6, v7, vec, upb, qkvb, gvec, gub, gqb,
           x_ref, cot_ref, rope_ref, native, spread, act_s, slope_s,
           h1, dh, na, nm, nat, nmt, qkv, dqkv, ctx, dctx, acc, dnm,
           loc_sem, ag_send, ag_ici, ag_d2d, rs_send, rs_recv, ex_send, ex_recv):
    me = lax.axis_index('node') * 8 + lax.axis_index('local')
    chip = lax.div(me, 2)
    core = lax.rem(me, 2)
    other = 1 - core
    W, G = (wa, wu, wd), (ga, gu, gd, gs)
    R = ((ra0, ra1, ra2), (ru0, ru1, ru2), (rd0, rd1, rd2), (rs0, rs1, rs2, rs3))
    node = lax.div(chip, 4)
    zrows = pl.ds(pl.multiple_of(node * SEQ, SEQ), SEQ)

    def dev(c, k):
        i = c * 2 + k
        return (lax.div(i, 8), lax.rem(i, 8))

    def rows_of(l, w, start, n):
        rows = pl.ds(start, n * ROWS[w])
        if w == AO and l == 1:
            return W[w].at[l, rows, pl.ds(0, FF)]
        return W[w].at[l, rows]

    def block(l, w, c, k):
        return rows_of(l, w, pl.multiple_of((c * 2 + k) * ROWS[w], ROWS[w]), 1)

    def part(l, w, k, mask):
        base = (flip(chip, mask) * 2 + core) * ROWS[w]
        cuts = WIDE if w == AO and l == 0 else CUTS[w]
        lo, hi = cuts[k], cuts[k + 1]
        if w == DN:
            return W[w].at[l, pl.ds(pl.multiple_of(base + lo, 16), hi - lo)]
        return W[w].at[l, pl.ds(pl.multiple_of(base, SH), SH), lo:hi]

    def push(l, w, src, to, recv_sem):
        pltpu.make_async_remote_copy(src_ref=src, dst_ref=src, send_sem=ag_send.at[l, w], recv_sem=recv_sem,
                                     device_id=to, device_id_type=MESH).start()

    def to_link(l, w, k, mask, a):
        push(l, w, part(l, w, k, mask), dev(flip(chip, a), core), ag_ici.at[l, w, k, mask ^ a])

    def to_partner(l, w, k, mask):
        push(l, w, part(l, w, k, mask), dev(chip, other), ag_d2d.at[l, w])

    def await_in(l, w, src, recv_sem):
        pltpu.make_async_remote_copy(src_ref=src, dst_ref=src, send_sem=ag_send.at[l, w], recv_sem=recv_sem,
                                     device_id=dev(chip, other), device_id_type=MESH).wait_recv()

    def got(l, w, k, mask):
        await_in(l, w, part(l, w, k, mask), ag_ici.at[l, w, k, mask])

    def got_partner(l, w):
        await_in(l, w, rows_of(l, w, 0, 8), ag_d2d.at[l, w])

    def sent(l, w):
        src = rows_of(l, w, 0, 15)
        pltpu.make_async_remote_copy(src_ref=src, dst_ref=src, send_sem=ag_send.at[l, w], recv_sem=ag_d2d.at[l, w],
                                     device_id=dev(chip, other), device_id_type=MESH).wait_send()

    def own(l, w):
        for i in range(3):
            for k in range(3):
                to_link(l, w, k, 0, ORDERS[k][i])
        push(l, w, block(l, w, chip, core), dev(chip, other), ag_d2d.at[l, w])

    def f1(l, w):
        for k, (a, b, c) in enumerate(ORDERS):
            got(l, w, k, a)
            to_link(l, w, k, a, b)
        for k, (a, b, c) in enumerate(ORDERS):
            to_link(l, w, k, a, c)
            to_partner(l, w, k, a)

    def f2(l, w):
        for k, (a, b, c) in enumerate(ORDERS):
            got(l, w, k, b)
            to_link(l, w, k, b, c)
            to_partner(l, w, k, b)

    def f3(l, w):
        for k, (a, b, c) in enumerate(ORDERS):
            got(l, w, k, a | b)
            to_link(l, w, k, a | b, c)
            to_partner(l, w, k, a | b)

    def f4(l, w):
        for i in range(4):
            for k, (a, b, c) in enumerate(ORDERS):
                m = (c, a | c, b | c, 7)[i]
                got(l, w, k, m)
                to_partner(l, w, k, m)

    rs = {}

    def rs_copy(l, w, k, stage, src, dst, to):
        cp = pltpu.make_async_remote_copy(src_ref=src, dst_ref=dst, send_sem=rs_send.at[l, w, k, stage],
                                          recv_sem=rs_recv.at[l, w, k, stage], device_id=to, device_id_type=MESH)
        cp.start()
        rs[l, w, k, stage] = cp

    def pick(axes, a, v):
        return tuple(v if m == a else ALL for m in axes)

    def drained(l, w, stage):
        for k in range(len(routes(w))):
            rs[l, w, k, stage].wait_send()

    def step(l, w, stage):
        axes = axes_of(w)
        n = len(axes)
        for k, route in enumerate(routes(w)):
            cut = piece(w, k)
            if stage == 0:
                rs_copy(l, w, k, 0, G[w].at[(ALL,) * n + (other,) + cut], R[w][0].at[(l,) + (ALL,) * n + cut],
                        dev(chip, other))
                continue
            rs[l, w, k, stage - 1].wait_recv()
            buf = R[w][stage - 1]
            left = [m for m in axes if m not in route[:stage - 1]]
            before = [m for m in axes if m not in route[:stage - 2]] if stage > 1 else axes

            def mine(where):
                if stage == 1:
                    return G[w][where + (core,) + cut]
                at = list(where)
                at.insert(before.index(route[stage - 2]), bit(chip, route[stage - 2]))
                return R[w][stage - 2][(l,) + tuple(at) + cut]

            if stage == n + 1:
                emit(l, w, k, cut, buf[(l,) + cut] + mine(()))
                continue
            for i in range(2 ** len(left)):
                where = tuple((i >> j) & 1 for j in range(len(left)))
                at = (l,) + where + cut
                buf[at] = buf[at] + mine(where)
            a = route[stage - 1]
            src = buf.at[(l,) + pick(left, a, 1 - bit(chip, a)) + cut]
            rs_copy(l, w, k, stage, src, R[w][stage].at[(l,) + (ALL,) * (len(left) - 1) + cut],
                    dev(flip(chip, a), core))

    def emit(l, w, k, cut, total):
        if w == SM:
            os_ref[l] = total
            return
        total = total.astype(BF)
        if w != AO:
            (None, ou_ref, od_ref)[w][(l,) + cut] = total
        elif k == 0:
            oq_ref[(l,) + cut] = total
        else:
            n = Q3 - cut[1].start
            oq_ref[l, :, cut[1].start:] = total[:, :n]
            oo_ref[l] = total[:, n:]

    def s0(l, w):
        step(l, w, 0)

    def s1(l, w):
        step(l, w, 1)

    def s2(l, w):
        step(l, w, 2)

    def s3(l, w):
        step(l, w, 3)

    def s4(l, w):
        step(l, w, 4)

    def normed(h_bf):
        h32 = h_bf.astype(F32)
        cen = h32 - row_of(jnp.mean, h32)
        rstd = lax.rsqrt(row_of(jnp.mean, cen * cen) + EPSILON)
        return cen * rstd, rstd

    def norms(h_ref, l):
        xhat, _ = normed(h_ref[EV])
        n1 = (xhat * vec[l, 0:1, :] + vec[l, 1:2, :]).astype(BF)
        n2 = (xhat * vec[l, 3:4, :] + vec[l, 4:5, :]).astype(BF)
        na[EV] = n1
        nm[EV] = n2
        nat[l] = n1.T
        nmt[l] = n2.T

    def rope(xs, back, n):
        c, p, q = (rope_ref[t, :n] for t in range(3))
        if back:
            return xs * c + pltpu.roll(xs * p, 8, 1) + pltpu.roll(xs * q, 120, 1)
        return xs * c + pltpu.roll(xs, 120, 1) * p + pltpu.roll(xs, 8, 1) * q

    def make_qkv(l):
        for t in range(3):
            cols = slice(DM * t, DM * t + DM)
            raw = mm(na[EV], wa[l, :, cols]) + qkvb[l, :, cols]
            for s in range(4):
                part = raw[:, LN * s:LN * s + LN]
                if t < 2:
                    part = rope(part, False, TOK)
                qkv[l, :, DM * t + LN * s:DM * t + LN * s + LN] = part.astype(BF)

    def heads(l, bwd, lo, hi):
        lane = lax.broadcasted_iota(jnp.int32, (1, LN), 1)
        sides = [(lane < HD).astype(F32), (lane >= HD).astype(F32)]
        row, key = (lax.broadcasted_iota(jnp.int32, (SEQ, SEQ), t) for t in range(2))
        causal = row >= key

        def pair(seq, col):
            rows = slice(SEQ * seq, SEQ * seq + SEQ)
            q, k, v = (qkv[l, rows, pl.ds(col + DM * t, LN)] for t in range(3))
            dc = dctx[rows, pl.ds(col, LN)] if bwd else None
            out = dq = dk = dv = 0.0
            for side in sides:
                one, eighth = side.astype(BF), (side * 0.125).astype(BF)
                qm = q * eighth
                sc = jnp.where(causal, mm_nt(qm, k), -1e30)
                e = jnp.exp(sc - row_of(jnp.max, sc))
                p = e * (1.0 / row_of(jnp.sum, e))
                pb = p.astype(BF)
                out += mm(pb, v * one)
                if bwd:
                    dcm = dc * one
                    dp = mm_nt(dcm, v).astype(BF).astype(F32)
                    ds = (p * (dp - row_of(jnp.sum, dp * p))).astype(BF)
                    dq += mm(ds, k * eighth)
                    dk += mm_tn(ds, qm)
                    dv += mm_tn(pb, dcm)
            ctx[rows, pl.ds(col, LN)] = out.astype(BF)
            if bwd:
                for t, d in enumerate((dq, dk, dv)):
                    d = d.astype(BF).astype(F32)
                    if t < 2:
                        d = rope(d, True, SEQ)
                    if seq == 0:
                        gqb[0:1, pl.ds(col + DM * t, LN)] = col_sum(d)
                    dqkv[rows, pl.ds(col + DM * t, LN)] = d.astype(BF)

        def body(j, carry):
            col = pl.multiple_of(j * LN, LN)
            for seq in range(2):
                pair(seq, col)
            return carry

        lax.fori_loop(lo, hi, body, 0)

    def up_part(l, t):
        col = pl.multiple_of(t * DM, DM)
        pre = mm(nm[EV], wu[l, :, pl.ds(col, DM)]) + upb[l, :, pl.ds(col, DM)]
        cdf = 0.5 * (1.0 + lax.erf(pre * 0.7071067811865476))
        return col, pre, cdf, (pre * cdf).astype(BF)

    def activate(l, fwd, lo, hi):
        def body(t, carry):
            col, pre, cdf, act = up_part(l, t)
            act_s[l, :, pl.ds(col, DM)] = act
            slope_s[l, :, pl.ds(col, DM)] = cdf + pre * (0.3989422804014327 * jnp.exp(-0.5 * pre * pre))
            if fwd:
                acc[EV] += mm(act, wd[l, pl.ds(col, DM), :])
            return carry

        if fwd and lo == 0:
            acc[EV] = jnp.zeros_like(acc)
        lax.fori_loop(lo, hi, body, 0)

    def down_grad(l, dout):
        def grad(t, carry):
            col = pl.multiple_of(node * 2 * DM + t * DM, DM)
            gd[t] = mm_tn(act_s[l, :, pl.ds(col, DM)], dout[EV]).reshape(2, 2, LN, DM)
            return carry

        lax.fori_loop(0, 2, grad, 0)

    def mlp_b(l, dout, fwd, lo, hi):
        def body(t, carry):
            col = pl.multiple_of(t * DM, DM)
            wd_t = wd[l, pl.ds(col, DM), :]
            if fwd:
                acc[:SEQ] += mm(act_s[l, :SEQ, pl.ds(col, DM)], wd_t)
            dpre = mm_nt(dout[EV], wd_t).astype(BF).astype(F32) * slope_s[l, :, pl.ds(col, DM)]
            gub[0:1, pl.ds(col, DM)] = col_sum(dpre[:SEQ])
            dpb = dpre.astype(BF)
            gu[:, :, :, :, pl.ds(col, DM)] = mm(nmt[l, zrows, :], dpb).reshape(2, 2, 2, SH, DM)
            dnm[EV] += mm_nt(dpb, wu[l, :, pl.ds(col, DM)])
            return carry

        if lo == 0:
            dnm[EV] = jnp.zeros_like(dnm)
            if fwd:
                acc[EV] = jnp.zeros_like(acc)
        lax.fori_loop(lo, hi, body, 0)

    def attn_grads(l, dout):
        ga[:, :, :, :, Q3:] = mm_tn(ctx[:, zrows], dout[EV]).reshape(2, 2, 2, SH, DM)
        for t in range(3):
            cols = slice(DM * t, DM * t + DM)
            ga[:, :, :, :, cols] = mm(nat[l, zrows, :], dqkv[:, cols]).reshape(2, 2, 2, SH, DM)

    def layer_end(h_ref, l, dout, n):
        dna = mm_nt(dqkv[:n], wa[l, :, 0:Q3]).astype(BF).astype(F32)
        dnm32 = dnm[:n].astype(BF).astype(F32)
        xhat, rstd = normed(h_ref[:n])
        d32 = dout[:n].astype(F32)
        own_tok = slice(0, SEQ)
        sums = [dna * xhat, dna, d32, dnm32 * xhat, dnm32, d32]
        for i, v in enumerate(sums):
            gvec[i:i + 1, :] = col_sum(v[own_tok])
        dx = dna * vec[l, 0:1, :] + dnm32 * vec[l, 3:4, :]
        dhid = rstd * (dx - row_of(jnp.mean, dx) - xhat * row_of(jnp.mean, dx * xhat))
        return (d32 + dhid).astype(BF)

    def small_grads():
        for d in range(ND):
            at = (d // 8, d // 4 % 2, d // 2 % 2, d % 2)
            gs[at] = jnp.zeros((8, LN), F32)
            gs[at + (slice(0, 6), slice(0, SH))] = gvec[0:6, SH * d:SH * d + SH]
            gs[at + (slice(6, 7), ALL)] = gub[0:1, LN * d:LN * d + LN]
            for lo, col, n in bias_parts(d):
                gs[at + (slice(7, 8), slice(lo, lo + n))] = gqb[0:1, col:col + n]

    def vectors():
        for d in range(ND):
            both = wa[0, SH * d:SH * d + 16, FF:].astype(F32)
            for l in range(LAYERS):
                rows = both[8 * l:8 * l + 8]
                vec[l, 0:6, SH * d:SH * d + SH] = rows[0:6, 0:SH]
                upb[l, 0:1, LN * d:LN * d + LN] = rows[6:7]
                for lo, col, n in bias_parts(d):
                    qkvb[l, 0:1, col:col + n] = rows[7:8, lo:lo + n]

    def bias_parts(d):
        base = HD * (d // 2)
        if d % 2 == 0:
            return ((0, base, HD), (HD, DM + base, SH))
        return ((0, DM + base + SH, SH), (SH, 1024 + base, HD))

    def swap(i, ref):
        return pltpu.make_async_remote_copy(src_ref=ref.at[pl.ds(0, SEQ)], dst_ref=ref.at[pl.ds(SEQ, SEQ)],
                                            send_sem=ex_send.at[i], recv_sem=ex_recv.at[i],
                                            device_id=dev(flip(chip, 4), core), device_id_type=MESH)

    swap_x, swap_cot = swap(0, x_ref), swap(1, cot_ref)
    (A0, U0, D0, V0), (A1, U1, D1, V1) = [[(l, w) for w in (AO, UP, DN, SM)] for l in range(LAYERS)]
    native_in = pltpu.make_async_copy(wq_in, native, loc_sem.at[0, 0])
    first = [pltpu.make_async_copy(wu_in.at[0], block(0, UP, chip, core), loc_sem.at[0, 1])]
    qo = pl.ds(pl.multiple_of(me * SH, SH), SH)
    rest = [pltpu.make_async_copy(wo_in.at[l], W[AO].at[l, qo, pl.ds(Q3, DM)], loc_sem.at[l + 2, 2])
            for l in range(LAYERS)]
    rest += [pltpu.make_async_copy(wd_in.at[l], block(l, DN, chip, core), loc_sem.at[l + 2, 3]) for l in range(LAYERS)]
    rest += [pltpu.make_async_copy(wu_in.at[1], block(1, UP, chip, core), loc_sem.at[0, 2]),
             pltpu.make_async_copy(x_in, x_ref.at[pl.ds(0, SEQ)], loc_sem.at[0, 3]),
             pltpu.make_async_copy(cot_in, cot_ref.at[pl.ds(0, SEQ)], loc_sem.at[1, 0]),
             pltpu.make_async_copy(rope_in, rope_ref.at[:, pl.ds(0, SEQ)], loc_sem.at[1, 1]),
             pltpu.make_async_copy(rope_in, rope_ref.at[:, pl.ds(SEQ, SEQ)], loc_sem.at[1, 2])]
    params, tmp = (p0, p1, p2, p3, p4, p5, p6, p7), (v0, v1, v2, v3, v4, v5, v6, v7)
    little = [pltpu.make_async_copy(params[i], tmp[i], loc_sem.at[4 + i // 4, i % 4]) for i in range(8)]
    first[0].start()
    native_in.start()
    for cp in little + rest:
        cp.start()

    barrier = pltpu.get_barrier_semaphore()
    near = [dev(chip, other)] + [dev(flip(chip, a), core) for a in CHIP_AXES]
    for to in near:
        pl.semaphore_signal(barrier, inc=1, device_id=to, device_id_type=MESH)
    first[0].wait()
    pl.semaphore_wait(barrier, len(near))
    own(*U0)

    native_in.wait()
    for l in range(LAYERS):
        flat = native[l].astype(F32).reshape(SEQ, 3 * HD)
        spread[0] = flat[:, :LN]
        spread[1, :, :HD] = flat[:, LN:]
        for h in range(8):
            rows = [spread[i, pl.ds(h, SH, stride=8), :].astype(BF) for i in range(2)]
            for t in range(3):
                lo = HD * (t % 2)
                wa[l, qo, DM * t + HD * h:DM * t + HD * h + HD] = rows[t // 2][:, lo:lo + HD]
        if l == 0:
            for cp in little + rest:
                cp.wait()
            spread[0, 0:SH] = jnp.zeros((SH, LN), F32)
            for i in range(8):
                for m in range(LAYERS):
                    spread[0, 8 * m + i:8 * m + i + 1, 0:tmp[i].shape[1]] = tmp[i][m:m + 1, :].astype(F32)
            wa[0, qo, FF:] = spread[0, 0:SH].astype(BF)
            own(*A0)
    swap_x.start()
    f1(*A0)
    f1(*U0)
    f2(*A0)
    own(*D0)
    f2(*U0)
    f3(*A0)
    f3(*U0)
    f1(*D0)
    f4(*A0)
    own(*U1)
    f4(*U0)
    got_partner(*A0)
    vectors()
    swap_x.wait_recv()
    norms(x_ref, 0)
    f2(*D0)
    make_qkv(0)
    f3(*D0)
    heads(0, False, 0, 1)
    f1(*U1)
    heads(0, False, 1, 2)
    f2(*U1)
    own(*A1)
    heads(0, False, 2, 4)
    f4(*D0)
    got_partner(*U0)
    got_partner(*D0)
    swap_cot.start()
    activate(0, True, 0, 2)
    f3(*U1)
    f1(*A1)
    activate(0, True, 2, 4)
    own(*D1)
    acc[EV] += mm(ctx[EV], wa[0, :, Q3:FF])
    h1[EV] = (x_ref[EV].astype(F32) + acc[EV] + vec[0, 2:3, :] + vec[0, 5:6, :]).astype(BF)
    f4(*U1)
    f2(*A1)
    norms(h1, 1)
    got_partner(*U1)
    activate(1, False, 0, 4)
    swap_cot.wait_recv()
    down_grad(1, cot_ref)
    s0(*D1)
    f3(*A1)
    f1(*D1)
    f4(*A1)
    s1(*D1)
    f2(*D1)
    got_partner(*A1)
    make_qkv(1)
    dctx[EV] = mm_nt(cot_ref[EV], wa[1, :, Q3:FF]).astype(BF)
    f3(*D1)
    heads(1, True, 0, 2)
    f4(*D1)
    heads(1, True, 2, 3)
    s2(*D1)
    heads(1, True, 3, 4)
    attn_grads(1, cot_ref)
    s0(*A1)
    got_partner(*D1)
    mlp_b(1, cot_ref, True, 0, 2)
    s1(*A1)
    mlp_b(1, cot_ref, True, 2, 4)
    s0(*U1)
    dh[EV] = layer_end(h1, 1, cot_ref, TOK)
    s1(*U1)
    acc[:SEQ] += mm(ctx[:SEQ], wa[1, :, Q3:FF])
    y_ref[EV] = (h1[:SEQ].astype(F32) + acc[:SEQ] + vec[1, 2:3, :] + vec[1, 5:6, :]).astype(BF)
    small_grads()
    s0(*V1)

    drained(*D1, 0)
    down_grad(0, dh)
    s0(*D0)
    drained(*U1, 0)
    mlp_b(0, dh, False, 0, 2)
    s1(*D0)
    s2(*A1)
    mlp_b(0, dh, False, 2, 4)
    s0(*U0)
    s1(*V1)
    dctx[EV] = mm_nt(dh[EV], wa[0, :, Q3:FF]).astype(BF)
    s1(*U0)
    heads(0, True, 0, 2)
    s2(*U1)
    s2(*V1)
    heads(0, True, 2, 4)
    drained(*V1, 0)
    drained(*A1, 0)
    attn_grads(0, dh)
    s0(*A0)
    s3(*V1)
    xg_ref[EV] = layer_end(x_ref, 0, dh, SEQ)
    s1(*A0)
    small_grads()
    s0(*V0)
    s2(*D0)
    s1(*V0)
    for stage, at in ((s2, U0), (s3, D1), (s3, A1), (s2, V0), (s3, U1), (s4, V1), (s2, A0), (s3, V0), (s3, D0), (s3, U0),
                      (s4, V0), (s3, A0)):
        stage(*at)
    swap_x.wait_send()
    swap_cot.wait_send()
    for w in (DN, UP, AO, SM):
        drained(0, w, 0)
        for l in range(LAYERS):
            if w != SM:
                sent(l, w)
            for stage in range(1, len(axes_of(w)) + 1):
                drained(l, w, stage)


def finish(y, xg, oq, oo, ou, od, osm, *outs):
    *outs, spread = outs
    yo, xo, g1, b1, gq, bq, go, bo, g2, b2, gup, bu, gdn, bd = outs
    yo[0] = y[EV]
    xo[0] = xg[EV]
    go[EV] = oo[EV]
    gup[EV] = ou[EV]
    gdn[EV] = od[EV]
    for row, ref in enumerate((g1, b1, bo, g2, b2, bd, bu, bq)):
        for l in range(LAYERS):
            ref[l:l + 1, :] = osm[l, row:row + 1, 0:ref.shape[1]].astype(BF)
    for l in range(LAYERS):
        for h in range(8):
            q, k, v = (oq[l, :, DM * t + HD * h:DM * t + HD * h + HD].astype(F32) for t in range(3))
            spread[0, pl.ds(h, SH, stride=8), :] = jnp.concatenate([q, k], axis=1)
            spread[1, pl.ds(h, SH, stride=8), :] = jnp.concatenate([v, v], axis=1)
        gq[l, :, :, :LN] = spread[0].reshape(SH, 8, LN).astype(BF)
        gq[l, :, :, LN:] = spread[1, :, :HD].reshape(SH, 8, HD).astype(BF)


def rope_constants():
    rot, half, hd = 16, 8, HD
    inv = (1.0 / (10000.0 ** (np.arange(0, rot, 2, dtype=np.float32) / np.float32(rot)))).astype(np.float32)
    ang = np.arange(SEQ, dtype=np.float32)[:, None] * inv[None, :]
    cos, sin = np.cos(ang).astype(np.float32), np.sin(ang).astype(np.float32)
    c = np.ones((SEQ, LN), np.float32)
    p = np.zeros((SEQ, LN), np.float32)
    q = np.zeros((SEQ, LN), np.float32)
    for base in (0, hd):
        c[:, base:base + half] = cos
        c[:, base + half:base + rot] = cos
        p[:, base:base + half] = -sin
        q[:, base + half:base + rot] = sin
    return np.stack([c, p, q])


def solution(mesh):
    shard_axes = ('node', 'local')
    act_spec = P(shard_axes)
    param_spec = P(None, shard_axes)
    consts = rope_constants()
    vm = pl.BlockSpec(memory_space=pltpu.VMEM)
    hbm = pl.BlockSpec(memory_space=pl.ANY)

    def device_step(x, y_cot, g1, b1, wqkv, bqkv, wout, bout, g2, b2, wup, bup, wdn, bdn):
        little = (g1, b1, bout, g2, b2, bdn, bup, bqkv)

        def v(shape, dt):
            return pltpu.VMEM(shape, dt)

        wshape = [(LAYERS, ND * ROWS[w], WIDTH if w == AO else COLS[w]) for w in range(3)]
        scratch = [v(wshape[w], BF) for w in range(3)]
        scratch += [v((2,) * (len(axes_of(w)) + 1) + (ROWS[w], COLS[w]), F32) for w in range(4)]
        for w in range(4):
            n = len(axes_of(w))
            scratch += [v((LAYERS,) + (2,) * (n - i) + (ROWS[w], COLS[w]), F32) for i in range(n + 1)]
        scratch += [v(p.shape, BF) for p in little]
        scratch += [v((LAYERS, 8, DM), F32), v((LAYERS, 1, FF), F32), v((LAYERS, 1, Q3), F32),
                    v((8, DM), F32), v((1, FF), F32), v((1, Q3), F32)]
        scratch += [v((TOK, DM), BF)] * 2
        scratch += [v((3, TOK, LN), F32), v((LAYERS, SH, 8, 3 * HD), BF), v((2, SEQ, LN), F32), v((LAYERS, TOK, FF), BF),
                    v((LAYERS, TOK, FF), F32)]
        scratch += [v((TOK, DM), BF)] * 4 + [v((LAYERS, DM, TOK), BF)] * 2 + [v((LAYERS, TOK, Q3), BF), v((TOK, Q3), BF)]
        scratch += [v((TOK, DM), BF)] * 2 + [v((TOK, DM), F32)] * 2
        dma = pltpu.SemaphoreType.DMA
        scratch += [dma((6, 4)), dma((LAYERS, 3)), dma((LAYERS, 3, 3, 8)), dma((LAYERS, 3)), dma((LAYERS, 4, 3, 4)),
                    dma((LAYERS, 4, 3, 4)), dma((2,)), dma((2,))]
        sds = jax.ShapeDtypeStruct
        mids = pl.pallas_call(
            kernel,
            out_shape=[sds((SEQ, DM), BF), sds((SEQ, DM), BF), sds((LAYERS, SH, Q3), BF), sds((LAYERS, SH, DM), BF),
                       sds((LAYERS, SH, FF), BF), sds((LAYERS, LN, DM), BF), sds((LAYERS, 8, LN), F32)],
            in_specs=[hbm] * 15,
            out_specs=[vm] * 7,
            scratch_shapes=scratch,
            compiler_params=pltpu.CompilerParams(has_side_effects=True, collective_id=0, vmem_limit_bytes=67043328),
            name='step',
        )(x[0], y_cot[0], wqkv, wout, wup, wdn, *little, consts)
        y, xg, oq, oo, ou, od, osm = mids
        like = (x, y_cot, g1, b1, wqkv, bqkv, wout, bout, g2, b2, wup, bup, wdn, bdn)
        return pl.pallas_call(finish, out_shape=[sds(p.shape, BF) for p in like], in_specs=[vm] * 7,
                              out_specs=[vm] * 14, scratch_shapes=[v((2, SEQ, LN), F32)],
                              name='finish')(y, xg, oq, oo, ou, od, osm)

    return jax.shard_map(device_step, mesh=mesh,
                         in_specs=(act_spec, act_spec) + (param_spec,) * 12,
                         out_specs=(act_spec, act_spec) + (param_spec,) * 12,
                         check_vma=False)
```

```python
import numpy as np
import jax
import jax.numpy as jnp
from jax import lax
from jax.experimental import pallas as pl
from jax.experimental.pallas import tpu as pltpu
from jax.sharding import PartitionSpec as P

BF, F32 = jnp.bfloat16, jnp.float32
MESH = pl.DeviceIdType.MESH
EPSILON = 1e-5
LAYERS, SEQ, DM, FF, ND = 2, 256, 512, 2048, 16
SH, HD, LN, Q3 = 32, 64, 128, 1536
ROWS = (SH, SH, LN, 8)
COLS = (FF, FF, DM, LN)
WIDTH = FF + LN
AO, UP, DN, SM = range(4)
ORDERS = ((1, 2, 4), (2, 4, 1), (4, 1, 2))
CHIP_AXES = [4, 2, 1]
CUTS = ((0, 384, 1152, FF), (0, 384, 1152, FF), (0, SH, 80, LN))
WIDE = (0, 384, 1152, WIDTH)
ROUTES = ((1, 2), (2, 1))
ALL, EV = slice(None), ...
TOK = 2 * SEQ


def routes(w):
    return ORDERS[2:] if w == SM else ROUTES


def axes_of(w):
    return CHIP_AXES if w == SM else CHIP_AXES[1:]


def piece(w, k):
    if w == SM:
        return ALL, ALL
    n = (ROWS if w == DN else COLS)[w] // 2
    part = slice(n * k, n * k + n)
    return (part, ALL) if w == DN else (ALL, part)


def bit(v, a):
    return lax.rem(lax.div(v, a), 2)


def flip(v, mask):
    for a in (1, 2, 4):
        if mask & a:
            v = v + a - 2 * a * bit(v, a)
    return v


def col_sum(v):
    return jnp.sum(v, axis=0, keepdims=True)


def row_of(f, v):
    return f(v, axis=-1, keepdims=True)


def mm(a, b):
    return jnp.dot(a, b, preferred_element_type=F32)


def mm_nt(a, b):
    return lax.dot_general(a, b, (((1,), (1,)), ((), ())), preferred_element_type=F32)


def mm_tn(a, b):
    return lax.dot_general(a, b, (((0,), (0,)), ((), ())), preferred_element_type=F32)


def kernel(x_in, cot_in, wq_in, wo_in, wu_in, wd_in, p0, p1, p2, p3, p4, p5, p6, p7, rope_in,
           y_ref, xg_ref, oq_ref, oo_ref, ou_ref, od_ref, os_ref,
           wa, wu, wd, ga, gu, gd, gs, ra0, ra1, ra2, ru0, ru1, ru2, rd0, rd1, rd2, rs0, rs1, rs2, rs3,
           v0, v1, v2, v3, v4, v5, v6, v7, vec, upb, qkvb, gvec, gub, gqb,
           x_ref, cot_ref, rope_ref, native, spread, act_s, slope_s,
           h1, dh, na, nm, nat, nmt, qkv, dqkv, ctx, dctx, acc, dnm,
           loc_sem, ag_send, ag_ici, ag_d2d, rs_send, rs_recv, ex_send, ex_recv):
    me = lax.axis_index('node') * 8 + lax.axis_index('local')
    chip = lax.div(me, 2)
    core = lax.rem(me, 2)
    other = 1 - core
    W, G = (wa, wu, wd), (ga, gu, gd, gs)
    R = ((ra0, ra1, ra2), (ru0, ru1, ru2), (rd0, rd1, rd2), (rs0, rs1, rs2, rs3))
    node = lax.div(chip, 4)
    zrows = pl.ds(pl.multiple_of(node * SEQ, SEQ), SEQ)

    def dev(c, k):
        i = c * 2 + k
        return (lax.div(i, 8), lax.rem(i, 8))

    def rows_of(l, w, start, n):
        rows = pl.ds(start, n * ROWS[w])
        if w == AO and l == 1:
            return W[w].at[l, rows, pl.ds(0, FF)]
        return W[w].at[l, rows]

    def block(l, w, c, k):
        return rows_of(l, w, pl.multiple_of((c * 2 + k) * ROWS[w], ROWS[w]), 1)

    def part(l, w, k, mask):
        base = (flip(chip, mask) * 2 + core) * ROWS[w]
        cuts = WIDE if w == AO and l == 0 else CUTS[w]
        lo, hi = cuts[k], cuts[k + 1]
        if w == DN:
            return W[w].at[l, pl.ds(pl.multiple_of(base + lo, 16), hi - lo)]
        return W[w].at[l, pl.ds(pl.multiple_of(base, SH), SH), lo:hi]

    def push(l, w, src, to, recv_sem):
        pltpu.make_async_remote_copy(src_ref=src, dst_ref=src, send_sem=ag_send.at[l, w], recv_sem=recv_sem,
                                     device_id=to, device_id_type=MESH).start()

    def to_link(l, w, k, mask, a):
        push(l, w, part(l, w, k, mask), dev(flip(chip, a), core), ag_ici.at[l, w, k, mask ^ a])

    def to_partner(l, w, k, mask):
        push(l, w, part(l, w, k, mask), dev(chip, other), ag_d2d.at[l, w])

    def await_in(l, w, src, recv_sem):
        pltpu.make_async_remote_copy(src_ref=src, dst_ref=src, send_sem=ag_send.at[l, w], recv_sem=recv_sem,
                                     device_id=dev(chip, other), device_id_type=MESH).wait_recv()

    def got(l, w, k, mask):
        await_in(l, w, part(l, w, k, mask), ag_ici.at[l, w, k, mask])

    def got_partner(l, w):
        await_in(l, w, rows_of(l, w, 0, 8), ag_d2d.at[l, w])

    def sent(l, w):
        src = rows_of(l, w, 0, 15)
        pltpu.make_async_remote_copy(src_ref=src, dst_ref=src, send_sem=ag_send.at[l, w], recv_sem=ag_d2d.at[l, w],
                                     device_id=dev(chip, other), device_id_type=MESH).wait_send()

    def own(l, w):
        for i in range(3):
            for k in range(3):
                to_link(l, w, k, 0, ORDERS[k][i])
        push(l, w, block(l, w, chip, core), dev(chip, other), ag_d2d.at[l, w])

    def f1(l, w):
        for k, (a, b, c) in enumerate(ORDERS):
            got(l, w, k, a)
            to_link(l, w, k, a, b)
        for k, (a, b, c) in enumerate(ORDERS):
            to_link(l, w, k, a, c)
            to_partner(l, w, k, a)

    def f2(l, w):
        for k, (a, b, c) in enumerate(ORDERS):
            got(l, w, k, b)
            to_link(l, w, k, b, c)
            to_partner(l, w, k, b)

    def f3(l, w):
        for k, (a, b, c) in enumerate(ORDERS):
            got(l, w, k, a | b)
            to_link(l, w, k, a | b, c)
            to_partner(l, w, k, a | b)

    def f4(l, w):
        for i in range(4):
            for k, (a, b, c) in enumerate(ORDERS):
                m = (c, a | c, b | c, 7)[i]
                got(l, w, k, m)
                to_partner(l, w, k, m)

    rs = {}

    def rs_copy(l, w, k, stage, src, dst, to):
        cp = pltpu.make_async_remote_copy(src_ref=src, dst_ref=dst, send_sem=rs_send.at[l, w, k, stage],
                                          recv_sem=rs_recv.at[l, w, k, stage], device_id=to, device_id_type=MESH)
        cp.start()
        rs[l, w, k, stage] = cp

    def pick(axes, a, v):
        return tuple(v if m == a else ALL for m in axes)

    def drained(l, w, stage):
        for k in range(len(routes(w))):
            rs[l, w, k, stage].wait_send()

    def step(l, w, stage):
        axes = axes_of(w)
        n = len(axes)
        for k, route in enumerate(routes(w)):
            cut = piece(w, k)
            if stage == 0:
                rs_copy(l, w, k, 0, G[w].at[(ALL,) * n + (other,) + cut], R[w][0].at[(l,) + (ALL,) * n + cut],
                        dev(chip, other))
                continue
            rs[l, w, k, stage - 1].wait_recv()
            buf = R[w][stage - 1]
            left = [m for m in axes if m not in route[:stage - 1]]
            before = [m for m in axes if m not in route[:stage - 2]] if stage > 1 else axes

            def mine(where):
                if stage == 1:
                    return G[w][where + (core,) + cut]
                at = list(where)
                at.insert(before.index(route[stage - 2]), bit(chip, route[stage - 2]))
                return R[w][stage - 2][(l,) + tuple(at) + cut]

            if stage == n + 1:
                emit(l, w, k, cut, buf[(l,) + cut] + mine(()))
                continue
            for i in range(2 ** len(left)):
                where = tuple((i >> j) & 1 for j in range(len(left)))
                at = (l,) + where + cut
                buf[at] = buf[at] + mine(where)
            a = route[stage - 1]
            src = buf.at[(l,) + pick(left, a, 1 - bit(chip, a)) + cut]
            rs_copy(l, w, k, stage, src, R[w][stage].at[(l,) + (ALL,) * (len(left) - 1) + cut],
                    dev(flip(chip, a), core))

    def emit(l, w, k, cut, total):
        if w == SM:
            os_ref[l] = total
            return
        total = total.astype(BF)
        if w != AO:
            (None, ou_ref, od_ref)[w][(l,) + cut] = total
        elif k == 0:
            oq_ref[(l,) + cut] = total
        else:
            n = Q3 - cut[1].start
            oq_ref[l, :, cut[1].start:] = total[:, :n]
            oo_ref[l] = total[:, n:]

    def s0(l, w):
        step(l, w, 0)

    def s1(l, w):
        step(l, w, 1)

    def s2(l, w):
        step(l, w, 2)

    def s3(l, w):
        step(l, w, 3)

    def s4(l, w):
        step(l, w, 4)

    def normed(h_bf):
        h32 = h_bf.astype(F32)
        cen = h32 - row_of(jnp.mean, h32)
        rstd = lax.rsqrt(row_of(jnp.mean, cen * cen) + EPSILON)
        return cen * rstd, rstd

    def norms(h_ref, l):
        xhat, _ = normed(h_ref[EV])
        n1 = (xhat * vec[l, 0:1, :] + vec[l, 1:2, :]).astype(BF)
        n2 = (xhat * vec[l, 3:4, :] + vec[l, 4:5, :]).astype(BF)
        na[EV] = n1
        nm[EV] = n2
        nat[l] = n1.T
        nmt[l] = n2.T

    def rope(xs, back, n):
        c, p, q = (rope_ref[t, :n] for t in range(3))
        if back:
            return xs * c + pltpu.roll(xs * p, 8, 1) + pltpu.roll(xs * q, 120, 1)
        return xs * c + pltpu.roll(xs, 120, 1) * p + pltpu.roll(xs, 8, 1) * q

    def make_qkv(l):
        for t in range(3):
            cols = slice(DM * t, DM * t + DM)
            raw = mm(na[EV], wa[l, :, cols]) + qkvb[l, :, cols]
            for s in range(4):
                part = raw[:, LN * s:LN * s + LN]
                if t < 2:
                    part = rope(part, False, TOK)
                qkv[l, :, DM * t + LN * s:DM * t + LN * s + LN] = part.astype(BF)

    def heads(l, bwd, lo, hi):
        lane = lax.broadcasted_iota(jnp.int32, (1, LN), 1)
        sides = [(lane < HD).astype(F32), (lane >= HD).astype(F32)]
        row, key = (lax.broadcasted_iota(jnp.int32, (TOK, SEQ), t) for t in range(2))
        causal = lax.rem(row, SEQ) >= key

        def stacked(v, scale):
            return jnp.concatenate([v * (side * scale).astype(BF) for side in sides])

        def along(v):
            return jnp.concatenate([v[:SEQ], v[SEQ:]], axis=1)

        def pair(seq, col):
            rows = slice(SEQ * seq, SEQ * seq + SEQ)
            q, k, v = (qkv[l, rows, pl.ds(col + DM * t, LN)] for t in range(3))
            qs = stacked(q, 0.125)
            sc = jnp.where(causal, mm_nt(qs, k), -1e30)
            e = jnp.exp(sc - row_of(jnp.max, sc))
            p = e * (1.0 / row_of(jnp.sum, e))
            pb = p.astype(BF)
            ctx[rows, pl.ds(col, LN)] = mm(along(pb), stacked(v, 1.0)).astype(BF)
            if not bwd:
                return
            ds_ = stacked(dctx[rows, pl.ds(col, LN)], 1.0)
            dp = mm_nt(ds_, v).astype(BF).astype(F32)
            ds = (p * (dp - row_of(jnp.sum, dp * p))).astype(BF)
            grads = (mm(along(ds), stacked(k, 0.125)), mm_tn(ds, qs), mm_tn(pb, ds_))
            for t, d in enumerate(grads):
                d = d.astype(BF).astype(F32)
                if t < 2:
                    d = rope(d, True, SEQ)
                if seq == 0:
                    gqb[0:1, pl.ds(col + DM * t, LN)] = col_sum(d)
                dqkv[rows, pl.ds(col + DM * t, LN)] = d.astype(BF)

        def body(j, carry):
            col = pl.multiple_of(j * LN, LN)
            for seq in range(2):
                pair(seq, col)
            return carry

        lax.fori_loop(lo, hi, body, 0)

    def up_part(l, t):
        col = pl.multiple_of(t * DM, DM)
        pre = mm(nm[EV], wu[l, :, pl.ds(col, DM)]) + upb[l, :, pl.ds(col, DM)]
        cdf = 0.5 * (1.0 + lax.erf(pre * 0.7071067811865476))
        return col, pre, cdf, (pre * cdf).astype(BF)

    def activate(l, fwd, lo, hi):
        def body(t, carry):
            col, pre, cdf, act = up_part(l, t)
            act_s[l, :, pl.ds(col, DM)] = act
            slope_s[l, :, pl.ds(col, DM)] = cdf + pre * (0.3989422804014327 * jnp.exp(-0.5 * pre * pre))
            if fwd:
                acc[EV] += mm(act, wd[l, pl.ds(col, DM), :])
            return carry

        if fwd and lo == 0:
            acc[EV] = jnp.zeros_like(acc)
        lax.fori_loop(lo, hi, body, 0)

    def down_grad(l, dout):
        def grad(t, carry):
            col = pl.multiple_of(node * 2 * DM + t * DM, DM)
            gd[t] = mm_tn(act_s[l, :, pl.ds(col, DM)], dout[EV]).reshape(2, 2, LN, DM)
            return carry

        lax.fori_loop(0, 2, grad, 0)

    def mlp_b(l, dout, fwd, lo, hi):
        def body(t, carry):
            col = pl.multiple_of(t * DM, DM)
            wd_t = wd[l, pl.ds(col, DM), :]
            if fwd:
                acc[:SEQ] += mm(act_s[l, :SEQ, pl.ds(col, DM)], wd_t)
            dpre = mm_nt(dout[EV], wd_t).astype(BF).astype(F32) * slope_s[l, :, pl.ds(col, DM)]
            gub[0:1, pl.ds(col, DM)] = col_sum(dpre[:SEQ])
            dpb = dpre.astype(BF)
            gu[:, :, :, :, pl.ds(col, DM)] = mm(nmt[l, zrows, :], dpb).reshape(2, 2, 2, SH, DM)
            dnm[EV] += mm_nt(dpb, wu[l, :, pl.ds(col, DM)])
            return carry

        if lo == 0:
            dnm[EV] = jnp.zeros_like(dnm)
            if fwd:
                acc[EV] = jnp.zeros_like(acc)
        lax.fori_loop(lo, hi, body, 0)

    def attn_grads(l, dout):
        ga[:, :, :, :, Q3:] = mm_tn(ctx[:, zrows], dout[EV]).reshape(2, 2, 2, SH, DM)
        for t in range(3):
            cols = slice(DM * t, DM * t + DM)
            ga[:, :, :, :, cols] = mm(nat[l, zrows, :], dqkv[:, cols]).reshape(2, 2, 2, SH, DM)

    def layer_end(h_ref, l, dout, n):
        dna = mm_nt(dqkv[:n], wa[l, :, 0:Q3]).astype(BF).astype(F32)
        dnm32 = dnm[:n].astype(BF).astype(F32)
        xhat, rstd = normed(h_ref[:n])
        d32 = dout[:n].astype(F32)
        own_tok = slice(0, SEQ)
        sums = [dna * xhat, dna, d32, dnm32 * xhat, dnm32, d32]
        for i, v in enumerate(sums):
            gvec[i:i + 1, :] = col_sum(v[own_tok])
        dx = dna * vec[l, 0:1, :] + dnm32 * vec[l, 3:4, :]
        dhid = rstd * (dx - row_of(jnp.mean, dx) - xhat * row_of(jnp.mean, dx * xhat))
        return (d32 + dhid).astype(BF)

    def small_grads():
        for d in range(ND):
            at = (d // 8, d // 4 % 2, d // 2 % 2, d % 2)
            gs[at] = jnp.zeros((8, LN), F32)
            gs[at + (slice(0, 6), slice(0, SH))] = gvec[0:6, SH * d:SH * d + SH]
            gs[at + (slice(6, 7), ALL)] = gub[0:1, LN * d:LN * d + LN]
            for lo, col, n in bias_parts(d):
                gs[at + (slice(7, 8), slice(lo, lo + n))] = gqb[0:1, col:col + n]

    def vectors():
        for d in range(ND):
            both = wa[0, SH * d:SH * d + 16, FF:].astype(F32)
            for l in range(LAYERS):
                rows = both[8 * l:8 * l + 8]
                vec[l, 0:6, SH * d:SH * d + SH] = rows[0:6, 0:SH]
                upb[l, 0:1, LN * d:LN * d + LN] = rows[6:7]
                for lo, col, n in bias_parts(d):
                    qkvb[l, 0:1, col:col + n] = rows[7:8, lo:lo + n]

    def bias_parts(d):
        base = HD * (d // 2)
        if d % 2 == 0:
            return ((0, base, HD), (HD, DM + base, SH))
        return ((0, DM + base + SH, SH), (SH, 1024 + base, HD))

    def swap(i, ref):
        return pltpu.make_async_remote_copy(src_ref=ref.at[pl.ds(0, SEQ)], dst_ref=ref.at[pl.ds(SEQ, SEQ)],
                                            send_sem=ex_send.at[i], recv_sem=ex_recv.at[i],
                                            device_id=dev(flip(chip, 4), core), device_id_type=MESH)

    swap_x, swap_cot = swap(0, x_ref), swap(1, cot_ref)
    (A0, U0, D0, V0), (A1, U1, D1, V1) = [[(l, w) for w in (AO, UP, DN, SM)] for l in range(LAYERS)]
    native_in = pltpu.make_async_copy(wq_in, native, loc_sem.at[0, 0])
    first = [pltpu.make_async_copy(wu_in.at[0], block(0, UP, chip, core), loc_sem.at[0, 1])]
    qo = pl.ds(pl.multiple_of(me * SH, SH), SH)
    rest = [pltpu.make_async_copy(wo_in.at[l], W[AO].at[l, qo, pl.ds(Q3, DM)], loc_sem.at[l + 2, 2])
            for l in range(LAYERS)]
    rest += [pltpu.make_async_copy(wd_in.at[l], block(l, DN, chip, core), loc_sem.at[l + 2, 3]) for l in range(LAYERS)]
    rest += [pltpu.make_async_copy(wu_in.at[1], block(1, UP, chip, core), loc_sem.at[0, 2]),
             pltpu.make_async_copy(x_in, x_ref.at[pl.ds(0, SEQ)], loc_sem.at[0, 3]),
             pltpu.make_async_copy(cot_in, cot_ref.at[pl.ds(0, SEQ)], loc_sem.at[1, 0]),
             pltpu.make_async_copy(rope_in, rope_ref.at[:, pl.ds(0, SEQ)], loc_sem.at[1, 1]),
             pltpu.make_async_copy(rope_in, rope_ref.at[:, pl.ds(SEQ, SEQ)], loc_sem.at[1, 2])]
    params, tmp = (p0, p1, p2, p3, p4, p5, p6, p7), (v0, v1, v2, v3, v4, v5, v6, v7)
    little = [pltpu.make_async_copy(params[i], tmp[i], loc_sem.at[4 + i // 4, i % 4]) for i in range(8)]
    first[0].start()
    native_in.start()
    for cp in little + rest:
        cp.start()

    barrier = pltpu.get_barrier_semaphore()
    near = [dev(chip, other)] + [dev(flip(chip, a), core) for a in CHIP_AXES]
    for to in near:
        pl.semaphore_signal(barrier, inc=1, device_id=to, device_id_type=MESH)
    first[0].wait()
    pl.semaphore_wait(barrier, len(near))
    own(*U0)

    native_in.wait()
    for l in range(LAYERS):
        flat = native[l].astype(F32).reshape(SEQ, 3 * HD)
        spread[0] = flat[:, :LN]
        spread[1, :, :HD] = flat[:, LN:]
        for h in range(8):
            rows = [spread[i, pl.ds(h, SH, stride=8), :].astype(BF) for i in range(2)]
            for t in range(3):
                lo = HD * (t % 2)
                wa[l, qo, DM * t + HD * h:DM * t + HD * h + HD] = rows[t // 2][:, lo:lo + HD]
        if l == 0:
            for cp in little + rest:
                cp.wait()
            spread[0, 0:SH] = jnp.zeros((SH, LN), F32)
            for i in range(8):
                for m in range(LAYERS):
                    spread[0, 8 * m + i:8 * m + i + 1, 0:tmp[i].shape[1]] = tmp[i][m:m + 1, :].astype(F32)
            wa[0, qo, FF:] = spread[0, 0:SH].astype(BF)
            own(*A0)
    swap_x.start()
    f1(*A0)
    f1(*U0)
    f2(*A0)
    own(*D0)
    f2(*U0)
    f3(*A0)
    f3(*U0)
    f1(*D0)
    f4(*A0)
    own(*U1)
    f4(*U0)
    got_partner(*A0)
    vectors()
    swap_x.wait_recv()
    norms(x_ref, 0)
    f2(*D0)
    make_qkv(0)
    f3(*D0)
    heads(0, False, 0, 1)
    f1(*U1)
    heads(0, False, 1, 2)
    f2(*U1)
    own(*A1)
    heads(0, False, 2, 4)
    f4(*D0)
    got_partner(*U0)
    got_partner(*D0)
    swap_cot.start()
    activate(0, True, 0, 2)
    f3(*U1)
    f1(*A1)
    activate(0, True, 2, 4)
    own(*D1)
    acc[EV] += mm(ctx[EV], wa[0, :, Q3:FF])
    h1[EV] = (x_ref[EV].astype(F32) + acc[EV] + vec[0, 2:3, :] + vec[0, 5:6, :]).astype(BF)
    f4(*U1)
    f2(*A1)
    norms(h1, 1)
    got_partner(*U1)
    activate(1, False, 0, 4)
    swap_cot.wait_recv()
    down_grad(1, cot_ref)
    s0(*D1)
    f3(*A1)
    f1(*D1)
    f4(*A1)
    s1(*D1)
    f2(*D1)
    got_partner(*A1)
    make_qkv(1)
    dctx[EV] = mm_nt(cot_ref[EV], wa[1, :, Q3:FF]).astype(BF)
    f3(*D1)
    heads(1, True, 0, 2)
    f4(*D1)
    heads(1, True, 2, 3)
    s2(*D1)
    heads(1, True, 3, 4)
    attn_grads(1, cot_ref)
    s0(*A1)
    got_partner(*D1)
    mlp_b(1, cot_ref, True, 0, 2)
    s1(*A1)
    mlp_b(1, cot_ref, True, 2, 4)
    s0(*U1)
    dh[EV] = layer_end(h1, 1, cot_ref, TOK)
    s1(*U1)
    acc[:SEQ] += mm(ctx[:SEQ], wa[1, :, Q3:FF])
    y_ref[EV] = (h1[:SEQ].astype(F32) + acc[:SEQ] + vec[1, 2:3, :] + vec[1, 5:6, :]).astype(BF)
    small_grads()
    s0(*V1)

    drained(*D1, 0)
    down_grad(0, dh)
    s0(*D0)
    drained(*U1, 0)
    mlp_b(0, dh, False, 0, 2)
    s1(*D0)
    s2(*A1)
    mlp_b(0, dh, False, 2, 4)
    s0(*U0)
    s1(*V1)
    dctx[EV] = mm_nt(dh[EV], wa[0, :, Q3:FF]).astype(BF)
    s1(*U0)
    heads(0, True, 0, 2)
    s2(*U1)
    s2(*V1)
    s2(*D0)
    heads(0, True, 2, 4)
    xg_ref[EV] = layer_end(x_ref, 0, dh, SEQ)
    drained(*V1, 0)
    small_grads()
    s0(*V0)
    drained(*A1, 0)
    attn_grads(0, dh)
    s0(*A0)
    s1(*V0)
    s3(*V1)
    s1(*A0)
    for stage, at in ((s2, V0), (s2, U0), (s3, D1), (s3, A1), (s3, V0), (s2, A0), (s3, U1), (s4, V1), (s3, D0),
                      (s3, U0), (s4, V0), (s3, A0)):
        stage(*at)
    swap_x.wait_send()
    swap_cot.wait_send()
    for w in (DN, UP, AO, SM):
        drained(0, w, 0)
        for l in range(LAYERS):
            if w != SM:
                sent(l, w)
            for stage in range(1, len(axes_of(w)) + 1):
                drained(l, w, stage)


def finish(y, xg, oq, oo, ou, od, osm, *outs):
    *outs, spread = outs
    yo, xo, g1, b1, gq, bq, go, bo, g2, b2, gup, bu, gdn, bd = outs
    yo[0] = y[EV]
    xo[0] = xg[EV]
    go[EV] = oo[EV]
    gup[EV] = ou[EV]
    gdn[EV] = od[EV]
    for row, ref in enumerate((g1, b1, bo, g2, b2, bd, bu, bq)):
        for l in range(LAYERS):
            ref[l:l + 1, :] = osm[l, row:row + 1, 0:ref.shape[1]].astype(BF)
    for l in range(LAYERS):
        for h in range(8):
            q, k, v = (oq[l, :, DM * t + HD * h:DM * t + HD * h + HD].astype(F32) for t in range(3))
            spread[0, pl.ds(h, SH, stride=8), :] = jnp.concatenate([q, k], axis=1)
            spread[1, pl.ds(h, SH, stride=8), :] = jnp.concatenate([v, v], axis=1)
        gq[l, :, :, :LN] = spread[0].reshape(SH, 8, LN).astype(BF)
        gq[l, :, :, LN:] = spread[1, :, :HD].reshape(SH, 8, HD).astype(BF)


def rope_constants():
    rot, half, hd = 16, 8, HD
    inv = (1.0 / (10000.0 ** (np.arange(0, rot, 2, dtype=np.float32) / np.float32(rot)))).astype(np.float32)
    ang = np.arange(SEQ, dtype=np.float32)[:, None] * inv[None, :]
    cos, sin = np.cos(ang).astype(np.float32), np.sin(ang).astype(np.float32)
    c = np.ones((SEQ, LN), np.float32)
    p = np.zeros((SEQ, LN), np.float32)
    q = np.zeros((SEQ, LN), np.float32)
    for base in (0, hd):
        c[:, base:base + half] = cos
        c[:, base + half:base + rot] = cos
        p[:, base:base + half] = -sin
        q[:, base + half:base + rot] = sin
    return np.stack([c, p, q])


def solution(mesh):
    shard_axes = ('node', 'local')
    act_spec = P(shard_axes)
    param_spec = P(None, shard_axes)
    consts = rope_constants()
    vm = pl.BlockSpec(memory_space=pltpu.VMEM)
    hbm = pl.BlockSpec(memory_space=pl.ANY)

    def device_step(x, y_cot, g1, b1, wqkv, bqkv, wout, bout, g2, b2, wup, bup, wdn, bdn):
        little = (g1, b1, bout, g2, b2, bdn, bup, bqkv)

        def v(shape, dt):
            return pltpu.VMEM(shape, dt)

        wshape = [(LAYERS, ND * ROWS[w], WIDTH if w == AO else COLS[w]) for w in range(3)]
        scratch = [v(wshape[w], BF) for w in range(3)]
        scratch += [v((2,) * (len(axes_of(w)) + 1) + (ROWS[w], COLS[w]), F32) for w in range(4)]
        for w in range(4):
            n = len(axes_of(w))
            scratch += [v((LAYERS,) + (2,) * (n - i) + (ROWS[w], COLS[w]), F32) for i in range(n + 1)]
        scratch += [v(p.shape, BF) for p in little]
        scratch += [v((LAYERS, 8, DM), F32), v((LAYERS, 1, FF), F32), v((LAYERS, 1, Q3), F32),
                    v((8, DM), F32), v((1, FF), F32), v((1, Q3), F32)]
        scratch += [v((TOK, DM), BF)] * 2
        scratch += [v((3, TOK, LN), F32), v((LAYERS, SH, 8, 3 * HD), BF), v((2, SEQ, LN), F32), v((LAYERS, TOK, FF), BF),
                    v((LAYERS, TOK, FF), F32)]
        scratch += [v((TOK, DM), BF)] * 4 + [v((LAYERS, DM, TOK), BF)] * 2 + [v((LAYERS, TOK, Q3), BF), v((TOK, Q3), BF)]
        scratch += [v((TOK, DM), BF)] * 2 + [v((TOK, DM), F32)] * 2
        dma = pltpu.SemaphoreType.DMA
        scratch += [dma((6, 4)), dma((LAYERS, 3)), dma((LAYERS, 3, 3, 8)), dma((LAYERS, 3)), dma((LAYERS, 4, 3, 4)),
                    dma((LAYERS, 4, 3, 4)), dma((2,)), dma((2,))]
        sds = jax.ShapeDtypeStruct
        mids = pl.pallas_call(
            kernel,
            out_shape=[sds((SEQ, DM), BF), sds((SEQ, DM), BF), sds((LAYERS, SH, Q3), BF), sds((LAYERS, SH, DM), BF),
                       sds((LAYERS, SH, FF), BF), sds((LAYERS, LN, DM), BF), sds((LAYERS, 8, LN), F32)],
            in_specs=[hbm] * 15,
            out_specs=[vm] * 7,
            scratch_shapes=scratch,
            compiler_params=pltpu.CompilerParams(has_side_effects=True, collective_id=0, vmem_limit_bytes=67043328),
            name='step',
        )(x[0], y_cot[0], wqkv, wout, wup, wdn, *little, consts)
        y, xg, oq, oo, ou, od, osm = mids
        like = (x, y_cot, g1, b1, wqkv, bqkv, wout, bout, g2, b2, wup, bup, wdn, bdn)
        return pl.pallas_call(finish, out_shape=[sds(p.shape, BF) for p in like], in_specs=[vm] * 7,
                              out_specs=[vm] * 14, scratch_shapes=[v((2, SEQ, LN), F32)],
                              name='finish')(y, xg, oq, oo, ou, od, osm)

    return jax.shard_map(device_step, mesh=mesh,
                         in_specs=(act_spec, act_spec) + (param_spec,) * 12,
                         out_specs=(act_spec, act_spec) + (param_spec,) * 12,
                         check_vma=False)
```

```python
import numpy as np
import jax
import jax.numpy as jnp
from jax import lax
from jax.experimental import pallas as pl
from jax.experimental.pallas import tpu as pltpu
from jax.sharding import PartitionSpec as P

BF, F32 = jnp.bfloat16, jnp.float32
MESH = pl.DeviceIdType.MESH
EPSILON = 1e-5
LAYERS, SEQ, DM, FF, ND = 2, 256, 512, 2048, 16
SH, HD, LN, Q3 = 32, 64, 128, 1536
ROWS = (SH, SH, LN, 8)
COLS = (FF, FF, DM, LN)
WIDTH = FF + LN
AO, UP, DN, SM = range(4)
ORDERS = ((1, 2, 4), (2, 4, 1), (4, 1, 2))
CHIP_AXES = [4, 2, 1]
CUTS = ((0, 256, 1024, FF), (0, 256, 1024, FF), (0, SH, 80, LN))
WIDE = (0, 256, 1024, WIDTH)
ROUTES = ((1, 2), (2, 1))
ALL, EV = slice(None), ...
TOK = 2 * SEQ


def routes(w):
    return ORDERS[2:] if w == SM else ROUTES


def axes_of(w):
    return CHIP_AXES if w == SM else CHIP_AXES[1:]


def piece(w, k):
    if w == SM:
        return ALL, ALL
    n = (ROWS if w == DN else COLS)[w] // 2
    part = slice(n * k, n * k + n)
    return (part, ALL) if w == DN else (ALL, part)


def bit(v, a):
    return lax.rem(lax.div(v, a), 2)


def flip(v, mask):
    for a in (1, 2, 4):
        if mask & a:
            v = v + a - 2 * a * bit(v, a)
    return v


def col_sum(v):
    return jnp.sum(v, axis=0, keepdims=True)


def row_of(f, v):
    return f(v, axis=-1, keepdims=True)


def mm(a, b):
    return jnp.dot(a, b, preferred_element_type=F32)


def mm_nt(a, b):
    return lax.dot_general(a, b, (((1,), (1,)), ((), ())), preferred_element_type=F32)


def mm_tn(a, b):
    return lax.dot_general(a, b, (((0,), (0,)), ((), ())), preferred_element_type=F32)


def kernel(x_in, cot_in, wq_in, wo_in, wu_in, wd_in, p0, p1, p2, p3, p4, p5, p6, p7, rope_in,
           y_ref, xg_ref, oq_ref, oo_ref, ou_ref, od_ref, os_ref,
           wa, wu, wd, ga, gu, gd, gs, ra0, ra1, ra2, ru0, ru1, ru2, rd0, rd1, rd2, rs0, rs1, rs2, rs3,
           v0, v1, v2, v3, v4, v5, v6, v7, vec, upb, qkvb, gvec, gub, gqb,
           x_ref, cot_ref, rope_ref, native, spread, act_s, slope_s,
           h1, dh, na, nm, nat, nmt, qkv, dqkv, ctx, dctx, acc, dnm,
           loc_sem, ag_send, ag_ici, ag_d2d, rs_send, rs_recv, ex_send, ex_recv):
    me = lax.axis_index('node') * 8 + lax.axis_index('local')
    chip = lax.div(me, 2)
    core = lax.rem(me, 2)
    other = 1 - core
    W, G = (wa, wu, wd), (ga, gu, gd, gs)
    R = ((ra0, ra1, ra2), (ru0, ru1, ru2), (rd0, rd1, rd2), (rs0, rs1, rs2, rs3))
    node = lax.div(chip, 4)
    zrows = pl.ds(pl.multiple_of(node * SEQ, SEQ), SEQ)

    def dev(c, k):
        i = c * 2 + k
        return (lax.div(i, 8), lax.rem(i, 8))

    def rows_of(l, w, start, n):
        rows = pl.ds(start, n * ROWS[w])
        if w == AO and l == 1:
            return W[w].at[l, rows, pl.ds(0, FF)]
        return W[w].at[l, rows]

    def block(l, w, c, k):
        return rows_of(l, w, pl.multiple_of((c * 2 + k) * ROWS[w], ROWS[w]), 1)

    def part(l, w, k, mask):
        base = (flip(chip, mask) * 2 + core) * ROWS[w]
        cuts = WIDE if w == AO and l == 0 else CUTS[w]
        lo, hi = cuts[k], cuts[k + 1]
        if w == DN:
            return W[w].at[l, pl.ds(pl.multiple_of(base + lo, 16), hi - lo)]
        return W[w].at[l, pl.ds(pl.multiple_of(base, SH), SH), lo:hi]

    def push(l, w, src, to, recv_sem):
        pltpu.make_async_remote_copy(src_ref=src, dst_ref=src, send_sem=ag_send.at[l, w], recv_sem=recv_sem,
                                     device_id=to, device_id_type=MESH).start()

    def to_link(l, w, k, mask, a):
        push(l, w, part(l, w, k, mask), dev(flip(chip, a), core), ag_ici.at[l, w, k, mask ^ a])

    def to_partner(l, w, k, mask):
        push(l, w, part(l, w, k, mask), dev(chip, other), ag_d2d.at[l, w])

    def await_in(l, w, src, recv_sem):
        pltpu.make_async_remote_copy(src_ref=src, dst_ref=src, send_sem=ag_send.at[l, w], recv_sem=recv_sem,
                                     device_id=dev(chip, other), device_id_type=MESH).wait_recv()

    def got(l, w, k, mask):
        await_in(l, w, part(l, w, k, mask), ag_ici.at[l, w, k, mask])

    def got_partner(l, w):
        await_in(l, w, rows_of(l, w, 0, 8), ag_d2d.at[l, w])

    def sent(l, w):
        src = rows_of(l, w, 0, 15)
        pltpu.make_async_remote_copy(src_ref=src, dst_ref=src, send_sem=ag_send.at[l, w], recv_sem=ag_d2d.at[l, w],
                                     device_id=dev(chip, other), device_id_type=MESH).wait_send()

    def own(l, w):
        for i in range(3):
            for k in range(3):
                to_link(l, w, k, 0, ORDERS[k][i])
        push(l, w, block(l, w, chip, core), dev(chip, other), ag_d2d.at[l, w])

    def f1(l, w):
        for k, (a, b, c) in enumerate(ORDERS):
            got(l, w, k, a)
            to_link(l, w, k, a, b)
        for k, (a, b, c) in enumerate(ORDERS):
            to_link(l, w, k, a, c)
            to_partner(l, w, k, a)

    def f2(l, w):
        for k, (a, b, c) in enumerate(ORDERS):
            got(l, w, k, b)
            to_link(l, w, k, b, c)
            to_partner(l, w, k, b)

    def f3(l, w):
        for k, (a, b, c) in enumerate(ORDERS):
            got(l, w, k, a | b)
            to_link(l, w, k, a | b, c)
            to_partner(l, w, k, a | b)

    def f4(l, w):
        for i in range(4):
            for k, (a, b, c) in enumerate(ORDERS):
                m = (c, a | c, b | c, 7)[i]
                got(l, w, k, m)
                to_partner(l, w, k, m)

    rs = {}

    def rs_copy(l, w, k, stage, src, dst, to):
        cp = pltpu.make_async_remote_copy(src_ref=src, dst_ref=dst, send_sem=rs_send.at[l, w, k, stage],
                                          recv_sem=rs_recv.at[l, w, k, stage], device_id=to, device_id_type=MESH)
        cp.start()
        rs[l, w, k, stage] = cp

    def pick(axes, a, v):
        return tuple(v if m == a else ALL for m in axes)

    def drained(l, w, stage):
        for k in range(len(routes(w))):
            rs[l, w, k, stage].wait_send()

    def step(l, w, stage):
        axes = axes_of(w)
        n = len(axes)
        for k, route in enumerate(routes(w)):
            cut = piece(w, k)
            if stage == 0:
                rs_copy(l, w, k, 0, G[w].at[(ALL,) * n + (other,) + cut], R[w][0].at[(l,) + (ALL,) * n + cut],
                        dev(chip, other))
                continue
            rs[l, w, k, stage - 1].wait_recv()
            buf = R[w][stage - 1]
            left = [m for m in axes if m not in route[:stage - 1]]
            before = [m for m in axes if m not in route[:stage - 2]] if stage > 1 else axes

            def mine(where):
                if stage == 1:
                    return G[w][where + (core,) + cut]
                at = list(where)
                at.insert(before.index(route[stage - 2]), bit(chip, route[stage - 2]))
                return R[w][stage - 2][(l,) + tuple(at) + cut]

            if stage == n + 1:
                emit(l, w, k, cut, buf[(l,) + cut] + mine(()))
                continue
            for i in range(2 ** len(left)):
                where = tuple((i >> j) & 1 for j in range(len(left)))
                at = (l,) + where + cut
                buf[at] = buf[at] + mine(where)
            a = route[stage - 1]
            src = buf.at[(l,) + pick(left, a, 1 - bit(chip, a)) + cut]
            rs_copy(l, w, k, stage, src, R[w][stage].at[(l,) + (ALL,) * (len(left) - 1) + cut],
                    dev(flip(chip, a), core))

    def emit(l, w, k, cut, total):
        if w == SM:
            os_ref[l] = total
            return
        total = total.astype(BF)
        if w != AO:
            (None, ou_ref, od_ref)[w][(l,) + cut] = total
        elif k == 0:
            oq_ref[(l,) + cut] = total
        else:
            n = Q3 - cut[1].start
            oq_ref[l, :, cut[1].start:] = total[:, :n]
            oo_ref[l] = total[:, n:]

    def s0(l, w):
        step(l, w, 0)

    def s1(l, w):
        step(l, w, 1)

    def s2(l, w):
        step(l, w, 2)

    def s3(l, w):
        step(l, w, 3)

    def s4(l, w):
        step(l, w, 4)

    def normed(h_bf):
        h32 = h_bf.astype(F32)
        cen = h32 - row_of(jnp.mean, h32)
        rstd = lax.rsqrt(row_of(jnp.mean, cen * cen) + EPSILON)
        return cen * rstd, rstd

    def norms(h_ref, l):
        xhat, _ = normed(h_ref[EV])
        n1 = (xhat * vec[l, 0:1, :] + vec[l, 1:2, :]).astype(BF)
        n2 = (xhat * vec[l, 3:4, :] + vec[l, 4:5, :]).astype(BF)
        na[EV] = n1
        nm[EV] = n2
        nat[l] = n1.T
        nmt[l] = n2.T

    def rope(xs, back, n):
        c, p, q = (rope_ref[t, :n] for t in range(3))
        if back:
            return xs * c + pltpu.roll(xs * p, 8, 1) + pltpu.roll(xs * q, 120, 1)
        return xs * c + pltpu.roll(xs, 120, 1) * p + pltpu.roll(xs, 8, 1) * q

    def make_qkv(l):
        for t in range(3):
            cols = slice(DM * t, DM * t + DM)
            raw = mm(na[EV], wa[l, :, cols]) + qkvb[l, :, cols]
            for s in range(4):
                part = raw[:, LN * s:LN * s + LN]
                if t < 2:
                    part = rope(part, False, TOK)
                qkv[l, :, DM * t + LN * s:DM * t + LN * s + LN] = part.astype(BF)

    def heads(l, bwd, lo, hi):
        lane = lax.broadcasted_iota(jnp.int32, (1, LN), 1)
        sides = [(lane < HD).astype(F32), (lane >= HD).astype(F32)]
        row, key = (lax.broadcasted_iota(jnp.int32, (TOK, SEQ), t) for t in range(2))
        causal = lax.rem(row, SEQ) >= key

        def stacked(v, scale):
            return jnp.concatenate([v * (side * scale).astype(BF) for side in sides])

        def along(v):
            return jnp.concatenate([v[:SEQ], v[SEQ:]], axis=1)

        def pair(seq, col):
            rows = slice(SEQ * seq, SEQ * seq + SEQ)
            q, k, v = (qkv[l, rows, pl.ds(col + DM * t, LN)] for t in range(3))
            qs = stacked(q, 0.125)
            sc = jnp.where(causal, mm_nt(qs, k), -1e30)
            e = jnp.exp(sc - row_of(jnp.max, sc))
            p = e * (1.0 / row_of(jnp.sum, e))
            pb = p.astype(BF)
            ctx[rows, pl.ds(col, LN)] = mm(along(pb), stacked(v, 1.0)).astype(BF)
            if not bwd:
                return
            ds_ = stacked(dctx[rows, pl.ds(col, LN)], 1.0)
            dp = mm_nt(ds_, v).astype(BF).astype(F32)
            ds = (p * (dp - row_of(jnp.sum, dp * p))).astype(BF)
            grads = (mm(along(ds), stacked(k, 0.125)), mm_tn(ds, qs), mm_tn(pb, ds_))
            for t, d in enumerate(grads):
                d = d.astype(BF).astype(F32)
                if t < 2:
                    d = rope(d, True, SEQ)
                if seq == 0:
                    gqb[0:1, pl.ds(col + DM * t, LN)] = col_sum(d)
                dqkv[rows, pl.ds(col + DM * t, LN)] = d.astype(BF)

        def body(j, carry):
            col = pl.multiple_of(j * LN, LN)
            for seq in range(2):
                pair(seq, col)
            return carry

        lax.fori_loop(lo, hi, body, 0)

    def up_part(l, t):
        col = pl.multiple_of(t * DM, DM)
        pre = mm(nm[EV], wu[l, :, pl.ds(col, DM)]) + upb[l, :, pl.ds(col, DM)]
        cdf = 0.5 * (1.0 + lax.erf(pre * 0.7071067811865476))
        return col, pre, cdf, (pre * cdf).astype(BF)

    def activate(l, fwd, lo, hi):
        def body(t, carry):
            col, pre, cdf, act = up_part(l, t)
            act_s[l, :, pl.ds(col, DM)] = act
            slope_s[l, :, pl.ds(col, DM)] = cdf + pre * (0.3989422804014327 * jnp.exp(-0.5 * pre * pre))
            if fwd:
                acc[EV] += mm(act, wd[l, pl.ds(col, DM), :])
            return carry

        if fwd and lo == 0:
            acc[EV] = jnp.zeros_like(acc)
        lax.fori_loop(lo, hi, body, 0)

    def down_grad(l, dout):
        def grad(t, carry):
            col = pl.multiple_of(node * 2 * DM + t * DM, DM)
            gd[t] = mm_tn(act_s[l, :, pl.ds(col, DM)], dout[EV]).reshape(2, 2, LN, DM)
            return carry

        lax.fori_loop(0, 2, grad, 0)

    def mlp_b(l, dout, fwd, lo, hi):
        def body(t, carry):
            col = pl.multiple_of(t * DM, DM)
            wd_t = wd[l, pl.ds(col, DM), :]
            if fwd:
                acc[:SEQ] += mm(act_s[l, :SEQ, pl.ds(col, DM)], wd_t)
            dpre = mm_nt(dout[EV], wd_t).astype(BF).astype(F32) * slope_s[l, :, pl.ds(col, DM)]
            gub[0:1, pl.ds(col, DM)] = col_sum(dpre[:SEQ])
            dpb = dpre.astype(BF)
            gu[:, :, :, :, pl.ds(col, DM)] = mm(nmt[l, zrows, :], dpb).reshape(2, 2, 2, SH, DM)
            dnm[EV] += mm_nt(dpb, wu[l, :, pl.ds(col, DM)])
            return carry

        if lo == 0:
            dnm[EV] = jnp.zeros_like(dnm)
            if fwd:
                acc[EV] = jnp.zeros_like(acc)
        lax.fori_loop(lo, hi, body, 0)

    def attn_grads(l, dout):
        ga[:, :, :, :, Q3:] = mm_tn(ctx[:, zrows], dout[EV]).reshape(2, 2, 2, SH, DM)
        for t in range(3):
            cols = slice(DM * t, DM * t + DM)
            ga[:, :, :, :, cols] = mm(nat[l, zrows, :], dqkv[:, cols]).reshape(2, 2, 2, SH, DM)

    def layer_end(h_ref, l, dout, n):
        dna = mm_nt(dqkv[:n], wa[l, :, 0:Q3]).astype(BF).astype(F32)
        dnm32 = dnm[:n].astype(BF).astype(F32)
        xhat, rstd = normed(h_ref[:n])
        d32 = dout[:n].astype(F32)
        own_tok = slice(0, SEQ)
        sums = [dna * xhat, dna, d32, dnm32 * xhat, dnm32, d32]
        for i, v in enumerate(sums):
            gvec[i:i + 1, :] = col_sum(v[own_tok])
        dx = dna * vec[l, 0:1, :] + dnm32 * vec[l, 3:4, :]
        dhid = rstd * (dx - row_of(jnp.mean, dx) - xhat * row_of(jnp.mean, dx * xhat))
        return (d32 + dhid).astype(BF)

    def small_grads():
        for d in range(ND):
            at = (d // 8, d // 4 % 2, d // 2 % 2, d % 2)
            gs[at] = jnp.zeros((8, LN), F32)
            gs[at + (slice(0, 6), slice(0, SH))] = gvec[0:6, SH * d:SH * d + SH]
            gs[at + (slice(6, 7), ALL)] = gub[0:1, LN * d:LN * d + LN]
            for lo, col, n in bias_parts(d):
                gs[at + (slice(7, 8), slice(lo, lo + n))] = gqb[0:1, col:col + n]

    def vectors():
        for d in range(ND):
            both = wa[0, SH * d:SH * d + 16, FF:].astype(F32)
            for l in range(LAYERS):
                rows = both[8 * l:8 * l + 8]
                vec[l, 0:6, SH * d:SH * d + SH] = rows[0:6, 0:SH]
                upb[l, 0:1, LN * d:LN * d + LN] = rows[6:7]
                for lo, col, n in bias_parts(d):
                    qkvb[l, 0:1, col:col + n] = rows[7:8, lo:lo + n]

    def bias_parts(d):
        base = HD * (d // 2)
        if d % 2 == 0:
            return ((0, base, HD), (HD, DM + base, SH))
        return ((0, DM + base + SH, SH), (SH, 1024 + base, HD))

    def swap(i, ref):
        return pltpu.make_async_remote_copy(src_ref=ref.at[pl.ds(0, SEQ)], dst_ref=ref.at[pl.ds(SEQ, SEQ)],
                                            send_sem=ex_send.at[i], recv_sem=ex_recv.at[i],
                                            device_id=dev(flip(chip, 4), core), device_id_type=MESH)

    swap_x, swap_cot = swap(0, x_ref), swap(1, cot_ref)
    (A0, U0, D0, V0), (A1, U1, D1, V1) = [[(l, w) for w in (AO, UP, DN, SM)] for l in range(LAYERS)]
    native_in = pltpu.make_async_copy(wq_in, native, loc_sem.at[0, 0])
    first = [pltpu.make_async_copy(wu_in.at[0], block(0, UP, chip, core), loc_sem.at[0, 1])]
    qo = pl.ds(pl.multiple_of(me * SH, SH), SH)
    rest = [pltpu.make_async_copy(wo_in.at[l], W[AO].at[l, qo, pl.ds(Q3, DM)], loc_sem.at[l + 2, 2])
            for l in range(LAYERS)]
    rest += [pltpu.make_async_copy(wd_in.at[l], block(l, DN, chip, core), loc_sem.at[l + 2, 3]) for l in range(LAYERS)]
    rest += [pltpu.make_async_copy(wu_in.at[1], block(1, UP, chip, core), loc_sem.at[0, 2]),
             pltpu.make_async_copy(x_in, x_ref.at[pl.ds(0, SEQ)], loc_sem.at[0, 3]),
             pltpu.make_async_copy(cot_in, cot_ref.at[pl.ds(0, SEQ)], loc_sem.at[1, 0]),
             pltpu.make_async_copy(rope_in, rope_ref.at[:, pl.ds(0, SEQ)], loc_sem.at[1, 1]),
             pltpu.make_async_copy(rope_in, rope_ref.at[:, pl.ds(SEQ, SEQ)], loc_sem.at[1, 2])]
    params, tmp = (p0, p1, p2, p3, p4, p5, p6, p7), (v0, v1, v2, v3, v4, v5, v6, v7)
    little = [pltpu.make_async_copy(params[i], tmp[i], loc_sem.at[4 + i // 4, i % 4]) for i in range(8)]
    first[0].start()
    native_in.start()
    for cp in little + rest:
        cp.start()

    barrier = pltpu.get_barrier_semaphore()
    near = [dev(chip, other)] + [dev(flip(chip, a), core) for a in CHIP_AXES]
    for to in near:
        pl.semaphore_signal(barrier, inc=1, device_id=to, device_id_type=MESH)
    first[0].wait()
    pl.semaphore_wait(barrier, len(near))
    own(*U0)

    native_in.wait()
    for l in range(LAYERS):
        flat = native[l].astype(F32).reshape(SEQ, 3 * HD)
        spread[0] = flat[:, :LN]
        spread[1, :, :HD] = flat[:, LN:]
        for h in range(8):
            rows = [spread[i, pl.ds(h, SH, stride=8), :].astype(BF) for i in range(2)]
            for t in range(3):
                lo = HD * (t % 2)
                wa[l, qo, DM * t + HD * h:DM * t + HD * h + HD] = rows[t // 2][:, lo:lo + HD]
        if l == 0:
            for cp in little + rest:
                cp.wait()
            spread[0, 0:SH] = jnp.zeros((SH, LN), F32)
            for i in range(8):
                for m in range(LAYERS):
                    spread[0, 8 * m + i:8 * m + i + 1, 0:tmp[i].shape[1]] = tmp[i][m:m + 1, :].astype(F32)
            wa[0, qo, FF:] = spread[0, 0:SH].astype(BF)
            own(*A0)
    swap_x.start()
    f1(*A0)
    f1(*U0)
    f2(*A0)
    own(*D0)
    f2(*U0)
    f3(*A0)
    f3(*U0)
    f1(*D0)
    f4(*A0)
    own(*U1)
    f4(*U0)
    got_partner(*A0)
    vectors()
    swap_x.wait_recv()
    norms(x_ref, 0)
    f2(*D0)
    make_qkv(0)
    f3(*D0)
    heads(0, False, 0, 1)
    f1(*U1)
    heads(0, False, 1, 2)
    f2(*U1)
    own(*A1)
    heads(0, False, 2, 4)
    f4(*D0)
    got_partner(*U0)
    got_partner(*D0)
    swap_cot.start()
    activate(0, True, 0, 2)
    f3(*U1)
    f1(*A1)
    activate(0, True, 2, 4)
    own(*D1)
    acc[EV] += mm(ctx[EV], wa[0, :, Q3:FF])
    h1[EV] = (x_ref[EV].astype(F32) + acc[EV] + vec[0, 2:3, :] + vec[0, 5:6, :]).astype(BF)
    f4(*U1)
    f2(*A1)
    norms(h1, 1)
    got_partner(*U1)
    activate(1, False, 0, 4)
    swap_cot.wait_recv()
    down_grad(1, cot_ref)
    s0(*D1)
    f3(*A1)
    f1(*D1)
    f4(*A1)
    s1(*D1)
    f2(*D1)
    got_partner(*A1)
    make_qkv(1)
    dctx[EV] = mm_nt(cot_ref[EV], wa[1, :, Q3:FF]).astype(BF)
    f3(*D1)
    heads(1, True, 0, 2)
    f4(*D1)
    heads(1, True, 2, 3)
    s2(*D1)
    heads(1, True, 3, 4)
    attn_grads(1, cot_ref)
    s0(*A1)
    got_partner(*D1)
    mlp_b(1, cot_ref, True, 0, 2)
    s1(*A1)
    mlp_b(1, cot_ref, True, 2, 4)
    s0(*U1)
    dh[EV] = layer_end(h1, 1, cot_ref, TOK)
    s1(*U1)
    acc[:SEQ] += mm(ctx[:SEQ], wa[1, :, Q3:FF])
    y_ref[EV] = (h1[:SEQ].astype(F32) + acc[:SEQ] + vec[1, 2:3, :] + vec[1, 5:6, :]).astype(BF)
    small_grads()
    s0(*V1)

    drained(*D1, 0)
    down_grad(0, dh)
    s0(*D0)
    drained(*U1, 0)
    mlp_b(0, dh, False, 0, 2)
    s1(*D0)
    s2(*A1)
    mlp_b(0, dh, False, 2, 4)
    s0(*U0)
    s1(*V1)
    dctx[EV] = mm_nt(dh[EV], wa[0, :, Q3:FF]).astype(BF)
    s1(*U0)
    heads(0, True, 0, 2)
    s2(*U1)
    s2(*V1)
    s2(*D0)
    heads(0, True, 2, 4)
    xg_ref[EV] = layer_end(x_ref, 0, dh, SEQ)
    drained(*V1, 0)
    small_grads()
    s0(*V0)
    drained(*A1, 0)
    attn_grads(0, dh)
    s0(*A0)
    s1(*V0)
    s3(*V1)
    s1(*A0)
    for stage, at in ((s2, V0), (s2, U0), (s3, D1), (s3, A1), (s3, V0), (s2, A0), (s3, U1), (s4, V1), (s3, D0),
                      (s3, U0), (s4, V0), (s3, A0)):
        stage(*at)
    swap_x.wait_send()
    swap_cot.wait_send()
    for w in (DN, UP, AO, SM):
        drained(0, w, 0)
        for l in range(LAYERS):
            if w != SM:
                sent(l, w)
            for stage in range(1, len(axes_of(w)) + 1):
                drained(l, w, stage)


def finish(y, xg, oq, oo, ou, od, osm, *outs):
    *outs, spread = outs
    yo, xo, g1, b1, gq, bq, go, bo, g2, b2, gup, bu, gdn, bd = outs
    yo[0] = y[EV]
    xo[0] = xg[EV]
    go[EV] = oo[EV]
    gup[EV] = ou[EV]
    gdn[EV] = od[EV]
    for row, ref in enumerate((g1, b1, bo, g2, b2, bd, bu, bq)):
        for l in range(LAYERS):
            ref[l:l + 1, :] = osm[l, row:row + 1, 0:ref.shape[1]].astype(BF)
    for l in range(LAYERS):
        for h in range(8):
            q, k, v = (oq[l, :, DM * t + HD * h:DM * t + HD * h + HD].astype(F32) for t in range(3))
            spread[0, pl.ds(h, SH, stride=8), :] = jnp.concatenate([q, k], axis=1)
            spread[1, pl.ds(h, SH, stride=8), :] = jnp.concatenate([v, v], axis=1)
        gq[l, :, :, :LN] = spread[0].reshape(SH, 8, LN).astype(BF)
        gq[l, :, :, LN:] = spread[1, :, :HD].reshape(SH, 8, HD).astype(BF)


def rope_constants():
    rot, half, hd = 16, 8, HD
    inv = (1.0 / (10000.0 ** (np.arange(0, rot, 2, dtype=np.float32) / np.float32(rot)))).astype(np.float32)
    ang = np.arange(SEQ, dtype=np.float32)[:, None] * inv[None, :]
    cos, sin = np.cos(ang).astype(np.float32), np.sin(ang).astype(np.float32)
    c = np.ones((SEQ, LN), np.float32)
    p = np.zeros((SEQ, LN), np.float32)
    q = np.zeros((SEQ, LN), np.float32)
    for base in (0, hd):
        c[:, base:base + half] = cos
        c[:, base + half:base + rot] = cos
        p[:, base:base + half] = -sin
        q[:, base + half:base + rot] = sin
    return np.stack([c, p, q])


def solution(mesh):
    shard_axes = ('node', 'local')
    act_spec = P(shard_axes)
    param_spec = P(None, shard_axes)
    consts = rope_constants()
    vm = pl.BlockSpec(memory_space=pltpu.VMEM)
    hbm = pl.BlockSpec(memory_space=pl.ANY)

    def device_step(x, y_cot, g1, b1, wqkv, bqkv, wout, bout, g2, b2, wup, bup, wdn, bdn):
        little = (g1, b1, bout, g2, b2, bdn, bup, bqkv)

        def v(shape, dt):
            return pltpu.VMEM(shape, dt)

        wshape = [(LAYERS, ND * ROWS[w], WIDTH if w == AO else COLS[w]) for w in range(3)]
        scratch = [v(wshape[w], BF) for w in range(3)]
        scratch += [v((2,) * (len(axes_of(w)) + 1) + (ROWS[w], COLS[w]), F32) for w in range(4)]
        for w in range(4):
            n = len(axes_of(w))
            scratch += [v((LAYERS,) + (2,) * (n - i) + (ROWS[w], COLS[w]), F32) for i in range(n + 1)]
        scratch += [v(p.shape, BF) for p in little]
        scratch += [v((LAYERS, 8, DM), F32), v((LAYERS, 1, FF), F32), v((LAYERS, 1, Q3), F32),
                    v((8, DM), F32), v((1, FF), F32), v((1, Q3), F32)]
        scratch += [v((TOK, DM), BF)] * 2
        scratch += [v((3, TOK, LN), F32), v((LAYERS, SH, 8, 3 * HD), BF), v((2, SEQ, LN), F32), v((LAYERS, TOK, FF), BF),
                    v((LAYERS, TOK, FF), F32)]
        scratch += [v((TOK, DM), BF)] * 4 + [v((LAYERS, DM, TOK), BF)] * 2 + [v((LAYERS, TOK, Q3), BF), v((TOK, Q3), BF)]
        scratch += [v((TOK, DM), BF)] * 2 + [v((TOK, DM), F32)] * 2
        dma = pltpu.SemaphoreType.DMA
        scratch += [dma((6, 4)), dma((LAYERS, 3)), dma((LAYERS, 3, 3, 8)), dma((LAYERS, 3)), dma((LAYERS, 4, 3, 4)),
                    dma((LAYERS, 4, 3, 4)), dma((2,)), dma((2,))]
        sds = jax.ShapeDtypeStruct
        mids = pl.pallas_call(
            kernel,
            out_shape=[sds((SEQ, DM), BF), sds((SEQ, DM), BF), sds((LAYERS, SH, Q3), BF), sds((LAYERS, SH, DM), BF),
                       sds((LAYERS, SH, FF), BF), sds((LAYERS, LN, DM), BF), sds((LAYERS, 8, LN), F32)],
            in_specs=[hbm] * 15,
            out_specs=[vm] * 7,
            scratch_shapes=scratch,
            compiler_params=pltpu.CompilerParams(has_side_effects=True, collective_id=0, vmem_limit_bytes=67043328),
            name='step',
        )(x[0], y_cot[0], wqkv, wout, wup, wdn, *little, consts)
        y, xg, oq, oo, ou, od, osm = mids
        like = (x, y_cot, g1, b1, wqkv, bqkv, wout, bout, g2, b2, wup, bup, wdn, bdn)
        return pl.pallas_call(finish, out_shape=[sds(p.shape, BF) for p in like], in_specs=[vm] * 7,
                              out_specs=[vm] * 14, scratch_shapes=[v((2, SEQ, LN), F32)],
                              name='finish')(y, xg, oq, oo, ou, od, osm)

    return jax.shard_map(device_step, mesh=mesh,
                         in_specs=(act_spec, act_spec) + (param_spec,) * 12,
                         out_specs=(act_spec, act_spec) + (param_spec,) * 12,
                         check_vma=False)
```

```python
import numpy as np
import jax
import jax.numpy as jnp
from jax import lax
from jax.experimental import pallas as pl
from jax.experimental.pallas import tpu as pltpu
from jax.sharding import PartitionSpec as P

BF, F32 = jnp.bfloat16, jnp.float32
MESH = pl.DeviceIdType.MESH
EPSILON = 1e-5
LAYERS, SEQ, DM, FF, ND = 2, 256, 512, 2048, 16
SH, HD, LN, Q3 = 32, 64, 128, 1536
ROWS = (SH, SH, LN, 8)
COLS = (FF, FF, DM, LN)
WIDTH = FF + LN
AO, UP, DN, SM = range(4)
ORDERS = ((1, 2, 4), (2, 4, 1), (4, 1, 2))
CHIP_AXES = [4, 2, 1]
CUTS = ((0, 128, 896, FF), (0, 128, 896, FF), (0, SH, 80, LN))
WIDE = (0, 128, 896, WIDTH)
ROUTES = ((1, 2), (2, 1))
ALL, EV = slice(None), ...
TOK = 2 * SEQ


def routes(w):
    return ORDERS[2:] if w == SM else ROUTES


def axes_of(w):
    return CHIP_AXES if w == SM else CHIP_AXES[1:]


def piece(w, k):
    if w == SM:
        return ALL, ALL
    n = (ROWS if w == DN else COLS)[w] // 2
    part = slice(n * k, n * k + n)
    return (part, ALL) if w == DN else (ALL, part)


def bit(v, a):
    return lax.rem(lax.div(v, a), 2)


def flip(v, mask):
    for a in (1, 2, 4):
        if mask & a:
            v = v + a - 2 * a * bit(v, a)
    return v


def col_sum(v):
    return jnp.sum(v, axis=0, keepdims=True)


def row_of(f, v):
    return f(v, axis=-1, keepdims=True)


def mm(a, b):
    return jnp.dot(a, b, preferred_element_type=F32)


def mm_nt(a, b):
    return lax.dot_general(a, b, (((1,), (1,)), ((), ())), preferred_element_type=F32)


def mm_tn(a, b):
    return lax.dot_general(a, b, (((0,), (0,)), ((), ())), preferred_element_type=F32)


def kernel(x_in, cot_in, wq_in, wo_in, wu_in, wd_in, p0, p1, p2, p3, p4, p5, p6, p7, rope_in,
           y_ref, xg_ref, oq_ref, oo_ref, ou_ref, od_ref, os_ref,
           wa, wu, wd, ga, gu, gd, gs, ra0, ra1, ra2, ru0, ru1, ru2, rd0, rd1, rd2, rs0, rs1, rs2, rs3,
           v0, v1, v2, v3, v4, v5, v6, v7, vec, upb, qkvb, gvec, gub, gqb,
           x_ref, cot_ref, rope_ref, native, spread, act_s, slope_s,
           h1, dh, na, nm, nat, nmt, qkv, dqkv, ctx, dctx, acc, dnm,
           loc_sem, ag_send, ag_ici, ag_d2d, rs_send, rs_recv, ex_send, ex_recv):
    me = lax.axis_index('node') * 8 + lax.axis_index('local')
    chip = lax.div(me, 2)
    core = lax.rem(me, 2)
    other = 1 - core
    W, G = (wa, wu, wd), (ga, gu, gd, gs)
    R = ((ra0, ra1, ra2), (ru0, ru1, ru2), (rd0, rd1, rd2), (rs0, rs1, rs2, rs3))
    node = lax.div(chip, 4)
    zrows = pl.ds(pl.multiple_of(node * SEQ, SEQ), SEQ)

    def dev(c, k):
        i = c * 2 + k
        return (lax.div(i, 8), lax.rem(i, 8))

    def rows_of(l, w, start, n):
        rows = pl.ds(start, n * ROWS[w])
        if w == AO and l == 1:
            return W[w].at[l, rows, pl.ds(0, FF)]
        return W[w].at[l, rows]

    def block(l, w, c, k):
        return rows_of(l, w, pl.multiple_of((c * 2 + k) * ROWS[w], ROWS[w]), 1)

    def part(l, w, k, mask):
        base = (flip(chip, mask) * 2 + core) * ROWS[w]
        cuts = WIDE if w == AO and l == 0 else CUTS[w]
        lo, hi = cuts[k], cuts[k + 1]
        if w == DN:
            return W[w].at[l, pl.ds(pl.multiple_of(base + lo, 16), hi - lo)]
        return W[w].at[l, pl.ds(pl.multiple_of(base, SH), SH), lo:hi]

    def push(l, w, src, to, recv_sem):
        pltpu.make_async_remote_copy(src_ref=src, dst_ref=src, send_sem=ag_send.at[l, w], recv_sem=recv_sem,
                                     device_id=to, device_id_type=MESH).start()

    def to_link(l, w, k, mask, a):
        push(l, w, part(l, w, k, mask), dev(flip(chip, a), core), ag_ici.at[l, w, k, mask ^ a])

    def to_partner(l, w, k, mask):
        push(l, w, part(l, w, k, mask), dev(chip, other), ag_d2d.at[l, w])

    def await_in(l, w, src, recv_sem):
        pltpu.make_async_remote_copy(src_ref=src, dst_ref=src, send_sem=ag_send.at[l, w], recv_sem=recv_sem,
                                     device_id=dev(chip, other), device_id_type=MESH).wait_recv()

    def got(l, w, k, mask):
        await_in(l, w, part(l, w, k, mask), ag_ici.at[l, w, k, mask])

    def got_partner(l, w):
        await_in(l, w, rows_of(l, w, 0, 8), ag_d2d.at[l, w])

    def sent(l, w):
        src = rows_of(l, w, 0, 15)
        pltpu.make_async_remote_copy(src_ref=src, dst_ref=src, send_sem=ag_send.at[l, w], recv_sem=ag_d2d.at[l, w],
                                     device_id=dev(chip, other), device_id_type=MESH).wait_send()

    def own(l, w):
        for i in range(3):
            for k in range(3):
                to_link(l, w, k, 0, ORDERS[k][i])
        push(l, w, block(l, w, chip, core), dev(chip, other), ag_d2d.at[l, w])

    def f1(l, w):
        for k, (a, b, c) in enumerate(ORDERS):
            got(l, w, k, a)
            to_link(l, w, k, a, b)
        for k, (a, b, c) in enumerate(ORDERS):
            to_link(l, w, k, a, c)
            to_partner(l, w, k, a)

    def f2(l, w):
        for k, (a, b, c) in enumerate(ORDERS):
            got(l, w, k, b)
            to_link(l, w, k, b, c)
            to_partner(l, w, k, b)

    def f3(l, w):
        for k, (a, b, c) in enumerate(ORDERS):
            got(l, w, k, a | b)
            to_link(l, w, k, a | b, c)
            to_partner(l, w, k, a | b)

    def f4(l, w):
        for i in range(4):
            for k, (a, b, c) in enumerate(ORDERS):
                m = (c, a | c, b | c, 7)[i]
                got(l, w, k, m)
                to_partner(l, w, k, m)

    rs = {}

    def rs_copy(l, w, k, stage, src, dst, to):
        cp = pltpu.make_async_remote_copy(src_ref=src, dst_ref=dst, send_sem=rs_send.at[l, w, k, stage],
                                          recv_sem=rs_recv.at[l, w, k, stage], device_id=to, device_id_type=MESH)
        cp.start()
        rs[l, w, k, stage] = cp

    def pick(axes, a, v):
        return tuple(v if m == a else ALL for m in axes)

    def drained(l, w, stage):
        for k in range(len(routes(w))):
            rs[l, w, k, stage].wait_send()

    def step(l, w, stage):
        axes = axes_of(w)
        n = len(axes)
        for k, route in enumerate(routes(w)):
            cut = piece(w, k)
            if stage == 0:
                rs_copy(l, w, k, 0, G[w].at[(ALL,) * n + (other,) + cut], R[w][0].at[(l,) + (ALL,) * n + cut],
                        dev(chip, other))
                continue
            rs[l, w, k, stage - 1].wait_recv()
            buf = R[w][stage - 1]
            left = [m for m in axes if m not in route[:stage - 1]]
            before = [m for m in axes if m not in route[:stage - 2]] if stage > 1 else axes

            def mine(where):
                if stage == 1:
                    return G[w][where + (core,) + cut]
                at = list(where)
                at.insert(before.index(route[stage - 2]), bit(chip, route[stage - 2]))
                return R[w][stage - 2][(l,) + tuple(at) + cut]

            if stage == n + 1:
                emit(l, w, k, cut, buf[(l,) + cut] + mine(()))
                continue
            for i in range(2 ** len(left)):
                where = tuple((i >> j) & 1 for j in range(len(left)))
                at = (l,) + where + cut
                buf[at] = buf[at] + mine(where)
            a = route[stage - 1]
            src = buf.at[(l,) + pick(left, a, 1 - bit(chip, a)) + cut]
            rs_copy(l, w, k, stage, src, R[w][stage].at[(l,) + (ALL,) * (len(left) - 1) + cut],
                    dev(flip(chip, a), core))

    def emit(l, w, k, cut, total):
        if w == SM:
            os_ref[l] = total
            return
        total = total.astype(BF)
        if w != AO:
            (None, ou_ref, od_ref)[w][(l,) + cut] = total
        elif k == 0:
            oq_ref[(l,) + cut] = total
        else:
            n = Q3 - cut[1].start
            oq_ref[l, :, cut[1].start:] = total[:, :n]
            oo_ref[l] = total[:, n:]

    def s0(l, w):
        step(l, w, 0)

    def s1(l, w):
        step(l, w, 1)

    def s2(l, w):
        step(l, w, 2)

    def s3(l, w):
        step(l, w, 3)

    def s4(l, w):
        step(l, w, 4)

    def normed(h_bf):
        h32 = h_bf.astype(F32)
        cen = h32 - row_of(jnp.mean, h32)
        rstd = lax.rsqrt(row_of(jnp.mean, cen * cen) + EPSILON)
        return cen * rstd, rstd

    def norms(h_ref, l):
        xhat, _ = normed(h_ref[EV])
        n1 = (xhat * vec[l, 0:1, :] + vec[l, 1:2, :]).astype(BF)
        n2 = (xhat * vec[l, 3:4, :] + vec[l, 4:5, :]).astype(BF)
        na[EV] = n1
        nm[EV] = n2
        nat[l] = n1.T
        nmt[l] = n2.T

    def rope(xs, back, n):
        c, p, q = (rope_ref[t, :n] for t in range(3))
        if back:
            return xs * c + pltpu.roll(xs * p, 8, 1) + pltpu.roll(xs * q, 120, 1)
        return xs * c + pltpu.roll(xs, 120, 1) * p + pltpu.roll(xs, 8, 1) * q

    def make_qkv(l):
        for t in range(3):
            cols = slice(DM * t, DM * t + DM)
            raw = mm(na[EV], wa[l, :, cols]) + qkvb[l, :, cols]
            for s in range(4):
                part = raw[:, LN * s:LN * s + LN]
                if t < 2:
                    part = rope(part, False, TOK)
                qkv[l, :, DM * t + LN * s:DM * t + LN * s + LN] = part.astype(BF)

    def heads(l, bwd, lo, hi):
        lane = lax.broadcasted_iota(jnp.int32, (1, LN), 1)
        sides = [(lane < HD).astype(F32), (lane >= HD).astype(F32)]
        row, key = (lax.broadcasted_iota(jnp.int32, (TOK, SEQ), t) for t in range(2))
        causal = lax.rem(row, SEQ) >= key

        def stacked(v, scale):
            return jnp.concatenate([v * (side * scale).astype(BF) for side in sides])

        def along(v):
            return jnp.concatenate([v[:SEQ], v[SEQ:]], axis=1)

        def pair(seq, col):
            rows = slice(SEQ * seq, SEQ * seq + SEQ)
            q, k, v = (qkv[l, rows, pl.ds(col + DM * t, LN)] for t in range(3))
            qs = stacked(q, 0.125)
            sc = jnp.where(causal, mm_nt(qs, k), -1e30)
            e = jnp.exp(sc - row_of(jnp.max, sc))
            p = e * (1.0 / row_of(jnp.sum, e))
            pb = p.astype(BF)
            ctx[rows, pl.ds(col, LN)] = mm(along(pb), stacked(v, 1.0)).astype(BF)
            if not bwd:
                return
            ds_ = stacked(dctx[rows, pl.ds(col, LN)], 1.0)
            dp = mm_nt(ds_, v).astype(BF).astype(F32)
            ds = (p * (dp - row_of(jnp.sum, dp * p))).astype(BF)
            grads = (mm(along(ds), stacked(k, 0.125)), mm_tn(ds, qs), mm_tn(pb, ds_))
            for t, d in enumerate(grads):
                d = d.astype(BF).astype(F32)
                if t < 2:
                    d = rope(d, True, SEQ)
                if seq == 0:
                    gqb[0:1, pl.ds(col + DM * t, LN)] = col_sum(d)
                dqkv[rows, pl.ds(col + DM * t, LN)] = d.astype(BF)

        def body(j, carry):
            col = pl.multiple_of(j * LN, LN)
            for seq in range(2):
                pair(seq, col)
            return carry

        lax.fori_loop(lo, hi, body, 0)

    def up_part(l, t):
        col = pl.multiple_of(t * DM, DM)
        pre = mm(nm[EV], wu[l, :, pl.ds(col, DM)]) + upb[l, :, pl.ds(col, DM)]
        cdf = 0.5 * (1.0 + lax.erf(pre * 0.7071067811865476))
        return col, pre, cdf, (pre * cdf).astype(BF)

    def activate(l, fwd, lo, hi):
        def body(t, carry):
            col, pre, cdf, act = up_part(l, t)
            act_s[l, :, pl.ds(col, DM)] = act
            slope_s[l, :, pl.ds(col, DM)] = cdf + pre * (0.3989422804014327 * jnp.exp(-0.5 * pre * pre))
            if fwd:
                acc[EV] += mm(act, wd[l, pl.ds(col, DM), :])
            return carry

        if fwd and lo == 0:
            acc[EV] = jnp.zeros_like(acc)
        lax.fori_loop(lo, hi, body, 0)

    def down_grad(l, dout):
        def grad(t, carry):
            col = pl.multiple_of(node * 2 * DM + t * DM, DM)
            gd[t] = mm_tn(act_s[l, :, pl.ds(col, DM)], dout[EV]).reshape(2, 2, LN, DM)
            return carry

        lax.fori_loop(0, 2, grad, 0)

    def mlp_b(l, dout, fwd, lo, hi):
        def body(t, carry):
            col = pl.multiple_of(t * DM, DM)
            wd_t = wd[l, pl.ds(col, DM), :]
            if fwd:
                acc[:SEQ] += mm(act_s[l, :SEQ, pl.ds(col, DM)], wd_t)
            dpre = mm_nt(dout[EV], wd_t).astype(BF).astype(F32) * slope_s[l, :, pl.ds(col, DM)]
            gub[0:1, pl.ds(col, DM)] = col_sum(dpre[:SEQ])
            dpb = dpre.astype(BF)
            gu[:, :, :, :, pl.ds(col, DM)] = mm(nmt[l, zrows, :], dpb).reshape(2, 2, 2, SH, DM)
            dnm[EV] += mm_nt(dpb, wu[l, :, pl.ds(col, DM)])
            return carry

        if lo == 0:
            dnm[EV] = jnp.zeros_like(dnm)
            if fwd:
                acc[EV] = jnp.zeros_like(acc)
        lax.fori_loop(lo, hi, body, 0)

    def attn_grads(l, dout):
        ga[:, :, :, :, Q3:] = mm_tn(ctx[:, zrows], dout[EV]).reshape(2, 2, 2, SH, DM)
        for t in range(3):
            cols = slice(DM * t, DM * t + DM)
            ga[:, :, :, :, cols] = mm(nat[l, zrows, :], dqkv[:, cols]).reshape(2, 2, 2, SH, DM)

    def layer_end(h_ref, l, dout, n):
        dna = mm_nt(dqkv[:n], wa[l, :, 0:Q3]).astype(BF).astype(F32)
        dnm32 = dnm[:n].astype(BF).astype(F32)
        xhat, rstd = normed(h_ref[:n])
        d32 = dout[:n].astype(F32)
        own_tok = slice(0, SEQ)
        sums = [dna * xhat, dna, d32, dnm32 * xhat, dnm32, d32]
        for i, v in enumerate(sums):
            gvec[i:i + 1, :] = col_sum(v[own_tok])
        dx = dna * vec[l, 0:1, :] + dnm32 * vec[l, 3:4, :]
        dhid = rstd * (dx - row_of(jnp.mean, dx) - xhat * row_of(jnp.mean, dx * xhat))
        return (d32 + dhid).astype(BF)

    def small_grads():
        for d in range(ND):
            at = (d // 8, d // 4 % 2, d // 2 % 2, d % 2)
            gs[at] = jnp.zeros((8, LN), F32)
            gs[at + (slice(0, 6), slice(0, SH))] = gvec[0:6, SH * d:SH * d + SH]
            gs[at + (slice(6, 7), ALL)] = gub[0:1, LN * d:LN * d + LN]
            for lo, col, n in bias_parts(d):
                gs[at + (slice(7, 8), slice(lo, lo + n))] = gqb[0:1, col:col + n]

    def vectors():
        for d in range(ND):
            both = wa[0, SH * d:SH * d + 16, FF:].astype(F32)
            for l in range(LAYERS):
                rows = both[8 * l:8 * l + 8]
                vec[l, 0:6, SH * d:SH * d + SH] = rows[0:6, 0:SH]
                upb[l, 0:1, LN * d:LN * d + LN] = rows[6:7]
                for lo, col, n in bias_parts(d):
                    qkvb[l, 0:1, col:col + n] = rows[7:8, lo:lo + n]

    def bias_parts(d):
        base = HD * (d // 2)
        if d % 2 == 0:
            return ((0, base, HD), (HD, DM + base, SH))
        return ((0, DM + base + SH, SH), (SH, 1024 + base, HD))

    def swap(i, ref):
        return pltpu.make_async_remote_copy(src_ref=ref.at[pl.ds(0, SEQ)], dst_ref=ref.at[pl.ds(SEQ, SEQ)],
                                            send_sem=ex_send.at[i], recv_sem=ex_recv.at[i],
                                            device_id=dev(flip(chip, 4), core), device_id_type=MESH)

    swap_x, swap_cot = swap(0, x_ref), swap(1, cot_ref)
    (A0, U0, D0, V0), (A1, U1, D1, V1) = [[(l, w) for w in (AO, UP, DN, SM)] for l in range(LAYERS)]
    native_in = pltpu.make_async_copy(wq_in, native, loc_sem.at[0, 0])
    first = [pltpu.make_async_copy(wu_in.at[0], block(0, UP, chip, core), loc_sem.at[0, 1])]
    qo = pl.ds(pl.multiple_of(me * SH, SH), SH)
    rest = [pltpu.make_async_copy(wo_in.at[l], W[AO].at[l, qo, pl.ds(Q3, DM)], loc_sem.at[l + 2, 2])
            for l in range(LAYERS)]
    rest += [pltpu.make_async_copy(wd_in.at[l], block(l, DN, chip, core), loc_sem.at[l + 2, 3]) for l in range(LAYERS)]
    rest += [pltpu.make_async_copy(wu_in.at[1], block(1, UP, chip, core), loc_sem.at[0, 2]),
             pltpu.make_async_copy(x_in, x_ref.at[pl.ds(0, SEQ)], loc_sem.at[0, 3]),
             pltpu.make_async_copy(cot_in, cot_ref.at[pl.ds(0, SEQ)], loc_sem.at[1, 0]),
             pltpu.make_async_copy(rope_in, rope_ref.at[:, pl.ds(0, SEQ)], loc_sem.at[1, 1]),
             pltpu.make_async_copy(rope_in, rope_ref.at[:, pl.ds(SEQ, SEQ)], loc_sem.at[1, 2])]
    params, tmp = (p0, p1, p2, p3, p4, p5, p6, p7), (v0, v1, v2, v3, v4, v5, v6, v7)
    little = [pltpu.make_async_copy(params[i], tmp[i], loc_sem.at[4 + i // 4, i % 4]) for i in range(8)]
    first[0].start()
    native_in.start()
    for cp in little + rest:
        cp.start()

    barrier = pltpu.get_barrier_semaphore()
    near = [dev(chip, other)] + [dev(flip(chip, a), core) for a in CHIP_AXES]
    for to in near:
        pl.semaphore_signal(barrier, inc=1, device_id=to, device_id_type=MESH)
    first[0].wait()
    pl.semaphore_wait(barrier, len(near))
    own(*U0)

    native_in.wait()
    for l in range(LAYERS):
        flat = native[l].astype(F32).reshape(SEQ, 3 * HD)
        spread[0] = flat[:, :LN]
        spread[1, :, :HD] = flat[:, LN:]
        for h in range(8):
            rows = [spread[i, pl.ds(h, SH, stride=8), :].astype(BF) for i in range(2)]
            for t in range(3):
                lo = HD * (t % 2)
                wa[l, qo, DM * t + HD * h:DM * t + HD * h + HD] = rows[t // 2][:, lo:lo + HD]
        if l == 0:
            for cp in little + rest:
                cp.wait()
            spread[0, 0:SH] = jnp.zeros((SH, LN), F32)
            for i in range(8):
                for m in range(LAYERS):
                    spread[0, 8 * m + i:8 * m + i + 1, 0:tmp[i].shape[1]] = tmp[i][m:m + 1, :].astype(F32)
            wa[0, qo, FF:] = spread[0, 0:SH].astype(BF)
            own(*A0)
    swap_x.start()
    f1(*A0)
    f1(*U0)
    f2(*A0)
    own(*D0)
    f2(*U0)
    f3(*A0)
    f3(*U0)
    f1(*D0)
    f4(*A0)
    own(*U1)
    f4(*U0)
    got_partner(*A0)
    vectors()
    swap_x.wait_recv()
    norms(x_ref, 0)
    f2(*D0)
    make_qkv(0)
    f3(*D0)
    heads(0, False, 0, 1)
    f1(*U1)
    heads(0, False, 1, 2)
    f2(*U1)
    own(*A1)
    heads(0, False, 2, 4)
    f4(*D0)
    got_partner(*U0)
    got_partner(*D0)
    swap_cot.start()
    activate(0, True, 0, 2)
    f3(*U1)
    f1(*A1)
    activate(0, True, 2, 4)
    own(*D1)
    acc[EV] += mm(ctx[EV], wa[0, :, Q3:FF])
    h1[EV] = (x_ref[EV].astype(F32) + acc[EV] + vec[0, 2:3, :] + vec[0, 5:6, :]).astype(BF)
    f4(*U1)
    f2(*A1)
    norms(h1, 1)
    got_partner(*U1)
    activate(1, False, 0, 4)
    swap_cot.wait_recv()
    down_grad(1, cot_ref)
    s0(*D1)
    f3(*A1)
    f1(*D1)
    f4(*A1)
    s1(*D1)
    f2(*D1)
    got_partner(*A1)
    make_qkv(1)
    dctx[EV] = mm_nt(cot_ref[EV], wa[1, :, Q3:FF]).astype(BF)
    f3(*D1)
    heads(1, True, 0, 2)
    f4(*D1)
    heads(1, True, 2, 3)
    s2(*D1)
    heads(1, True, 3, 4)
    attn_grads(1, cot_ref)
    s0(*A1)
    got_partner(*D1)
    mlp_b(1, cot_ref, True, 0, 2)
    s1(*A1)
    mlp_b(1, cot_ref, True, 2, 4)
    s0(*U1)
    dh[EV] = layer_end(h1, 1, cot_ref, TOK)
    s1(*U1)
    acc[:SEQ] += mm(ctx[:SEQ], wa[1, :, Q3:FF])
    y_ref[EV] = (h1[:SEQ].astype(F32) + acc[:SEQ] + vec[1, 2:3, :] + vec[1, 5:6, :]).astype(BF)
    small_grads()
    s0(*V1)

    drained(*D1, 0)
    down_grad(0, dh)
    s0(*D0)
    drained(*U1, 0)
    mlp_b(0, dh, False, 0, 2)
    s1(*D0)
    s2(*A1)
    mlp_b(0, dh, False, 2, 4)
    s0(*U0)
    s1(*V1)
    dctx[EV] = mm_nt(dh[EV], wa[0, :, Q3:FF]).astype(BF)
    s1(*U0)
    heads(0, True, 0, 2)
    s2(*U1)
    s2(*V1)
    s2(*D0)
    heads(0, True, 2, 4)
    xg_ref[EV] = layer_end(x_ref, 0, dh, SEQ)
    drained(*V1, 0)
    small_grads()
    s0(*V0)
    drained(*A1, 0)
    attn_grads(0, dh)
    s0(*A0)
    s1(*V0)
    s3(*V1)
    s1(*A0)
    for stage, at in ((s2, V0), (s2, U0), (s3, D1), (s3, A1), (s3, V0), (s2, A0), (s3, U1), (s4, V1), (s3, D0),
                      (s3, U0), (s4, V0), (s3, A0)):
        stage(*at)
    swap_x.wait_send()
    swap_cot.wait_send()
    for w in (DN, UP, AO, SM):
        drained(0, w, 0)
        for l in range(LAYERS):
            if w != SM:
                sent(l, w)
            for stage in range(1, len(axes_of(w)) + 1):
                drained(l, w, stage)


def finish(y, xg, oq, oo, ou, od, osm, *outs):
    *outs, spread = outs
    yo, xo, g1, b1, gq, bq, go, bo, g2, b2, gup, bu, gdn, bd = outs
    yo[0] = y[EV]
    xo[0] = xg[EV]
    go[EV] = oo[EV]
    gup[EV] = ou[EV]
    gdn[EV] = od[EV]
    for row, ref in enumerate((g1, b1, bo, g2, b2, bd, bu, bq)):
        for l in range(LAYERS):
            ref[l:l + 1, :] = osm[l, row:row + 1, 0:ref.shape[1]].astype(BF)
    for l in range(LAYERS):
        for h in range(8):
            q, k, v = (oq[l, :, DM * t + HD * h:DM * t + HD * h + HD].astype(F32) for t in range(3))
            spread[0, pl.ds(h, SH, stride=8), :] = jnp.concatenate([q, k], axis=1)
            spread[1, pl.ds(h, SH, stride=8), :] = jnp.concatenate([v, v], axis=1)
        gq[l, :, :, :LN] = spread[0].reshape(SH, 8, LN).astype(BF)
        gq[l, :, :, LN:] = spread[1, :, :HD].reshape(SH, 8, HD).astype(BF)


def rope_constants():
    rot, half, hd = 16, 8, HD
    inv = (1.0 / (10000.0 ** (np.arange(0, rot, 2, dtype=np.float32) / np.float32(rot)))).astype(np.float32)
    ang = np.arange(SEQ, dtype=np.float32)[:, None] * inv[None, :]
    cos, sin = np.cos(ang).astype(np.float32), np.sin(ang).astype(np.float32)
    c = np.ones((SEQ, LN), np.float32)
    p = np.zeros((SEQ, LN), np.float32)
    q = np.zeros((SEQ, LN), np.float32)
    for base in (0, hd):
        c[:, base:base + half] = cos
        c[:, base + half:base + rot] = cos
        p[:, base:base + half] = -sin
        q[:, base + half:base + rot] = sin
    return np.stack([c, p, q])


def solution(mesh):
    shard_axes = ('node', 'local')
    act_spec = P(shard_axes)
    param_spec = P(None, shard_axes)
    consts = rope_constants()
    vm = pl.BlockSpec(memory_space=pltpu.VMEM)
    hbm = pl.BlockSpec(memory_space=pl.ANY)

    def device_step(x, y_cot, g1, b1, wqkv, bqkv, wout, bout, g2, b2, wup, bup, wdn, bdn):
        little = (g1, b1, bout, g2, b2, bdn, bup, bqkv)

        def v(shape, dt):
            return pltpu.VMEM(shape, dt)

        wshape = [(LAYERS, ND * ROWS[w], WIDTH if w == AO else COLS[w]) for w in range(3)]
        scratch = [v(wshape[w], BF) for w in range(3)]
        scratch += [v((2,) * (len(axes_of(w)) + 1) + (ROWS[w], COLS[w]), F32) for w in range(4)]
        for w in range(4):
            n = len(axes_of(w))
            scratch += [v((LAYERS,) + (2,) * (n - i) + (ROWS[w], COLS[w]), F32) for i in range(n + 1)]
        scratch += [v(p.shape, BF) for p in little]
        scratch += [v((LAYERS, 8, DM), F32), v((LAYERS, 1, FF), F32), v((LAYERS, 1, Q3), F32),
                    v((8, DM), F32), v((1, FF), F32), v((1, Q3), F32)]
        scratch += [v((TOK, DM), BF)] * 2
        scratch += [v((3, TOK, LN), F32), v((LAYERS, SH, 8, 3 * HD), BF), v((2, SEQ, LN), F32), v((LAYERS, TOK, FF), BF),
                    v((LAYERS, TOK, FF), F32)]
        scratch += [v((TOK, DM), BF)] * 4 + [v((LAYERS, DM, TOK), BF)] * 2 + [v((LAYERS, TOK, Q3), BF), v((TOK, Q3), BF)]
        scratch += [v((TOK, DM), BF)] * 2 + [v((TOK, DM), F32)] * 2
        dma = pltpu.SemaphoreType.DMA
        scratch += [dma((6, 4)), dma((LAYERS, 3)), dma((LAYERS, 3, 3, 8)), dma((LAYERS, 3)), dma((LAYERS, 4, 3, 4)),
                    dma((LAYERS, 4, 3, 4)), dma((2,)), dma((2,))]
        sds = jax.ShapeDtypeStruct
        mids = pl.pallas_call(
            kernel,
            out_shape=[sds((SEQ, DM), BF), sds((SEQ, DM), BF), sds((LAYERS, SH, Q3), BF), sds((LAYERS, SH, DM), BF),
                       sds((LAYERS, SH, FF), BF), sds((LAYERS, LN, DM), BF), sds((LAYERS, 8, LN), F32)],
            in_specs=[hbm] * 15,
            out_specs=[vm] * 7,
            scratch_shapes=scratch,
            compiler_params=pltpu.CompilerParams(has_side_effects=True, collective_id=0, vmem_limit_bytes=67043328),
            name='step',
        )(x[0], y_cot[0], wqkv, wout, wup, wdn, *little, consts)
        y, xg, oq, oo, ou, od, osm = mids
        like = (x, y_cot, g1, b1, wqkv, bqkv, wout, bout, g2, b2, wup, bup, wdn, bdn)
        return pl.pallas_call(finish, out_shape=[sds(p.shape, BF) for p in like], in_specs=[vm] * 7,
                              out_specs=[vm] * 14, scratch_shapes=[v((2, SEQ, LN), F32)],
                              name='finish')(y, xg, oq, oo, ou, od, osm)

    return jax.shard_map(device_step, mesh=mesh,
                         in_specs=(act_spec, act_spec) + (param_spec,) * 12,
                         out_specs=(act_spec, act_spec) + (param_spec,) * 12,
                         check_vma=False)
```
